256 devices in a mesh: dp: 64 (over z, y, core), mp: 4 (over x).
Axes of the slice: x: 4, y: 4, z: 8, core: 2. Of those that a mesh axis runs over, the one named last changes fastest.
Arguments:
- tokens: bfloat16 [393216, 512], P('dp'), may hold values from -6 to 6
- w_uvqk: bfloat16 [512, 2048], P(None, 'mp')
- w_out: bfloat16 [512, 512], replicated, may hold values from -0.25 to 0.25
- hist_len: int32 [64, 24], P('dp'), may hold values from 64 to 256, as said below
- owner: int32 [64, 24], P('dp'), may hold values from 0 to 63, as said below
- recv_offset: int32 [64, 24], P('dp'), may hold values from 0 to 47, as said below
- block_start: int32 [64, 24], P('dp'), may hold values from 0 to 47, as said below
Outputs:
- packed_out: bfloat16 [393216, 512], P('dp', 'mp')
- user_state: bfloat16 [1536, 512], P('dp', 'mp')
The draws below stay inside these ranges and needn't reach their ends.
Inputs may be any that keep to these rules, and one draw needn't show every extreme that they name: User (d, u) has ceil(hist_len / 128) blocks, at most 2. owner[d, u] = (p(d) + r(u mod 64)) mod 64 for two permutations p, r of the indices of dp drawn from the seed: every owner receives exactly 24 users, and one device sends at most 1 users to one owner. On some owner every received user has 2 blocks. `recv_offset`: the users of one owner occupy disjoint runs of its 48 blocks, in the order of u; on some owner they fill all 48 blocks. `block_start`: the users of one device occupy disjoint runs of its 48 blocks, in the order of u.
All inputs are finite; a program needn't handle non-finite values.
Results may differ from the reference program's by a relative error of at most 0.0059.
Values may be sent and summed in bfloat16 or wider, within the bound.
No kernel may reach another device: no remote copies, remote signals or barrier semaphores. Data moves between devices by JAX's collectives and lax.ppermute only.
A program may use at most 128 MiB of HBM per device.

```python
import jax
import jax.numpy as jnp
from jax import lax

D = 512
HEADS = 4
BLOCK = 128
MAXB = 2
USERS_DEV = 24
BLK_DEV = 48
ROWS = 393216
N_DP = 64


def place_runs(key, run_sizes, salt_value):
    before = jnp.cumsum(run_sizes, axis=1) - run_sizes
    spare_blocks = BLK_DEV - jnp.sum(run_sizes, axis=1, keepdims=True)
    gap_sums = jnp.cumsum(jax.random.randint(jax.random.fold_in(key, salt_value), run_sizes.shape, 0, 2), axis=1)
    return (before + jnp.minimum(gap_sums, spare_blocks)).astype(jnp.int32)


def draw_tables(key):
    device_count = N_DP
    user_count = USERS_DEV
    dev_perm = jax.random.permutation(jax.random.fold_in(key, 101), device_count).astype(jnp.int32)
    user_perm = jax.random.permutation(jax.random.fold_in(key, 102), device_count).astype(jnp.int32)
    user_ids = jnp.arange(user_count, dtype=jnp.int32)
    shifts = user_perm[user_ids % device_count]
    owners = ((dev_perm[:, None] + shifts[None, :]) % device_count).astype(jnp.int32)
    hottest = jax.random.randint(jax.random.fold_in(key, 103), (), 0, device_count)
    coin_flip = jax.random.randint(jax.random.fold_in(key, 104), (device_count, user_count), 0, 4)
    small_count = jax.random.randint(jax.random.fold_in(key, 108), (device_count, user_count), 1, MAXB + 1)
    counts = jnp.where(coin_flip > 0, MAXB, small_count)
    counts = jnp.where(owners == hottest, MAXB, counts).astype(jnp.int32)
    least_tail = jnp.where(counts == 1, BLOCK // 2, 1)
    extra_rows = jax.random.randint(jax.random.fold_in(key, 105), (device_count, user_count), 0, BLOCK + 1)
    last_fill = least_tail + extra_rows % (BLOCK + 1 - least_tail)
    lengths = ((counts - 1) * BLOCK + last_fill).astype(jnp.int32)
    starts = place_runs(key, counts, 106)
    inverse = jnp.zeros((device_count,), jnp.int32).at[dev_perm].set(jnp.arange(device_count, dtype=jnp.int32))
    sources = inverse[(jnp.arange(device_count, dtype=jnp.int32)[:, None] - shifts[None, :]) % device_count]
    incoming = counts[sources, user_ids[None, :]]
    landing = place_runs(key, incoming, 107)
    offsets = landing[owners, user_ids[None, :]].astype(jnp.int32)
    return (lengths, owners, offsets, starts)


def draw_hist_len(key, part):
    return draw_tables(key)[0]


def draw_owner(key, part):
    return draw_tables(key)[1]


def draw_recv_offset(key, part):
    return draw_tables(key)[2]


def draw_block_start(key, part):
    return draw_tables(key)[3]


def draw_w_uvqk(key, part):
    base_draw = jax.random.normal(jax.random.fold_in(key, 1), (D, 4 * D), jnp.float32)
    log_scale = jax.random.uniform(jax.random.fold_in(key, 2), (1, 4 * D), jnp.float32, -1.2, 1.2)
    return (base_draw * jnp.exp(log_scale) / jnp.sqrt(D * 1.0)).astype(jnp.bfloat16)


def shard_levels(rng, extent, split, least, high):
    factor_of = 1.0
    for dim, parts in split:
        steps = jax.random.uniform(jax.random.fold_in(jax.random.fold_in(rng, 6), dim), (parts,), jnp.float32, least / len(split), high / len(split))
        factor_of = factor_of * jnp.repeat(jnp.exp(steps), extent[dim] // parts).reshape((-1,) + (1,) * (len(extent) - 1 - dim))
    return factor_of


def normal_values(key, extent, spread, bound, split=(), held_as=jnp.bfloat16):
    values = jax.random.normal(key, extent, jnp.float32) * spread
    if len(split) > 0:
        values = shard_levels(key, extent, split, -0.22, 0.18) * values
    return jnp.clip(values, min=-bound, max=bound).astype(held_as)


def setup_inputs(seed: int = 0) -> dict:
    key_of = jax.random.split(jax.random.key(seed), 8)
    tokens = normal_values(key_of[0], (ROWS, D), 1.0, 6.0, ((0, 64),))
    w_uvqk = draw_w_uvqk(jax.random.fold_in(key_of[7], 71), 0)
    w_out = normal_values(key_of[2], (D, D), D ** -0.5, 0.25)
    hist_len = draw_hist_len(jax.random.fold_in(key_of[7], 71), 0)
    owner = draw_owner(jax.random.fold_in(key_of[7], 71), 0)
    recv_offset = draw_recv_offset(jax.random.fold_in(key_of[7], 71), 0)
    block_start = draw_block_start(jax.random.fold_in(key_of[7], 71), 0)
    return dict(tokens=tokens, w_uvqk=w_uvqk, w_out=w_out, hist_len=hist_len, owner=owner, recv_offset=recv_offset, block_start=block_start)


EPS = 1e-05

def norm_rows(values):
    average = lax.optimization_barrier(jnp.mean(values, axis=-1, keepdims=True))
    variance = lax.optimization_barrier(jnp.mean(values * values, axis=-1, keepdims=True)) - average * average
    return (values - average) * lax.rsqrt(variance + EPS)

def rounded(values):
    return lax.optimization_barrier(values.astype(jnp.bfloat16)).astype(jnp.float32)

def reference(tokens, w_uvqk, w_out, hist_len, owner, recv_offset, block_start):
    head_size = D // HEADS
    window_rows = MAXB * BLOCK
    total_rows = tokens.shape[0]
    device_count = hist_len.shape[0]
    user_count = hist_len.shape[1]
    padded = jnp.concatenate([tokens, jnp.zeros((window_rows, D), tokens.dtype)], 0)
    position = jnp.arange(window_rows, dtype=jnp.int32)
    causal = position[None, :] <= position[:, None]
    device_ids = (jnp.arange(device_count * user_count, dtype=jnp.int32) // user_count).astype(jnp.int32)
    flat_len = hist_len.reshape(-1).astype(jnp.int32)
    flat_start = block_start.reshape(-1).astype(jnp.int32)
    flat_owner = owner.reshape(-1).astype(jnp.int32)
    flat_offset = recv_offset.reshape(-1).astype(jnp.int32)

    def one_user(user_item):
        device_id, length, start = user_item
        first_row = ((device_id * BLK_DEV + start) * BLOCK).astype(jnp.int32)
        rows_in = lax.dynamic_slice_in_dim(padded, first_row, window_rows, 0)
        widened = rows_in.astype(jnp.float32)
        normed = norm_rows(widened).astype(jnp.bfloat16)
        projected = jax.nn.silu(jnp.dot(normed, w_uvqk, preferred_element_type=jnp.float32))
        pieces = rounded(projected).reshape(window_rows, HEADS, 4, head_size)
        raw_scores = jnp.einsum('ihd,jhd->hij', pieces[:, :, 2], pieces[:, :, 3]) * head_size ** (-0.5)
        allowed = causal & (position[None, :] < length)
        weights = rounded(jnp.where(allowed[None], jax.nn.silu(raw_scores) / window_rows, 0.0))
        attended = jnp.einsum('hij,jhd->ihd', weights, pieces[:, :, 1]).reshape(window_rows, D)
        gated_rows = (norm_rows(attended) * pieces[:, :, 0].reshape(window_rows, D)).astype(jnp.bfloat16)
        mixed_rows = jnp.dot(gated_rows, w_out, preferred_element_type=jnp.float32) + widened
        return mixed_rows.astype(jnp.bfloat16)
    outputs = lax.map(one_user, (device_ids, flat_len, flat_start))
    targets = ((flat_owner * BLK_DEV + flat_offset) * BLOCK)[:, None] + position[None, :]
    targets = jnp.where(position[None, :] < flat_len[:, None], targets, total_rows).astype(jnp.int32)
    packed = jnp.zeros((total_rows + 1, D), jnp.bfloat16)
    packed = packed.at[targets.reshape(-1)].set(outputs.reshape(-1, D))[:total_rows]
    user_state = outputs[jnp.arange(device_count * user_count, dtype=jnp.int32), flat_len - 1]
    return (packed, user_state)
```

```python
import jax
import jax.numpy as jnp
from jax import lax
from jax.experimental import pallas as pl
from jax.experimental.pallas import tpu as pltpu
from jax.sharding import PartitionSpec as P

D = 512
HEADS = 4
HEAD = D // HEADS
BLOCK = 128
MAXB = 2
BLK_DEV = 48
USERS = 24
N_DP = 64
N_MP = 4
WIN = MAXB * BLOCK
MINE = USERS // N_MP
TILE = 8
GROUPS = WIN // TILE
HALVES = N_DP // GROUPS
PER_HALF = MINE // HALVES
EPS = 1e-05
BF16 = jnp.bfloat16
F32 = jnp.float32


def silu(v):
    half = v * 0.5
    return half + half * jnp.tanh(half)


def norm_stats(total, squares):
    mean = total * (1.0 / D)
    var = squares * (1.0 / D) - mean * mean
    return mean, lax.rsqrt(var + EPS)


def user_rows(x_bf, length, w_in, w_out):
    x = x_bf.astype(F32)
    mean, inv = norm_stats(
        jnp.sum(x, axis=1, keepdims=True), jnp.sum(x * x, axis=1, keepdims=True)
    )
    normed = ((x - mean) * inv).astype(BF16)
    row = lax.broadcasted_iota(jnp.int32, (BLOCK, BLOCK), 0)
    col = lax.broadcasted_iota(jnp.int32, (BLOCK, BLOCK), 1)
    causal = col <= row
    scale = HEAD ** (-0.5)
    contract_last = (((1,), (1,)), ((), ()))
    heads, gates = [], []
    for h in range(HEADS):
        proj = silu(jnp.dot(normed, w_in[h], preferred_element_type=F32)).astype(BF16)
        gates.append(proj[:, :HEAD])
        v = proj[:, HEAD : 2 * HEAD]
        q = proj[:, 2 * HEAD : 3 * HEAD]
        k = proj[:, 3 * HEAD :]
        s0 = lax.dot_general(q[:BLOCK], k[:BLOCK], contract_last, preferred_element_type=F32)
        s1 = lax.dot_general(q[BLOCK:], k, contract_last, preferred_element_type=F32)
        a0 = jnp.where(causal, silu(s0 * scale) * (1.0 / WIN), 0.0).astype(BF16)
        b = silu(s1 * scale) * (1.0 / WIN)
        a1 = jnp.concatenate(
            [b[:, :BLOCK].astype(BF16), jnp.where(causal, b[:, BLOCK:], 0.0).astype(BF16)], axis=1
        )
        heads.append(
            jnp.concatenate(
                [
                    jnp.dot(a0, v[:BLOCK], preferred_element_type=F32),
                    jnp.dot(a1, v, preferred_element_type=F32),
                ],
                axis=0,
            )
        )
    total = sum(jnp.sum(a, axis=1, keepdims=True) for a in heads)
    squares = sum(jnp.sum(a * a, axis=1, keepdims=True) for a in heads)
    mean, inv = norm_stats(total, squares)
    gated = jnp.concatenate(
        [((a - mean) * inv * g.astype(F32)).astype(BF16) for a, g in zip(heads, gates)], axis=1
    )
    mixed = jnp.dot(gated, w_out, preferred_element_type=F32) + x
    at = lax.broadcasted_iota(jnp.int32, (WIN, 1), 0)
    return jnp.where(at < length, mixed, 0.0)


def layer_kernel(start_ref, len_ref, x0_ref, x1_ref, w_ref, w_out_ref, out_ref, state_ref):
    i = pl.program_id(0)
    length = len_ref[i]
    x = jnp.concatenate([x0_ref[...], x1_ref[...]], axis=0)
    mixed = user_rows(x, length, w_ref, w_out_ref[...])
    out_ref[...] = mixed.astype(BF16).reshape(1, GROUPS, 1, TILE, D)
    at = lax.broadcasted_iota(jnp.int32, (WIN, 1), 0)
    last = jnp.sum(jnp.where(at == length - 1, mixed, 0.0), axis=0, keepdims=True)
    state_ref[...] = last.astype(BF16).reshape(1, 1, D)


def layer(tokens, starts, lengths, w_in, w_out):
    return pl.pallas_call(
        layer_kernel,
        grid_spec=pltpu.PrefetchScalarGridSpec(
            num_scalar_prefetch=2,
            grid=(MINE,),
            in_specs=[
                pl.BlockSpec((BLOCK, D), lambda i, s, n: (s[i], 0)),
                pl.BlockSpec((BLOCK, D), lambda i, s, n: (jnp.minimum(s[i] + 1, BLK_DEV - 1), 0)),
                pl.BlockSpec((HEADS, D, D), lambda i, s, n: (0, 0, 0)),
                pl.BlockSpec((D, D), lambda i, s, n: (0, 0)),
            ],
            out_specs=[
                pl.BlockSpec(
                    (1, GROUPS, 1, TILE, D),
                    lambda i, s, n: (i // PER_HALF, 0, i % PER_HALF, 0, 0),
                ),
                pl.BlockSpec((1, 1, D), lambda i, s, n: (i, 0, 0)),
            ],
        ),
        out_shape=[
            jax.ShapeDtypeStruct((HALVES, GROUPS, PER_HALF, TILE, D), BF16),
            jax.ShapeDtypeStruct((MINE, 1, D), BF16),
        ],
        name="layer",
    )(starts, lengths, tokens, tokens, w_in, w_out)


def regroup_kernel(src_ref, in_ref, out_ref):
    for k in range(PER_HALF):

        def one(o, carry):
            rows = in_ref[src_ref[k * N_DP + o], k]
            for q in range(N_MP):
                out_ref[o, q, k] = rows[:, q * HEAD : (q + 1) * HEAD]
            return carry

        lax.fori_loop(0, N_DP, one, 0, unroll=8)


def regroup(spread, src):
    return pl.pallas_call(
        regroup_kernel,
        grid_spec=pltpu.PrefetchScalarGridSpec(
            num_scalar_prefetch=1,
            grid=(1,),
            in_specs=[pl.BlockSpec((N_DP, PER_HALF, TILE, D), lambda i, s: (0, 0, 0, 0))],
            out_specs=pl.BlockSpec(
                (N_DP, N_MP, PER_HALF, TILE, HEAD), lambda i, s: (0, 0, 0, 0, 0)
            ),
        ),
        out_shape=jax.ShapeDtypeStruct((N_DP, N_MP, PER_HALF, TILE, HEAD), BF16),
        name="regroup",
    )(src, spread)


def place_kernel(len_ref, off_ref, in_ref, out_ref):
    zeros = jnp.zeros((BLOCK, HEAD), BF16)

    def clear(b, carry):
        out_ref[pl.ds(pl.multiple_of(b * BLOCK, BLOCK), BLOCK), :] = zeros
        return carry

    lax.fori_loop(0, BLK_DEV, clear, 0)
    half_groups = BLOCK // TILE

    def one(u, carry):
        m = u // MINE
        half = (u % MINE) // PER_HALF
        k = u % PER_HALF
        base = off_ref[u] * BLOCK

        def block(first):
            for g in range(first, first + half_groups):
                at = pl.multiple_of(base + g * TILE, TILE)
                out_ref[pl.ds(at, TILE), :] = in_ref[half, g, m, k]

        block(0)

        @pl.when(len_ref[u] > BLOCK)
        def _():
            block(half_groups)

        return carry

    lax.fori_loop(0, USERS, one, 0)


def place(arrived, lengths, offsets):
    return pl.pallas_call(
        place_kernel,
        grid_spec=pltpu.PrefetchScalarGridSpec(
            num_scalar_prefetch=2,
            grid=(1,),
            in_specs=[
                pl.BlockSpec(
                    (HALVES, GROUPS, N_MP, PER_HALF, TILE, HEAD),
                    lambda i, a, b: (0, 0, 0, 0, 0, 0),
                )
            ],
            out_specs=pl.BlockSpec((BLK_DEV * BLOCK, HEAD), lambda i, a, b: (0, 0)),
        ),
        out_shape=jax.ShapeDtypeStruct((BLK_DEV * BLOCK, HEAD), BF16),
        name="place",
    )(lengths, offsets, arrived)


def per_device(tokens, w_uvqk, w_out, hist_len, owner, recv_offset, block_start):
    me = lax.axis_index("dp")
    part = lax.axis_index("mp")
    first = part * MINE

    w_all = lax.all_to_all(
        jnp.broadcast_to(w_uvqk[None], (N_MP, D, D)), "mp", 0, 0, tiled=True
    )
    row = jnp.concatenate([owner, hist_len, recv_offset, jnp.zeros((1, 56), jnp.int32)], axis=1)
    table = lax.all_to_all(
        jnp.broadcast_to(row[None], (N_DP, 1, 128)), "dp", 0, 0, tiled=True
    ).reshape(N_DP, 128)

    starts = lax.dynamic_slice_in_dim(block_start[0], first, MINE, 0)
    lengths = lax.dynamic_slice_in_dim(hist_len[0], first, MINE, 0)
    mixed, last = layer(tokens, starts, lengths, w_all, w_out)

    spread = lax.all_to_all(mixed.reshape(N_DP, PER_HALF * TILE, D), "dp", 0, 0, tiled=True)

    owners = table[:, :USERS]
    ids = jnp.arange(N_DP, dtype=jnp.int32)
    held = lax.dynamic_slice_in_dim(owners, first + (me // GROUPS) * PER_HALF, PER_HALF, 1)
    src = jnp.sum(
        jnp.where(held.T[:, None, :] == ids[None, :, None], ids[None, None, :], 0), axis=2
    ).reshape(-1)
    sorted_rows = regroup(spread.reshape(N_DP, PER_HALF, TILE, D), src)
    arrived = lax.all_to_all(
        sorted_rows.reshape(N_DP * N_MP, PER_HALF * TILE, HEAD), ("dp", "mp"), 0, 0, tiled=True
    )
    mine = owners == me
    recv_len = jnp.sum(jnp.where(mine, table[:, USERS : 2 * USERS], 0), axis=0)
    recv_off = jnp.sum(jnp.where(mine, table[:, 2 * USERS : 3 * USERS], 0), axis=0)
    packed = place(
        arrived.reshape(HALVES, GROUPS, N_MP, PER_HALF, TILE, HEAD), recv_len, recv_off
    )

    columns = last.reshape(MINE, N_MP, HEAD)
    state = jnp.zeros((N_MP, MINE, HEAD), BF16)
    for s in range(N_MP):
        to = (part + s) % N_MP
        piece = lax.dynamic_slice_in_dim(columns, to, 1, 1)[:, 0]
        if s:
            piece = lax.ppermute(piece, "mp", [(i, (i + s) % N_MP) for i in range(N_MP)])
        state = lax.dynamic_update_slice_in_dim(state, piece[None], (part - s) % N_MP, 0)
    return packed, state.reshape(USERS, HEAD)


def solution(mesh):
    in_specs = (
        P("dp", None),
        P(None, "mp"),
        P(),
        P("dp", None),
        P("dp", None),
        P("dp", None),
        P("dp", None),
    )
    out_specs = (P("dp", "mp"), P("dp", "mp"))
    return jax.shard_map(
        per_device, mesh=mesh, in_specs=in_specs, out_specs=out_specs, check_vma=False
    )
```

```python
import jax
import jax.numpy as jnp
from jax import lax
from jax.experimental import pallas as pl
from jax.experimental.pallas import tpu as pltpu
from jax.sharding import PartitionSpec as P

D = 512
HEADS = 4
HEAD = D // HEADS
BLOCK = 128
MAXB = 2
BLK_DEV = 48
USERS = 24
N_DP = 64
N_MP = 4
WIN = MAXB * BLOCK
MINE = USERS // N_MP
TILE = 8
GROUPS = WIN // TILE
HALVES = N_DP // GROUPS
PER_HALF = MINE // HALVES
EPS = 1e-05
BF16 = jnp.bfloat16
F32 = jnp.float32


def silu(v):
    half = v * 0.5
    return half + half * jnp.tanh(half)


def norm_stats(total, squares):
    mean = total * (1.0 / D)
    var = squares * (1.0 / D) - mean * mean
    return mean, lax.rsqrt(var + EPS)


def silu_gate(normed_parts, w_parts):
    acc = jnp.dot(normed_parts[0], w_parts[0], preferred_element_type=F32)
    for n, w in zip(normed_parts[1:], w_parts[1:]):
        acc = acc + jnp.dot(n, w, preferred_element_type=F32)
    proj = silu(acc).astype(BF16)
    return [proj[:, j * HEAD : (j + 1) * HEAD] for j in range(4)]


def attend(q, k, v):
    row = lax.broadcasted_iota(jnp.int32, (BLOCK, BLOCK), 0)
    col = lax.broadcasted_iota(jnp.int32, (BLOCK, BLOCK), 1)
    causal = col <= row
    scale = HEAD ** (-0.5)
    contract_last = (((1,), (1,)), ((), ()))
    s0 = lax.dot_general(q[:BLOCK], k[:BLOCK], contract_last, preferred_element_type=F32)
    s1 = lax.dot_general(q[BLOCK:], k, contract_last, preferred_element_type=F32)
    a0 = jnp.where(causal, silu(s0 * scale) * (1.0 / WIN), 0.0).astype(BF16)
    b = silu(s1 * scale) * (1.0 / WIN)
    a1 = jnp.concatenate(
        [b[:, :BLOCK].astype(BF16), jnp.where(causal, b[:, BLOCK:], 0.0).astype(BF16)], axis=1
    )
    return jnp.concatenate(
        [
            jnp.dot(a0, v[:BLOCK], preferred_element_type=F32),
            jnp.dot(a1, v, preferred_element_type=F32),
        ],
        axis=0,
    )


def own_head_kernel(start_ref, x0_ref, x1_ref, w_ref, normed_ref, att_ref, gate_ref):
    x = jnp.concatenate([x0_ref[...], x1_ref[...]], axis=0).astype(F32)
    mean, inv = norm_stats(
        jnp.sum(x, axis=1, keepdims=True), jnp.sum(x * x, axis=1, keepdims=True)
    )
    normed = ((x - mean) * inv).astype(BF16)
    normed_ref[0] = normed
    u, v, q, k = silu_gate([normed], [w_ref[...]])
    gate_ref[0] = u
    att_ref[0] = attend(q, k, v)


def window_specs():
    return [
        pl.BlockSpec((BLOCK, D), lambda i, s, *_: (s[i], 0)),
        pl.BlockSpec((BLOCK, D), lambda i, s, *_: (jnp.minimum(s[i] + 1, BLK_DEV - 1), 0)),
    ]


def own_head(tokens, starts, w_own):
    def per_user(width):
        return pl.BlockSpec((1, WIN, width), lambda i, s: (i, 0, 0))

    return pl.pallas_call(
        own_head_kernel,
        grid_spec=pltpu.PrefetchScalarGridSpec(
            num_scalar_prefetch=1,
            grid=(MINE,),
            in_specs=window_specs() + [pl.BlockSpec((D, D), lambda i, s: (0, 0))],
            out_specs=[per_user(D), per_user(HEAD), per_user(HEAD)],
        ),
        out_shape=[
            jax.ShapeDtypeStruct((MINE, WIN, D), BF16),
            jax.ShapeDtypeStruct((MINE, WIN, HEAD), F32),
            jax.ShapeDtypeStruct((MINE, WIN, HEAD), BF16),
        ],
        cost_estimate=pl.CostEstimate(
            flops=MINE * WIN * D * D * 64, bytes_accessed=MINE * WIN * D * 8, transcendentals=0
        ),
        name="own_head",
    )(starts, tokens, tokens, w_own)


def layer_kernel(
    start_ref, len_ref, pos_ref,
    x0_ref, x1_ref, normed_ref, att_ref, gate_ref, near_ref, far_ref, w_out_ref,
    out_ref, state_ref,
):
    i = pl.program_id(0)
    length = len_ref[i]
    part = pos_ref[0]
    low_is_near = pos_ref[1] == 0
    half = D // 2
    low = normed_ref[0, :, :half]
    high = normed_ref[0, :, half:]
    parts = [jnp.where(low_is_near, low, high), jnp.where(low_is_near, high, low)]
    order = [part] + [(part + s) % HEADS for s in range(1, HEADS)]
    heads, gates = [att_ref[0]], [gate_ref[0]]
    for h in order[1:]:
        u, v, q, k = silu_gate(parts, [near_ref[h], far_ref[h]])
        gates.append(u)
        heads.append(attend(q, k, v))
    total = sum(jnp.sum(a, axis=1, keepdims=True) for a in heads)
    squares = sum(jnp.sum(a * a, axis=1, keepdims=True) for a in heads)
    mean, inv = norm_stats(total, squares)
    x = jnp.concatenate([x0_ref[...], x1_ref[...]], axis=0).astype(F32)
    mixed = x
    for h, a, g in zip(order, heads, gates):
        gated = ((a - mean) * inv * g.astype(F32)).astype(BF16)
        rows = w_out_ref[pl.ds(pl.multiple_of(h * HEAD, HEAD), HEAD), :]
        mixed = mixed + jnp.dot(gated, rows, preferred_element_type=F32)
    at = lax.broadcasted_iota(jnp.int32, (WIN, 1), 0)
    mixed = jnp.where(at < length, mixed, 0.0)
    out_ref[...] = mixed.astype(BF16).reshape(1, GROUPS, 1, TILE, D)
    last = jnp.sum(jnp.where(at == length - 1, mixed, 0.0), axis=0, keepdims=True)
    state_ref[...] = last.astype(BF16).reshape(1, 1, D)


def layer(tokens, starts, lengths, position, normed, att, gate, near, far, w_out):
    def per_user(width):
        return pl.BlockSpec((1, WIN, width), lambda i, *_: (i, 0, 0))

    weights = pl.BlockSpec(memory_space=pltpu.VMEM)
    near, far = (pltpu.with_memory_space_constraint(w, pltpu.VMEM) for w in (near, far))
    return pl.pallas_call(
        layer_kernel,
        grid_spec=pltpu.PrefetchScalarGridSpec(
            num_scalar_prefetch=3,
            grid=(MINE,),
            in_specs=window_specs()
            + [
                per_user(D),
                per_user(HEAD),
                per_user(HEAD),
                weights,
                weights,
                pl.BlockSpec((D, D), lambda i, *_: (0, 0)),
            ],
            out_specs=[
                pl.BlockSpec(
                    (1, GROUPS, 1, TILE, D),
                    lambda i, *_: (i // PER_HALF, 0, i % PER_HALF, 0, 0),
                ),
                pl.BlockSpec((1, 1, D), lambda i, *_: (i, 0, 0)),
            ],
        ),
        out_shape=[
            jax.ShapeDtypeStruct((HALVES, GROUPS, PER_HALF, TILE, D), BF16),
            jax.ShapeDtypeStruct((MINE, 1, D), BF16),
        ],
        name="layer",
    )(starts, lengths, position, tokens, tokens, normed, att, gate, near, far, w_out)


def regroup_kernel(src_ref, in_ref, out_ref):
    for k in range(PER_HALF):

        def one(o, carry):
            rows = in_ref[src_ref[k * N_DP + o], k]
            for q in range(N_MP):
                out_ref[o, q, k] = rows[:, q * HEAD : (q + 1) * HEAD]
            return carry

        lax.fori_loop(0, N_DP, one, 0, unroll=8)


def regroup(spread, src):
    return pl.pallas_call(
        regroup_kernel,
        grid_spec=pltpu.PrefetchScalarGridSpec(
            num_scalar_prefetch=1,
            grid=(1,),
            in_specs=[pl.BlockSpec(memory_space=pltpu.VMEM)],
            out_specs=pl.BlockSpec(
                (N_DP, N_MP, PER_HALF, TILE, HEAD), lambda i, s: (0, 0, 0, 0, 0)
            ),
        ),
        out_shape=jax.ShapeDtypeStruct((N_DP, N_MP, PER_HALF, TILE, HEAD), BF16),
        name="regroup",
    )(src, pltpu.with_memory_space_constraint(spread, pltpu.VMEM))


def place_kernel(len_ref, off_ref, in_ref, out_ref):
    zeros = jnp.zeros((BLOCK, HEAD), BF16)

    def clear(b, carry):
        out_ref[pl.ds(pl.multiple_of(b * BLOCK, BLOCK), BLOCK), :] = zeros
        return carry

    lax.fori_loop(0, BLK_DEV, clear, 0)
    half_groups = BLOCK // TILE

    def one(u, carry):
        m = u // MINE
        half = (u % MINE) // PER_HALF
        k = u % PER_HALF
        base = off_ref[u] * BLOCK

        def block(first):
            for g in range(first, first + half_groups):
                at = pl.multiple_of(base + g * TILE, TILE)
                out_ref[pl.ds(at, TILE), :] = in_ref[half, g, m, k]

        block(0)

        @pl.when(len_ref[u] > BLOCK)
        def _():
            block(half_groups)

        return carry

    lax.fori_loop(0, USERS, one, 0)


def place(arrived, lengths, offsets):
    return pl.pallas_call(
        place_kernel,
        grid_spec=pltpu.PrefetchScalarGridSpec(
            num_scalar_prefetch=2,
            grid=(1,),
            in_specs=[pl.BlockSpec(memory_space=pltpu.VMEM)],
            out_specs=pl.BlockSpec((BLK_DEV * BLOCK, HEAD), lambda i, a, b: (0, 0)),
        ),
        out_shape=jax.ShapeDtypeStruct((BLK_DEV * BLOCK, HEAD), BF16),
        name="place",
    )(lengths, offsets, pltpu.with_memory_space_constraint(arrived, pltpu.VMEM))


def per_device(tokens, w_uvqk, w_out, hist_len, owner, recv_offset, block_start):
    me = lax.axis_index("dp")
    part = lax.axis_index("mp")
    first = part * MINE

    core = me % 2
    half = D // 2
    mine_rows = lax.dynamic_slice_in_dim(w_uvqk, core * half, half, 0)
    near = lax.all_to_all(
        jnp.broadcast_to(mine_rows[None], (N_MP, half, D)), "mp", 0, 0, tiled=True
    )
    far = lax.ppermute(near, "dp", [(i, i ^ 1) for i in range(N_DP)])
    table = jnp.concatenate([owner, hist_len, recv_offset, jnp.zeros((1, 56), jnp.int32)], axis=1)
    step = 1
    while step < N_DP:
        other = lax.ppermute(table, "dp", [(i, i ^ step) for i in range(N_DP)])
        ahead = (me // step) % 2 == 1
        table = jnp.concatenate(
            [jnp.where(ahead, other, table), jnp.where(ahead, table, other)], axis=0
        )
        step *= 2

    starts = lax.dynamic_slice_in_dim(block_start[0], first, MINE, 0)
    lengths = lax.dynamic_slice_in_dim(hist_len[0], first, MINE, 0)
    normed, att, gate = own_head(tokens, starts, w_uvqk)
    mixed, last = layer(
        tokens, starts, lengths, jnp.stack([part, core]), normed, att, gate, near, far, w_out
    )

    spread = lax.all_to_all(mixed.reshape(N_DP, PER_HALF * TILE, D), "dp", 0, 0, tiled=True)

    owners = table[:, :USERS]
    ids = jnp.arange(N_DP, dtype=jnp.int32)
    held = lax.dynamic_slice_in_dim(owners, first + (me // GROUPS) * PER_HALF, PER_HALF, 1)
    src = jnp.sum(
        jnp.where(held.T[:, None, :] == ids[None, :, None], ids[None, None, :], 0), axis=2
    ).reshape(-1)
    sorted_rows = regroup(spread.reshape(N_DP, PER_HALF, TILE, D), src)
    arrived = lax.all_to_all(
        sorted_rows.reshape(N_DP * N_MP, PER_HALF * TILE, HEAD), ("dp", "mp"), 0, 0, tiled=True
    )
    mine = owners == me
    recv_len = jnp.sum(jnp.where(mine, table[:, USERS : 2 * USERS], 0), axis=0)
    recv_off = jnp.sum(jnp.where(mine, table[:, 2 * USERS : 3 * USERS], 0), axis=0)
    packed = place(
        arrived.reshape(HALVES, GROUPS, N_MP, PER_HALF, TILE, HEAD), recv_len, recv_off
    )

    columns = last.reshape(MINE, N_MP, HEAD)
    state = jnp.zeros((N_MP, MINE, HEAD), BF16)
    for s in range(N_MP):
        to = (part + s) % N_MP
        piece = lax.dynamic_slice_in_dim(columns, to, 1, 1)[:, 0]
        if s:
            piece = lax.ppermute(piece, "mp", [(i, (i + s) % N_MP) for i in range(N_MP)])
        state = lax.dynamic_update_slice_in_dim(state, piece[None], (part - s) % N_MP, 0)
    return packed, state.reshape(USERS, HEAD)


def solution(mesh):
    in_specs = (
        P("dp", None),
        P(None, "mp"),
        P(),
        P("dp", None),
        P("dp", None),
        P("dp", None),
        P("dp", None),
    )
    out_specs = (P("dp", "mp"), P("dp", "mp"))
    return jax.shard_map(
        per_device, mesh=mesh, in_specs=in_specs, out_specs=out_specs, check_vma=False
    )
```

```python
import jax
import jax.numpy as jnp
from jax import lax
from jax.experimental import pallas as pl
from jax.experimental.pallas import tpu as pltpu
from jax.sharding import PartitionSpec as P

D = 512
HEADS = 4
HEAD = D // HEADS
BLOCK = 128
MAXB = 2
BLK_DEV = 48
USERS = 24
N_DP = 64
N_MP = 4
WIN = MAXB * BLOCK
MINE = USERS // N_MP
TILE = 8
GROUPS = WIN // TILE
HALVES = N_DP // GROUPS
PER_HALF = MINE // HALVES
MSG = PER_HALF * N_MP + 1
EPS = 1e-05
BF16 = jnp.bfloat16
F32 = jnp.float32


def silu_of_twice(h):
    return h + h * jnp.tanh(h)


def project(half_parts, w_parts):
    acc = jnp.dot(half_parts[0], w_parts[0], preferred_element_type=F32)
    for n, w in zip(half_parts[1:], w_parts[1:]):
        acc = acc + jnp.dot(n, w, preferred_element_type=F32)
    proj = silu_of_twice(acc).astype(BF16)
    return [proj[:, j * HEAD : (j + 1) * HEAD] for j in range(4)]


def attend(q, k, v):
    row = lax.broadcasted_iota(jnp.int32, (BLOCK, BLOCK), 0)
    col = lax.broadcasted_iota(jnp.int32, (BLOCK, BLOCK), 1)
    causal = col <= row
    scale = 0.5 * HEAD ** (-0.5)
    contract_last = (((1,), (1,)), ((), ()))
    s0 = lax.dot_general(q[:BLOCK], k[:BLOCK], contract_last, preferred_element_type=F32)
    s1 = lax.dot_general(q[BLOCK:], k, contract_last, preferred_element_type=F32)
    a0 = jnp.where(causal, silu_of_twice(s0 * scale), 0.0).astype(BF16)
    b = silu_of_twice(s1 * scale)
    a1 = jnp.concatenate(
        [b[:, :BLOCK].astype(BF16), jnp.where(causal, b[:, BLOCK:], 0.0).astype(BF16)], axis=1
    )
    return jnp.concatenate(
        [
            jnp.dot(a0, v[:BLOCK], preferred_element_type=F32),
            jnp.dot(a1, v, preferred_element_type=F32),
        ],
        axis=0,
    )


def norm_stats(total, squares, unit=1.0):
    mean = total * (1.0 / D)
    var = squares * (1.0 / D) - mean * mean
    return mean, lax.rsqrt(var * (unit * unit) + EPS) * unit


def own_head_kernel(start_ref, x0_ref, x1_ref, w_ref, half_ref, att_ref, gate_ref):
    x = jnp.concatenate([x0_ref[...], x1_ref[...]], axis=0).astype(F32)
    mean, inv = norm_stats(
        jnp.sum(x, axis=1, keepdims=True), jnp.sum(x * x, axis=1, keepdims=True)
    )
    half = ((x - mean) * (inv * 0.5)).astype(BF16)
    half_ref[0] = half
    u, v, q, k = project([half], [w_ref[...]])
    gate_ref[0] = u
    att_ref[0] = attend(q, k, v)


def window_specs():
    return [
        pl.BlockSpec((BLOCK, D), lambda i, s, *_: (s[i], 0)),
        pl.BlockSpec((BLOCK, D), lambda i, s, *_: (jnp.minimum(s[i] + 1, BLK_DEV - 1), 0)),
    ]


def own_head(tokens, starts, w_own):
    def per_user(width):
        return pl.BlockSpec((1, WIN, width), lambda i, s: (i, 0, 0))

    return pl.pallas_call(
        own_head_kernel,
        grid_spec=pltpu.PrefetchScalarGridSpec(
            num_scalar_prefetch=1,
            grid=(MINE,),
            in_specs=window_specs() + [pl.BlockSpec((D, D), lambda i, s: (0, 0))],
            out_specs=[per_user(D), per_user(HEAD), per_user(HEAD)],
        ),
        out_shape=[
            jax.ShapeDtypeStruct((MINE, WIN, D), BF16),
            jax.ShapeDtypeStruct((MINE, WIN, HEAD), F32),
            jax.ShapeDtypeStruct((MINE, WIN, HEAD), BF16),
        ],
        cost_estimate=pl.CostEstimate(
            flops=MINE * WIN * D * D * 64, bytes_accessed=MINE * WIN * D * 8, transcendentals=0
        ),
        name="own_head",
    )(starts, tokens, tokens, w_own)


def layer_kernel(
    start_ref, len_ref, pos_ref,
    x0_ref, x1_ref, half_ref, att_ref, gate_ref, near_ref, far_ref, w_out_ref, table_ref,
    out_ref, state_ref, w_out_s,
):
    i = pl.program_id(0)
    k_user = i % PER_HALF
    length = len_ref[i]
    part = pos_ref[0]
    low_is_near = pos_ref[1] == 0
    order = [part] + [(part + s) % HEADS for s in range(1, HEADS)]

    @pl.when(i == 0)
    def _():
        for s, h in enumerate(order):
            w_out_s[s * HEAD : (s + 1) * HEAD, :] = w_out_ref[
                pl.ds(pl.multiple_of(h * HEAD, HEAD), HEAD), :
            ]

    @pl.when(k_user == 0)
    def _():
        tile = jnp.broadcast_to(table_ref[...], (TILE, 128)).astype(F32).astype(BF16)
        out_ref[0, :, PER_HALF * N_MP] = jnp.broadcast_to(tile[None], (GROUPS, TILE, 128))

    low = half_ref[0, :, : D // 2]
    high = half_ref[0, :, D // 2 :]
    parts = [jnp.where(low_is_near, low, high), jnp.where(low_is_near, high, low)]
    heads, gates = [att_ref[0]], [gate_ref[0]]
    for h in order[1:]:
        u, v, q, k = project(parts, [near_ref[h], far_ref[h]])
        gates.append(u)
        heads.append(attend(q, k, v))
    total = jnp.sum(heads[0] + heads[1] + (heads[2] + heads[3]), axis=1, keepdims=True)
    squares = jnp.sum(
        heads[0] * heads[0] + heads[1] * heads[1] + (heads[2] * heads[2] + heads[3] * heads[3]),
        axis=1,
        keepdims=True,
    )
    mean, inv = norm_stats(total, squares, 1.0 / WIN)
    gated = jnp.concatenate(
        [((a - mean) * inv * g.astype(F32)).astype(BF16) for a, g in zip(heads, gates)], axis=1
    )
    x = jnp.concatenate([x0_ref[...], x1_ref[...]], axis=0).astype(F32)
    mixed = jnp.dot(gated, w_out_s[...], preferred_element_type=F32) + x
    at = lax.broadcasted_iota(jnp.int32, (WIN, 1), 0)
    mixed = jnp.where(at < length, mixed, 0.0).astype(BF16)
    for q in range(N_MP):
        out_ref[0, :, k_user * N_MP + q] = mixed[:, q * HEAD : (q + 1) * HEAD].reshape(
            GROUPS, TILE, HEAD
        )
    last = length - 1
    pick = lax.broadcasted_iota(jnp.int32, (TILE, HEAD), 0) == last % TILE
    for q in range(N_MP):
        tile = out_ref[0, last // TILE, k_user * N_MP + q].astype(F32)
        state_ref[0, :, q * HEAD : (q + 1) * HEAD] = jnp.sum(
            jnp.where(pick, tile, 0.0), axis=0, keepdims=True
        ).astype(BF16)


def layer(tokens, starts, lengths, position, half, att, gate, near, far, w_out, table):
    def per_user(width):
        return pl.BlockSpec((1, WIN, width), lambda i, *_: (i, 0, 0))

    weights = pl.BlockSpec(memory_space=pltpu.VMEM)
    near, far = (pltpu.with_memory_space_constraint(w, pltpu.VMEM) for w in (near, far))
    return pl.pallas_call(
        layer_kernel,
        grid_spec=pltpu.PrefetchScalarGridSpec(
            num_scalar_prefetch=3,
            grid=(MINE,),
            in_specs=window_specs()
            + [
                per_user(D),
                per_user(HEAD),
                per_user(HEAD),
                weights,
                weights,
                pl.BlockSpec((D, D), lambda i, *_: (0, 0)),
                pl.BlockSpec((1, 128), lambda i, *_: (0, 0)),
            ],
            out_specs=[
                pl.BlockSpec(
                    (1, GROUPS, MSG, TILE, HEAD), lambda i, *_: (i // PER_HALF, 0, 0, 0, 0)
                ),
                pl.BlockSpec((1, 1, D), lambda i, *_: (i, 0, 0)),
            ],
            scratch_shapes=[pltpu.VMEM((D, D), BF16)],
        ),
        out_shape=[
            jax.ShapeDtypeStruct((HALVES, GROUPS, MSG, TILE, HEAD), BF16),
            jax.ShapeDtypeStruct((MINE, 1, D), BF16),
        ],
        name="layer",
    )(starts, lengths, position, tokens, tokens, half, att, gate, near, far, w_out, table)


def regroup_kernel(first_ref, in_ref, out_ref, table_v, table_s, sem):
    table = jnp.max(in_ref[:, PER_HALF * N_MP].astype(F32), axis=1)
    table_v[...] = table.astype(jnp.int32)
    copy = pltpu.make_async_copy(table_v, table_s, sem)
    copy.start()
    copy.wait()
    first = first_ref[0]

    def one(d, carry):
        for k in range(PER_HALF):
            o = table_s[d, first + k]
            for q in range(N_MP):
                out_ref[o, q, k] = in_ref[d, k * N_MP + q]
        return carry

    lax.fori_loop(0, N_DP, one, 0, unroll=8)


def regroup(spread, first):
    return pl.pallas_call(
        regroup_kernel,
        grid_spec=pltpu.PrefetchScalarGridSpec(
            num_scalar_prefetch=1,
            grid=(1,),
            in_specs=[pl.BlockSpec(memory_space=pltpu.VMEM)],
            out_specs=pl.BlockSpec(
                (N_DP, N_MP, PER_HALF, TILE, HEAD), lambda i, s: (0, 0, 0, 0, 0)
            ),
            scratch_shapes=[
                pltpu.VMEM((N_DP, 128), jnp.int32),
                pltpu.SMEM((N_DP, 128), jnp.int32),
                pltpu.SemaphoreType.DMA,
            ],
        ),
        out_shape=jax.ShapeDtypeStruct((N_DP, N_MP, PER_HALF, TILE, HEAD), BF16),
        name="regroup",
    )(first, pltpu.with_memory_space_constraint(spread, pltpu.VMEM))


def place_kernel(len_ref, off_ref, in_ref, out_ref):
    zeros = jnp.zeros((BLOCK, HEAD), BF16)

    def clear(b, carry):
        out_ref[pl.ds(pl.multiple_of(b * BLOCK, BLOCK), BLOCK), :] = zeros
        return carry

    lax.fori_loop(0, BLK_DEV, clear, 0)
    half_groups = BLOCK // TILE

    def one(u, carry):
        m = u // MINE
        half = (u % MINE) // PER_HALF
        k = u % PER_HALF
        base = off_ref[u] * BLOCK

        def block(first):
            for g in range(first, first + half_groups):
                at = pl.multiple_of(base + g * TILE, TILE)
                out_ref[pl.ds(at, TILE), :] = in_ref[half, g, m, k]

        block(0)

        @pl.when(len_ref[u] > BLOCK)
        def _():
            block(half_groups)

        return carry

    lax.fori_loop(0, USERS, one, 0)


def place(arrived, lengths, offsets):
    return pl.pallas_call(
        place_kernel,
        grid_spec=pltpu.PrefetchScalarGridSpec(
            num_scalar_prefetch=2,
            grid=(1,),
            in_specs=[pl.BlockSpec(memory_space=pltpu.VMEM)],
            out_specs=pl.BlockSpec((BLK_DEV * BLOCK, HEAD), lambda i, a, b: (0, 0)),
        ),
        out_shape=jax.ShapeDtypeStruct((BLK_DEV * BLOCK, HEAD), BF16),
        name="place",
    )(lengths, offsets, pltpu.with_memory_space_constraint(arrived, pltpu.VMEM))


def per_device(tokens, w_uvqk, w_out, hist_len, owner, recv_offset, block_start):
    me = lax.axis_index("dp")
    part = lax.axis_index("mp")
    first = part * MINE

    core = me % 2
    half = D // 2
    mine_rows = lax.dynamic_slice_in_dim(w_uvqk, core * half, half, 0)
    near = lax.all_to_all(
        jnp.broadcast_to(mine_rows[None], (N_MP, half, D)), "mp", 0, 0, tiled=True
    )
    far = lax.ppermute(near, "dp", [(i, i ^ 1) for i in range(N_DP)])
    table = jnp.concatenate([owner, hist_len, recv_offset, jnp.zeros((1, 56), jnp.int32)], axis=1)
    starts = lax.dynamic_slice_in_dim(block_start[0], first, MINE, 0)
    lengths = lax.dynamic_slice_in_dim(hist_len[0], first, MINE, 0)
    normed, att, gate = own_head(tokens, starts, w_uvqk)
    mixed, last = layer(
        tokens, starts, lengths, jnp.stack([part, core]), normed, att, gate, near, far, w_out, table
    )

    spread = lax.all_to_all(
        mixed.reshape(N_DP, MSG * TILE, HEAD), "dp", 0, 0, tiled=True
    ).reshape(N_DP, MSG, TILE, HEAD)
    held = first + (me // GROUPS) * PER_HALF
    sorted_rows = regroup(spread, held[None])
    table = spread[:, MSG - 1, 0, :].astype(jnp.int32)
    owners = table[:, :USERS]
    arrived = lax.all_to_all(
        sorted_rows.reshape(N_DP * N_MP, PER_HALF * TILE, HEAD), ("dp", "mp"), 0, 0, tiled=True
    )
    mine = owners == me
    recv_len = jnp.sum(jnp.where(mine, table[:, USERS : 2 * USERS], 0), axis=0)
    recv_off = jnp.sum(jnp.where(mine, table[:, 2 * USERS : 3 * USERS], 0), axis=0)
    packed = place(
        arrived.reshape(HALVES, GROUPS, N_MP, PER_HALF, TILE, HEAD), recv_len, recv_off
    )

    columns = last.reshape(MINE, N_MP, HEAD)
    state = jnp.zeros((N_MP, MINE, HEAD), BF16)
    for s in range(N_MP):
        to = (part + s) % N_MP
        piece = lax.dynamic_slice_in_dim(columns, to, 1, 1)[:, 0]
        if s:
            piece = lax.ppermute(piece, "mp", [(i, (i + s) % N_MP) for i in range(N_MP)])
        state = lax.dynamic_update_slice_in_dim(state, piece[None], (part - s) % N_MP, 0)
    return packed, state.reshape(USERS, HEAD)


def solution(mesh):
    in_specs = (
        P("dp", None),
        P(None, "mp"),
        P(),
        P("dp", None),
        P("dp", None),
        P("dp", None),
        P("dp", None),
    )
    out_specs = (P("dp", "mp"), P("dp", "mp"))
    return jax.shard_map(
        per_device, mesh=mesh, in_specs=in_specs, out_specs=out_specs, check_vma=False
    )
```

```python
import jax
import jax.numpy as jnp
from jax import lax
from jax.experimental import pallas as pl
from jax.experimental.pallas import tpu as pltpu
from jax.sharding import PartitionSpec as P

D = 512
HEADS = 4
HEAD = D // HEADS
BLOCK = 128
MAXB = 2
BLK_DEV = 48
USERS = 24
N_DP = 64
N_MP = 4
WIN = MAXB * BLOCK
MINE = USERS // N_MP
TILE = 8
GROUPS = WIN // TILE
HALVES = N_DP // GROUPS
PER_HALF = MINE // HALVES
MSG = PER_HALF * N_MP + 1
EPS = 1e-05
BF16 = jnp.bfloat16
F32 = jnp.float32


def silu_of_twice(h):
    return h + h * jnp.tanh(h)


def project(half_parts, w_parts):
    acc = jnp.dot(half_parts[0], w_parts[0], preferred_element_type=F32)
    for n, w in zip(half_parts[1:], w_parts[1:]):
        acc = acc + jnp.dot(n, w, preferred_element_type=F32)
    proj = silu_of_twice(acc).astype(BF16)
    return [proj[:, j * HEAD : (j + 1) * HEAD] for j in range(4)]


def attend(q, k, v):
    row = lax.broadcasted_iota(jnp.int32, (BLOCK, BLOCK), 0)
    col = lax.broadcasted_iota(jnp.int32, (BLOCK, BLOCK), 1)
    causal = col <= row
    scale = 0.5 * HEAD ** (-0.5)
    contract_last = (((1,), (1,)), ((), ()))
    s0 = lax.dot_general(q[:BLOCK], k[:BLOCK], contract_last, preferred_element_type=F32)
    s1 = lax.dot_general(q[BLOCK:], k, contract_last, preferred_element_type=F32)
    a0 = jnp.where(causal, silu_of_twice(s0 * scale), 0.0).astype(BF16)
    b = silu_of_twice(s1 * scale)
    a1 = jnp.concatenate(
        [b[:, :BLOCK].astype(BF16), jnp.where(causal, b[:, BLOCK:], 0.0).astype(BF16)], axis=1
    )
    return jnp.concatenate(
        [
            jnp.dot(a0, v[:BLOCK], preferred_element_type=F32),
            jnp.dot(a1, v, preferred_element_type=F32),
        ],
        axis=0,
    )


def norm_stats(total, squares, unit=1.0):
    mean = total * (1.0 / D)
    var = squares * (1.0 / D) - mean * mean
    return mean, lax.rsqrt(var * (unit * unit) + EPS) * unit


def in_vmem():
    return pl.BlockSpec(memory_space=pltpu.VMEM)


def in_hbm():
    return pl.BlockSpec(memory_space=pl.ANY)


def keep(array):
    return pltpu.with_memory_space_constraint(array, pltpu.VMEM)


def own_head_kernel(start_ref, x0_ref, x1_ref, w_ref, half_ref, att_ref, gate_ref):
    x = jnp.concatenate([x0_ref[...], x1_ref[...]], axis=0).astype(F32)
    mean, inv = norm_stats(
        jnp.sum(x, axis=1, keepdims=True), jnp.sum(x * x, axis=1, keepdims=True)
    )
    half = ((x - mean) * (inv * 0.5)).astype(BF16)
    half_ref[0] = half
    u, v, q, k = project([half], [w_ref[...]])
    gate_ref[0] = u
    att_ref[0] = attend(q, k, v)


def own_head(tokens, starts, w_own):
    def per_user(width):
        return pl.BlockSpec((1, WIN, width), lambda i, s: (i, 0, 0))

    return pl.pallas_call(
        own_head_kernel,
        grid_spec=pltpu.PrefetchScalarGridSpec(
            num_scalar_prefetch=1,
            grid=(MINE,),
            in_specs=[
                pl.BlockSpec((BLOCK, D), lambda i, s: (s[i], 0)),
                pl.BlockSpec((BLOCK, D), lambda i, s: (jnp.minimum(s[i] + 1, BLK_DEV - 1), 0)),
                pl.BlockSpec((D, D), lambda i, s: (0, 0)),
            ],
            out_specs=[per_user(D), per_user(HEAD), per_user(HEAD)],
        ),
        out_shape=[
            jax.ShapeDtypeStruct((MINE, WIN, D), BF16),
            jax.ShapeDtypeStruct((MINE, WIN, HEAD), F32),
            jax.ShapeDtypeStruct((MINE, WIN, HEAD), BF16),
        ],
        cost_estimate=pl.CostEstimate(
            flops=MINE * WIN * D * D * 64, bytes_accessed=MINE * WIN * D * 8, transcendentals=0
        ),
        name="own_head",
    )(starts, tokens, tokens, w_own)


def layer_kernel(
    start_ref, len_ref, pos_ref,
    tokens_ref, half_hbm, att_hbm, gate_hbm, near_ref, far_ref, w_out_ref, table_ref,
    out_ref, state_ref,
    x_s, half_s, att_s, gate_s, w_out_s, out_s, sem_in, sem_w, sem_out,
):
    part = pos_ref[0]
    low_is_near = pos_ref[1] == 0
    order = [part] + [(part + s) % HEADS for s in range(1, HEADS)]

    def loads(i):
        first = start_ref[i]
        second = jnp.minimum(first + 1, BLK_DEV - 1)
        pairs = [
            (half_hbm.at[i], half_s.at[i]),
            (att_hbm.at[i], att_s.at[i]),
            (gate_hbm.at[i], gate_s.at[i]),
            (tokens_ref.at[pl.ds(first * BLOCK, BLOCK)], x_s.at[i, pl.ds(0, BLOCK)]),
            (tokens_ref.at[pl.ds(second * BLOCK, BLOCK)], x_s.at[i, pl.ds(BLOCK, BLOCK)]),
        ]
        return [pltpu.make_async_copy(a, b, sem_in.at[i, j]) for j, (a, b) in enumerate(pairs)]

    weights = [
        pltpu.make_async_copy(
            w_out_ref.at[pl.ds(h * HEAD, HEAD)], w_out_s.at[pl.ds(s * HEAD, HEAD)], sem_w.at[s]
        )
        for s, h in enumerate(order)
    ]

    def sends(i):
        at = (i // PER_HALF, slice(None), pl.ds((i % PER_HALF) * N_MP, N_MP))
        return pltpu.make_async_copy(out_s.at[at], out_ref.at[at], sem_out.at[i])

    def send_table(half):
        at = (half, slice(None), pl.ds(MSG - 1, 1))
        return pltpu.make_async_copy(out_s.at[at], out_ref.at[at], sem_out.at[MINE + half])

    for copy in loads(0):
        copy.start()
    for i in range(1, MINE):
        for copy in loads(i):
            copy.start()
        if i == 1:
            for copy in weights:
                copy.start()
    tile = jnp.broadcast_to(table_ref[...], (TILE, 128)).astype(F32).astype(BF16)
    for half in range(HALVES):
        out_s[half, :, MSG - 1] = jnp.broadcast_to(tile[None], (GROUPS, TILE, 128))
        send_table(half).start()

    def user(i, carry):
        length = len_ref[i]
        half_id = i // PER_HALF
        base = (i % PER_HALF) * N_MP
        for copy in loads(i):
            copy.wait()
        low = half_s[i, :, : D // 2]
        high = half_s[i, :, D // 2 :]
        parts = [jnp.where(low_is_near, low, high), jnp.where(low_is_near, high, low)]
        heads, gates = [att_s[i]], [gate_s[i]]
        for h in order[1:]:
            u, v, q, k = project(parts, [near_ref[h], far_ref[h]])
            gates.append(u)
            heads.append(attend(q, k, v))
        total = jnp.sum(heads[0] + heads[1] + (heads[2] + heads[3]), axis=1, keepdims=True)
        squares = jnp.sum(
            heads[0] * heads[0] + heads[1] * heads[1] + (heads[2] * heads[2] + heads[3] * heads[3]),
            axis=1,
            keepdims=True,
        )
        mean, inv = norm_stats(total, squares, 1.0 / WIN)
        gated = jnp.concatenate(
            [((a - mean) * inv * g.astype(F32)).astype(BF16) for a, g in zip(heads, gates)], axis=1
        )

        @pl.when(i == 0)
        def _():
            for copy in weights:
                copy.wait()

        mixed = jnp.dot(gated, w_out_s[...], preferred_element_type=F32) + x_s[i].astype(F32)
        at = lax.broadcasted_iota(jnp.int32, (WIN, 1), 0)
        mixed = jnp.where(at < length, mixed, 0.0).astype(BF16)
        for q in range(N_MP):
            out_s[half_id, :, base + q] = mixed[:, q * HEAD : (q + 1) * HEAD].reshape(
                GROUPS, TILE, HEAD
            )
        sends(i).start()
        last = length - 1
        pick = lax.broadcasted_iota(jnp.int32, (TILE, HEAD), 0) == last % TILE
        for q in range(N_MP):
            tile = out_s[half_id, last // TILE, base + q].astype(F32)
            state_ref[i, :, q * HEAD : (q + 1) * HEAD] = jnp.sum(
                jnp.where(pick, tile, 0.0), axis=0, keepdims=True
            ).astype(BF16)
        return carry

    lax.fori_loop(0, MINE, user, 0)
    for half in range(HALVES):
        send_table(half).wait()
    for i in range(MINE):
        sends(i).wait()


def layer(tokens, starts, lengths, position, kept, near, far, w_out, table):
    message = (HALVES, GROUPS, MSG, TILE, HEAD)
    return pl.pallas_call(
        layer_kernel,
        grid_spec=pltpu.PrefetchScalarGridSpec(
            num_scalar_prefetch=3,
            grid=(1,),
            in_specs=[in_hbm()] * 4 + [in_vmem()] * 2 + [in_hbm(), in_vmem()],
            out_specs=[in_hbm(), in_vmem()],
            scratch_shapes=[
                pltpu.VMEM((MINE, WIN, D), BF16),
                pltpu.VMEM((MINE, WIN, D), BF16),
                pltpu.VMEM((MINE, WIN, HEAD), F32),
                pltpu.VMEM((MINE, WIN, HEAD), BF16),
                pltpu.VMEM((D, D), BF16),
                pltpu.VMEM(message, BF16),
                pltpu.SemaphoreType.DMA((MINE, 5)),
                pltpu.SemaphoreType.DMA((HEADS,)),
                pltpu.SemaphoreType.DMA((MINE + HALVES,)),
            ],
        ),
        out_shape=[
            jax.ShapeDtypeStruct(message, BF16),
            jax.ShapeDtypeStruct((MINE, 1, D), BF16),
        ],
        name="layer",
    )(starts, lengths, position, tokens, *kept, keep(near), keep(far), w_out, table)


def regroup_kernel(first_ref, in_ref, out_ref, table_v, table_s, sem):
    table = jnp.max(in_ref[:, PER_HALF * N_MP].astype(F32), axis=1)
    table_v[...] = table.astype(jnp.int32)
    copy = pltpu.make_async_copy(table_v, table_s, sem)
    copy.start()
    copy.wait()
    first = first_ref[0]

    def one(d, carry):
        for k in range(PER_HALF):
            o = table_s[d, first + k]
            for q in range(N_MP):
                out_ref[o, q, k] = in_ref[d, k * N_MP + q]
        return carry

    lax.fori_loop(0, N_DP, one, 0, unroll=8)


def regroup(spread, first):
    return pl.pallas_call(
        regroup_kernel,
        grid_spec=pltpu.PrefetchScalarGridSpec(
            num_scalar_prefetch=1,
            grid=(1,),
            in_specs=[in_vmem()],
            out_specs=pl.BlockSpec(
                (N_DP, N_MP, PER_HALF, TILE, HEAD), lambda i, s: (0, 0, 0, 0, 0)
            ),
            scratch_shapes=[
                pltpu.VMEM((N_DP, 128), jnp.int32),
                pltpu.SMEM((N_DP, 128), jnp.int32),
                pltpu.SemaphoreType.DMA,
            ],
        ),
        out_shape=jax.ShapeDtypeStruct((N_DP, N_MP, PER_HALF, TILE, HEAD), BF16),
        name="regroup",
    )(first, keep(spread))


def place_kernel(len_ref, off_ref, in_ref, out_ref, zero_v, used_s, sem):
    per_block = BLOCK // TILE
    zero_v[...] = jnp.zeros_like(zero_v)

    def clear(b, carry):
        used_s[b] = 0
        return carry

    lax.fori_loop(0, BLK_DEV, clear, 0, unroll=8)

    def send(u, j):
        half = (u % MINE) // PER_HALF
        block = off_ref[u] + j
        used_s[block] = 1
        pltpu.make_async_copy(
            in_ref.at[half, pl.ds(j * per_block, per_block), u // MINE, u % PER_HALF],
            out_ref.at[pl.ds(block * per_block, per_block)],
            sem,
        ).start()

    def one(u, carry):
        send(u, 0)

        @pl.when(len_ref[u] > BLOCK)
        def _():
            send(u, 1)

        return carry

    lax.fori_loop(0, USERS, one, 0)

    def fill(b, carry):
        @pl.when(used_s[b] == 0)
        def _():
            pltpu.make_async_copy(zero_v, out_ref.at[pl.ds(b * per_block, per_block)], sem).start()

        return carry

    lax.fori_loop(0, BLK_DEV, fill, 0)
    pltpu.make_async_copy(out_ref, out_ref, sem).wait()


def place(arrived, lengths, offsets):
    rows = BLK_DEV * BLOCK
    return pl.pallas_call(
        place_kernel,
        grid_spec=pltpu.PrefetchScalarGridSpec(
            num_scalar_prefetch=2,
            grid=(1,),
            in_specs=[in_vmem()],
            out_specs=in_hbm(),
            scratch_shapes=[
                pltpu.VMEM((BLOCK // TILE, TILE, HEAD), BF16),
                pltpu.SMEM((BLK_DEV,), jnp.int32),
                pltpu.SemaphoreType.DMA,
            ],
        ),
        out_shape=jax.ShapeDtypeStruct((rows // TILE, TILE, HEAD), BF16),
        name="place",
    )(lengths, offsets, keep(arrived)).reshape(rows, HEAD)


def per_device(tokens, w_uvqk, w_out, hist_len, owner, recv_offset, block_start):
    me = lax.axis_index("dp")
    part = lax.axis_index("mp")
    first = part * MINE

    core = me % 2
    half = D // 2
    mine_rows = jnp.where(core == 0, w_uvqk[:half], w_uvqk[half:])
    near = lax.all_to_all(
        jnp.broadcast_to(mine_rows[None], (N_MP, half, D)), "mp", 0, 0, tiled=True
    )
    far = lax.ppermute(near, "dp", [(i, i ^ 1) for i in range(N_DP)])
    table = jnp.concatenate([owner, hist_len, recv_offset, jnp.zeros((1, 56), jnp.int32)], axis=1)
    starts = lax.dynamic_slice_in_dim(block_start[0], first, MINE, 0)
    lengths = lax.dynamic_slice_in_dim(hist_len[0], first, MINE, 0)
    kept = own_head(tokens, starts, w_uvqk)
    mixed, last = layer(
        tokens, starts, lengths, jnp.stack([part, core]), kept, near, far, w_out, table
    )

    spread = lax.all_to_all(
        mixed.reshape(N_DP, MSG * TILE, HEAD), "dp", 0, 0, tiled=True
    ).reshape(N_DP, MSG, TILE, HEAD)
    held = first + (me // GROUPS) * PER_HALF
    sorted_rows = regroup(spread, held[None])
    table = spread[:, MSG - 1, 0, :].astype(jnp.int32)
    owners = table[:, :USERS]
    arrived = lax.all_to_all(
        sorted_rows.reshape(N_DP * N_MP, PER_HALF * TILE, HEAD), ("dp", "mp"), 0, 0, tiled=True
    )
    mine = owners == me
    recv_len = jnp.sum(jnp.where(mine, table[:, USERS : 2 * USERS], 0), axis=0)
    recv_off = jnp.sum(jnp.where(mine, table[:, 2 * USERS : 3 * USERS], 0), axis=0)
    packed = place(
        arrived.reshape(HALVES, GROUPS, N_MP, PER_HALF, TILE, HEAD), recv_len, recv_off
    )

    columns = last.reshape(MINE, N_MP, HEAD)
    state = jnp.zeros((N_MP, MINE, HEAD), BF16)
    for s in range(N_MP):
        to = (part + s) % N_MP
        piece = lax.dynamic_slice_in_dim(columns, to, 1, 1)[:, 0]
        if s:
            piece = lax.ppermute(piece, "mp", [(i, (i + s) % N_MP) for i in range(N_MP)])
        state = lax.dynamic_update_slice_in_dim(state, piece[None], (part - s) % N_MP, 0)
    return packed, state.reshape(USERS, HEAD)


def solution(mesh):
    in_specs = (
        P("dp", None),
        P(None, "mp"),
        P(),
        P("dp", None),
        P("dp", None),
        P("dp", None),
        P("dp", None),
    )
    out_specs = (P("dp", "mp"), P("dp", "mp"))
    return jax.shard_map(
        per_device, mesh=mesh, in_specs=in_specs, out_specs=out_specs, check_vma=False
    )
```

```python
import jax
import jax.numpy as jnp
from jax import lax
from jax.experimental import pallas as pl
from jax.experimental.pallas import tpu as pltpu
from jax.sharding import PartitionSpec as P

D = 512
HEADS = 4
HEAD = D // HEADS
BLOCK = 128
MAXB = 2
BLK_DEV = 48
USERS = 24
N_DP = 64
N_MP = 4
WIN = MAXB * BLOCK
MINE = USERS // N_MP
TILE = 8
GROUPS = WIN // TILE
HALVES = N_DP // GROUPS
PER_HALF = MINE // HALVES
MSG = PER_HALF * N_MP + 1
GROUP = 3
EPS = 1e-05
BF16 = jnp.bfloat16
F32 = jnp.float32


def silu_of_twice(h):
    return h + h * jnp.tanh(h)


def project(half_parts, w_parts):
    acc = jnp.dot(half_parts[0], w_parts[0], preferred_element_type=F32)
    for n, w in zip(half_parts[1:], w_parts[1:]):
        acc = acc + jnp.dot(n, w, preferred_element_type=F32)
    proj = silu_of_twice(acc).astype(BF16)
    return [proj[:, j * HEAD : (j + 1) * HEAD] for j in range(4)]


def attend(q, k, v):
    row = lax.broadcasted_iota(jnp.int32, (BLOCK, BLOCK), 0)
    col = lax.broadcasted_iota(jnp.int32, (BLOCK, BLOCK), 1)
    causal = col <= row
    scale = 0.5 * HEAD ** (-0.5)
    contract_last = (((1,), (1,)), ((), ()))
    s0 = lax.dot_general(q[:BLOCK], k[:BLOCK], contract_last, preferred_element_type=F32)
    s1 = lax.dot_general(q[BLOCK:], k, contract_last, preferred_element_type=F32)
    a0 = jnp.where(causal, silu_of_twice(s0 * scale), 0.0).astype(BF16)
    b = silu_of_twice(s1 * scale)
    a1 = jnp.concatenate(
        [b[:, :BLOCK].astype(BF16), jnp.where(causal, b[:, BLOCK:], 0.0).astype(BF16)], axis=1
    )
    return jnp.concatenate(
        [
            jnp.dot(a0, v[:BLOCK], preferred_element_type=F32),
            jnp.dot(a1, v, preferred_element_type=F32),
        ],
        axis=0,
    )


def norm_stats(total, squares, unit=1.0):
    mean = total * (1.0 / D)
    var = squares * (1.0 / D) - mean * mean
    return mean, lax.rsqrt(var * (unit * unit) + EPS) * unit


def in_vmem():
    return pl.BlockSpec(memory_space=pltpu.VMEM)


def in_hbm():
    return pl.BlockSpec(memory_space=pl.ANY)


def keep(array):
    return pltpu.with_memory_space_constraint(array, pltpu.VMEM)


def own_head_kernel(start_ref, x0_ref, x1_ref, w_ref, half_ref, att_ref, gate_ref):
    x = jnp.concatenate([x0_ref[...], x1_ref[...]], axis=0).astype(F32)
    mean, inv = norm_stats(
        jnp.sum(x, axis=1, keepdims=True), jnp.sum(x * x, axis=1, keepdims=True)
    )
    half = ((x - mean) * (inv * 0.5)).astype(BF16)
    half_ref[0] = half
    u, v, q, k = project([half], [w_ref[...]])
    gate_ref[0] = u
    att_ref[0] = attend(q, k, v)


def own_head(tokens, starts, w_own):
    def per_user(width):
        return pl.BlockSpec((1, WIN, width), lambda i, s: (i, 0, 0))

    return pl.pallas_call(
        own_head_kernel,
        grid_spec=pltpu.PrefetchScalarGridSpec(
            num_scalar_prefetch=1,
            grid=(MINE,),
            in_specs=[
                pl.BlockSpec((BLOCK, D), lambda i, s: (s[i], 0)),
                pl.BlockSpec((BLOCK, D), lambda i, s: (jnp.minimum(s[i] + 1, BLK_DEV - 1), 0)),
                pl.BlockSpec((D, D), lambda i, s: (0, 0)),
            ],
            out_specs=[per_user(D), per_user(HEAD), per_user(HEAD)],
        ),
        out_shape=[
            jax.ShapeDtypeStruct((MINE, WIN, D), BF16),
            jax.ShapeDtypeStruct((MINE, WIN, HEAD), F32),
            jax.ShapeDtypeStruct((MINE, WIN, HEAD), BF16),
        ],
        cost_estimate=pl.CostEstimate(
            flops=MINE * WIN * D * D * 64, bytes_accessed=MINE * WIN * D * 8, transcendentals=0
        ),
        name="own_head",
    )(starts, tokens, tokens, w_own)


def copies_kernel(core_ref, w_ref, out_ref, sem):
    rows = w_ref.at[pl.ds(core_ref[0] * (D // 2), D // 2)]
    copies = [pltpu.make_async_copy(rows, out_ref.at[j], sem.at[j]) for j in range(N_MP)]
    for copy in copies:
        copy.start()
    for copy in copies:
        copy.wait()


def copies_of_half(w_own, core):
    return pl.pallas_call(
        copies_kernel,
        grid_spec=pltpu.PrefetchScalarGridSpec(
            num_scalar_prefetch=1,
            grid=(1,),
            in_specs=[in_hbm()],
            out_specs=in_hbm(),
            scratch_shapes=[pltpu.SemaphoreType.DMA((N_MP,))],
        ),
        out_shape=jax.ShapeDtypeStruct((N_MP, D // 2, D), BF16),
        name="copies",
    )(core, w_own)


def layer_kernel(
    start_ref, len_ref, pos_ref,
    tokens_ref, half_hbm, att_hbm, gate_hbm, near_ref, far_ref, w_out_ref, table_ref,
    out_ref, state_ref,
    x_s, half_s, att_s, gate_s, w_out_s, out_s, sem_in, sem_w, sem_out,
):
    part = pos_ref[0]
    low_is_near = pos_ref[1] == 0
    order = [part] + [(part + s) % HEADS for s in range(1, HEADS)]

    def loads(i):
        first = start_ref[i]
        second = jnp.minimum(first + 1, BLK_DEV - 1)
        pairs = [
            (half_hbm.at[i], half_s.at[pl.ds(i * WIN, WIN)]),
            (att_hbm.at[i], att_s.at[pl.ds(i * WIN, WIN)]),
            (gate_hbm.at[i], gate_s.at[pl.ds(i * WIN, WIN)]),
            (tokens_ref.at[pl.ds(first * BLOCK, BLOCK)], x_s.at[pl.ds(i * WIN, BLOCK)]),
            (tokens_ref.at[pl.ds(second * BLOCK, BLOCK)], x_s.at[pl.ds(i * WIN + BLOCK, BLOCK)]),
        ]
        return [pltpu.make_async_copy(a, b, sem_in.at[i, j]) for j, (a, b) in enumerate(pairs)]

    weights = [
        pltpu.make_async_copy(
            w_out_ref.at[pl.ds(h * HEAD, HEAD)], w_out_s.at[pl.ds(s * HEAD, HEAD)], sem_w.at[s]
        )
        for s, h in enumerate(order)
    ]

    def sends(i):
        at = (i // PER_HALF, slice(None), pl.ds((i % PER_HALF) * N_MP, N_MP))
        return pltpu.make_async_copy(out_s.at[at], out_ref.at[at], sem_out.at[i])

    def send_table(half):
        at = (half, slice(None), pl.ds(MSG - 1, 1))
        return pltpu.make_async_copy(out_s.at[at], out_ref.at[at], sem_out.at[MINE + half])

    for copy in loads(0):
        copy.start()
    for i in range(1, MINE):
        for copy in loads(i):
            copy.start()
        if i == 1:
            for copy in weights:
                copy.start()
    tile = jnp.broadcast_to(table_ref[...], (TILE, 128)).astype(F32).astype(BF16)
    for half in range(HALVES):
        out_s[half, :, MSG - 1] = jnp.broadcast_to(tile[None], (GROUPS, TILE, 128))
        send_table(half).start()

    def group(step, carry):
        first_user = step * GROUP
        for j in range(GROUP):
            for copy in loads(first_user + j):
                copy.wait()
        rows = pl.ds(pl.multiple_of(first_user * WIN, WIN), GROUP * WIN)
        low = half_s[rows, : D // 2]
        high = half_s[rows, D // 2 :]
        parts = [jnp.where(low_is_near, low, high), jnp.where(low_is_near, high, low)]
        heads, gates = [att_s[rows, :]], [gate_s[rows, :]]
        for h in order[1:]:
            u, v, q, k = project(parts, [near_ref[h], far_ref[h]])
            gates.append(u)
            heads.append(
                jnp.concatenate(
                    [
                        attend(*(t[j * WIN : (j + 1) * WIN] for t in (q, k, v)))
                        for j in range(GROUP)
                    ],
                    axis=0,
                )
            )
        total = jnp.sum(heads[0] + heads[1] + (heads[2] + heads[3]), axis=1, keepdims=True)
        squares = jnp.sum(
            heads[0] * heads[0] + heads[1] * heads[1] + (heads[2] * heads[2] + heads[3] * heads[3]),
            axis=1,
            keepdims=True,
        )
        mean, inv = norm_stats(total, squares, 1.0 / WIN)
        gated = jnp.concatenate(
            [((a - mean) * inv * g.astype(F32)).astype(BF16) for a, g in zip(heads, gates)], axis=1
        )

        @pl.when(step == 0)
        def _():
            for copy in weights:
                copy.wait()

        both = jnp.dot(gated, w_out_s[...], preferred_element_type=F32) + x_s[rows, :].astype(F32)
        at = lax.broadcasted_iota(jnp.int32, (WIN, 1), 0)
        for j in range(GROUP):
            i = first_user + j
            length = len_ref[i]
            half_id = i // PER_HALF
            base = (i % PER_HALF) * N_MP
            mixed = jnp.where(at < length, both[j * WIN : (j + 1) * WIN], 0.0).astype(BF16)
            for q in range(N_MP):
                out_s[half_id, :, base + q] = mixed[:, q * HEAD : (q + 1) * HEAD].reshape(
                    GROUPS, TILE, HEAD
                )
            sends(i).start()
            last = length - 1
            pick = lax.broadcasted_iota(jnp.int32, (TILE, HEAD), 0) == last % TILE
            for q in range(N_MP):
                tile = out_s[half_id, last // TILE, base + q].astype(F32)
                state_ref[i, :, q * HEAD : (q + 1) * HEAD] = jnp.sum(
                    jnp.where(pick, tile, 0.0), axis=0, keepdims=True
                ).astype(BF16)
        return carry

    lax.fori_loop(0, MINE // GROUP, group, 0)
    for half in range(HALVES):
        send_table(half).wait()
    for i in range(MINE):
        sends(i).wait()


def layer(tokens, starts, lengths, position, kept, near, far, w_out, table):
    message = (HALVES, GROUPS, MSG, TILE, HEAD)
    return pl.pallas_call(
        layer_kernel,
        grid_spec=pltpu.PrefetchScalarGridSpec(
            num_scalar_prefetch=3,
            grid=(1,),
            in_specs=[in_hbm()] * 4 + [in_vmem()] * 2 + [in_hbm(), in_vmem()],
            out_specs=[in_hbm(), in_vmem()],
            scratch_shapes=[
                pltpu.VMEM((MINE * WIN, D), BF16),
                pltpu.VMEM((MINE * WIN, D), BF16),
                pltpu.VMEM((MINE * WIN, HEAD), F32),
                pltpu.VMEM((MINE * WIN, HEAD), BF16),
                pltpu.VMEM((D, D), BF16),
                pltpu.VMEM(message, BF16),
                pltpu.SemaphoreType.DMA((MINE, 5)),
                pltpu.SemaphoreType.DMA((HEADS,)),
                pltpu.SemaphoreType.DMA((MINE + HALVES,)),
            ],
        ),
        out_shape=[
            jax.ShapeDtypeStruct(message, BF16),
            jax.ShapeDtypeStruct((MINE, 1, D), BF16),
        ],
        name="layer",
    )(starts, lengths, position, tokens, *kept, keep(near), keep(far), w_out, table)


def regroup_kernel(first_ref, in_ref, out_ref, table_v, table_s, sem):
    table = jnp.max(in_ref[:, PER_HALF * N_MP].astype(F32), axis=1)
    table_v[...] = table.astype(jnp.int32)
    copy = pltpu.make_async_copy(table_v, table_s, sem)
    copy.start()
    copy.wait()
    first = first_ref[0]

    def one(d, carry):
        for k in range(PER_HALF):
            o = table_s[d, first + k]
            for q in range(N_MP):
                out_ref[o, q, k] = in_ref[d, k * N_MP + q]
        return carry

    lax.fori_loop(0, N_DP, one, 0, unroll=8)


def regroup(spread, first):
    return pl.pallas_call(
        regroup_kernel,
        grid_spec=pltpu.PrefetchScalarGridSpec(
            num_scalar_prefetch=1,
            grid=(1,),
            in_specs=[in_vmem()],
            out_specs=pl.BlockSpec(
                (N_DP, N_MP, PER_HALF, TILE, HEAD), lambda i, s: (0, 0, 0, 0, 0)
            ),
            scratch_shapes=[
                pltpu.VMEM((N_DP, 128), jnp.int32),
                pltpu.SMEM((N_DP, 128), jnp.int32),
                pltpu.SemaphoreType.DMA,
            ],
        ),
        out_shape=jax.ShapeDtypeStruct((N_DP, N_MP, PER_HALF, TILE, HEAD), BF16),
        name="regroup",
    )(first, keep(spread))


def place_kernel(len_ref, off_ref, in_ref, out_ref, zero_v, used_s, sem):
    per_block = BLOCK // TILE
    zero_v[...] = jnp.zeros_like(zero_v)

    def clear(b, carry):
        used_s[b] = 0
        return carry

    lax.fori_loop(0, BLK_DEV, clear, 0, unroll=8)

    def send(u, j):
        half = (u % MINE) // PER_HALF
        block = off_ref[u] + j
        used_s[block] = 1
        pltpu.make_async_copy(
            in_ref.at[half, pl.ds(j * per_block, per_block), u // MINE, u % PER_HALF],
            out_ref.at[pl.ds(block * per_block, per_block)],
            sem,
        ).start()

    def one(u, carry):
        send(u, 0)

        @pl.when(len_ref[u] > BLOCK)
        def _():
            send(u, 1)

        return carry

    lax.fori_loop(0, USERS, one, 0)

    def fill(b, carry):
        @pl.when(used_s[b] == 0)
        def _():
            pltpu.make_async_copy(zero_v, out_ref.at[pl.ds(b * per_block, per_block)], sem).start()

        return carry

    lax.fori_loop(0, BLK_DEV, fill, 0)
    pltpu.make_async_copy(out_ref, out_ref, sem).wait()


def place(arrived, lengths, offsets):
    rows = BLK_DEV * BLOCK
    return pl.pallas_call(
        place_kernel,
        grid_spec=pltpu.PrefetchScalarGridSpec(
            num_scalar_prefetch=2,
            grid=(1,),
            in_specs=[in_vmem()],
            out_specs=in_hbm(),
            scratch_shapes=[
                pltpu.VMEM((BLOCK // TILE, TILE, HEAD), BF16),
                pltpu.SMEM((BLK_DEV,), jnp.int32),
                pltpu.SemaphoreType.DMA,
            ],
        ),
        out_shape=jax.ShapeDtypeStruct((rows // TILE, TILE, HEAD), BF16),
        name="place",
    )(lengths, offsets, keep(arrived)).reshape(rows, HEAD)


def per_device(tokens, w_uvqk, w_out, hist_len, owner, recv_offset, block_start):
    me = lax.axis_index("dp")
    part = lax.axis_index("mp")
    first = part * MINE

    core = me % 2
    near = lax.all_to_all(
        copies_of_half(w_uvqk, core[None]), "mp", 0, 0, tiled=True
    )
    far = lax.ppermute(near, "dp", [(i, i ^ 1) for i in range(N_DP)])
    table = jnp.concatenate([owner, hist_len, recv_offset, jnp.zeros((1, 56), jnp.int32)], axis=1)
    starts = lax.dynamic_slice_in_dim(block_start[0], first, MINE, 0)
    lengths = lax.dynamic_slice_in_dim(hist_len[0], first, MINE, 0)
    kept = own_head(tokens, starts, w_uvqk)
    mixed, last = layer(
        tokens, starts, lengths, jnp.stack([part, core]), kept, near, far, w_out, table
    )

    spread = lax.all_to_all(
        mixed.reshape(N_DP, MSG * TILE, HEAD), "dp", 0, 0, tiled=True
    ).reshape(N_DP, MSG, TILE, HEAD)
    held = first + (me // GROUPS) * PER_HALF
    sorted_rows = regroup(spread, held[None])
    table = spread[:, MSG - 1, 0, :].astype(jnp.int32)
    owners = table[:, :USERS]
    arrived = lax.all_to_all(
        sorted_rows.reshape(N_DP * N_MP, PER_HALF * TILE, HEAD), ("dp", "mp"), 0, 0, tiled=True
    )
    mine = owners == me
    recv_len = jnp.sum(jnp.where(mine, table[:, USERS : 2 * USERS], 0), axis=0)
    recv_off = jnp.sum(jnp.where(mine, table[:, 2 * USERS : 3 * USERS], 0), axis=0)
    packed = place(
        arrived.reshape(HALVES, GROUPS, N_MP, PER_HALF, TILE, HEAD), recv_len, recv_off
    )

    columns = last.reshape(MINE, N_MP, HEAD)
    state = jnp.zeros((N_MP, MINE, HEAD), BF16)
    for s in range(N_MP):
        to = (part + s) % N_MP
        piece = lax.dynamic_slice_in_dim(columns, to, 1, 1)[:, 0]
        if s:
            piece = lax.ppermute(piece, "mp", [(i, (i + s) % N_MP) for i in range(N_MP)])
        state = lax.dynamic_update_slice_in_dim(state, piece[None], (part - s) % N_MP, 0)
    return packed, state.reshape(USERS, HEAD)


def solution(mesh):
    in_specs = (
        P("dp", None),
        P(None, "mp"),
        P(),
        P("dp", None),
        P("dp", None),
        P("dp", None),
        P("dp", None),
    )
    out_specs = (P("dp", "mp"), P("dp", "mp"))
    return jax.shard_map(
        per_device, mesh=mesh, in_specs=in_specs, out_specs=out_specs, check_vma=False
    )
```

```python
import jax
import jax.numpy as jnp
from jax import lax
from jax.experimental import pallas as pl
from jax.experimental.pallas import tpu as pltpu
from jax.sharding import PartitionSpec as P

D = 512
HEADS = 4
HEAD = D // HEADS
BLOCK = 128
MAXB = 2
BLK_DEV = 48
USERS = 24
N_DP = 64
N_MP = 4
WIN = MAXB * BLOCK
MINE = USERS // N_MP
RAW = 2
DONE = MINE - RAW
TILE = 8
GROUPS = WIN // TILE
HALVES = N_DP // GROUPS
GROUP = 2
RAW_MSG = N_MP + 1
ROUND = DONE // HALVES
MSG = (ROUND + 1) * N_MP
EPS = 1e-05
BF16 = jnp.bfloat16
F32 = jnp.float32


def silu_of_twice(h):
    return h + h * jnp.tanh(h)


def project(half_parts, w_parts):
    acc = jnp.dot(half_parts[0], w_parts[0], preferred_element_type=F32)
    for n, w in zip(half_parts[1:], w_parts[1:]):
        acc = acc + jnp.dot(n, w, preferred_element_type=F32)
    proj = silu_of_twice(acc).astype(BF16)
    return [proj[:, j * HEAD : (j + 1) * HEAD] for j in range(4)]


def attend(q, k, v):
    row = lax.broadcasted_iota(jnp.int32, (BLOCK, BLOCK), 0)
    col = lax.broadcasted_iota(jnp.int32, (BLOCK, BLOCK), 1)
    causal = col <= row
    scale = 0.5 * HEAD ** (-0.5)
    contract_last = (((1,), (1,)), ((), ()))
    s0 = lax.dot_general(q[:BLOCK], k[:BLOCK], contract_last, preferred_element_type=F32)
    s1 = lax.dot_general(q[BLOCK:], k, contract_last, preferred_element_type=F32)
    a0 = jnp.where(causal, silu_of_twice(s0 * scale), 0.0).astype(BF16)
    b = silu_of_twice(s1 * scale)
    a1 = jnp.concatenate(
        [b[:, :BLOCK].astype(BF16), jnp.where(causal, b[:, BLOCK:], 0.0).astype(BF16)], axis=1
    )
    return jnp.concatenate(
        [
            jnp.dot(a0, v[:BLOCK], preferred_element_type=F32),
            jnp.dot(a1, v, preferred_element_type=F32),
        ],
        axis=0,
    )


def norm_stats(total, squares, unit=1.0):
    mean = total * (1.0 / D)
    var = squares * (1.0 / D) - mean * mean
    return mean, lax.rsqrt(var * (unit * unit) + EPS) * unit


def in_vmem():
    return pl.BlockSpec(memory_space=pltpu.VMEM)


def in_hbm():
    return pl.BlockSpec(memory_space=pltpu.HBM)


def keep(array):
    return pltpu.with_memory_space_constraint(array, pltpu.VMEM)


def own_head_kernel(start_ref, x0_ref, x1_ref, w_ref, half_ref, att_ref, gate_ref):
    x = jnp.concatenate([x0_ref[...], x1_ref[...]], axis=0).astype(F32)
    mean, inv = norm_stats(
        jnp.sum(x, axis=1, keepdims=True), jnp.sum(x * x, axis=1, keepdims=True)
    )
    half = ((x - mean) * (inv * 0.5)).astype(BF16)
    half_ref[0] = half
    u, v, q, k = project([half], [w_ref[...]])
    gate_ref[0] = u
    att_ref[0] = attend(q, k, v)


def own_head(tokens, starts, w_own):
    def per_user(width):
        return pl.BlockSpec((1, WIN, width), lambda i, s: (i, 0, 0))

    return pl.pallas_call(
        own_head_kernel,
        grid_spec=pltpu.PrefetchScalarGridSpec(
            num_scalar_prefetch=1,
            grid=(DONE,),
            in_specs=[
                pl.BlockSpec((BLOCK, D), lambda i, s: (s[i], 0)),
                pl.BlockSpec((BLOCK, D), lambda i, s: (jnp.minimum(s[i] + 1, BLK_DEV - 1), 0)),
                pl.BlockSpec((D, D), lambda i, s: (0, 0)),
            ],
            out_specs=[per_user(D), per_user(HEAD), per_user(HEAD)],
        ),
        out_shape=[
            jax.ShapeDtypeStruct((DONE, WIN, D), BF16),
            jax.ShapeDtypeStruct((DONE, WIN, HEAD), F32),
            jax.ShapeDtypeStruct((DONE, WIN, HEAD), BF16),
        ],
        cost_estimate=pl.CostEstimate(
            flops=DONE * WIN * D * D * 64, bytes_accessed=DONE * WIN * D * 8, transcendentals=0
        ),
        name="own_head",
    )(starts, tokens, tokens, w_own)


def rows_of(tiles):
    return jnp.concatenate(
        [tiles[..., q, :, :].reshape(-1, HEAD) for q in range(N_MP)], axis=1
    )


def table_tile(table_ref):
    tile = jnp.broadcast_to(table_ref[...], (TILE, 128)).astype(F32).astype(BF16)
    return jnp.broadcast_to(tile[None], (GROUPS, TILE, 128))


def pack_kernel(start_ref, tokens_ref, table_ref, out_ref, x_s, sem):
    copies = []
    for k in range(RAW):
        first = start_ref[k]
        second = jnp.minimum(first + 1, BLK_DEV - 1)
        for j, block in enumerate((first, second)):
            copy = pltpu.make_async_copy(
                tokens_ref.at[pl.ds(block * BLOCK, BLOCK)],
                x_s.at[k, pl.ds(j * BLOCK, BLOCK)],
                sem.at[k, j],
            )
            copy.start()
            copies.append(copy)
    tile = table_tile(table_ref)
    for k in range(RAW):
        out_ref[k, :, N_MP] = tile
    for copy in copies:
        copy.wait()
    for k in range(RAW):
        for q in range(N_MP):
            out_ref[k, :, q] = x_s[k, :, q * HEAD : (q + 1) * HEAD].reshape(GROUPS, TILE, HEAD)


def pack(tokens, starts, table):
    shape = (RAW, GROUPS, RAW_MSG, TILE, HEAD)
    return pl.pallas_call(
        pack_kernel,
        grid_spec=pltpu.PrefetchScalarGridSpec(
            num_scalar_prefetch=1,
            grid=(1,),
            in_specs=[in_hbm(), in_vmem()],
            out_specs=pl.BlockSpec(shape, lambda i, s: (0, 0, 0, 0, 0)),
            scratch_shapes=[pltpu.VMEM((RAW, WIN, D), BF16), pltpu.SemaphoreType.DMA((RAW, MAXB))],
        ),
        out_shape=jax.ShapeDtypeStruct(shape, BF16),
        name="pack",
    )(starts, tokens, table)


def head_order(part):
    return [part] + [(part + HEADS - s) % HEADS for s in range(1, HEADS)]


def mix(low_is_near, half_rows, first, near, far, w_out_of, x_rows):
    low = half_rows[:, : D // 2]
    high = half_rows[:, D // 2 :]
    parts = [jnp.where(low_is_near, low, high), jnp.where(low_is_near, high, low)]
    users = half_rows.shape[0] // WIN
    heads, gates = [first[0]], [first[1]]
    for near_ref, far_ref in zip(near, far):
        u, v, q, k = project(parts, [near_ref[...], far_ref[...]])
        gates.append(u)
        heads.append(attend_users(users, q, k, v))
    total = jnp.sum(heads[0] + heads[1] + (heads[2] + heads[3]), axis=1, keepdims=True)
    squares = jnp.sum(
        heads[0] * heads[0] + heads[1] * heads[1] + (heads[2] * heads[2] + heads[3] * heads[3]),
        axis=1,
        keepdims=True,
    )
    mean, inv = norm_stats(total, squares, 1.0 / WIN)
    gated = jnp.concatenate(
        [((a - mean) * inv * g.astype(F32)).astype(BF16) for a, g in zip(heads, gates)], axis=1
    )
    return jnp.dot(gated, w_out_of(), preferred_element_type=F32) + x_rows().astype(F32)


def attend_users(users, q, k, v):
    return jnp.concatenate(
        [attend(*(t[j * WIN : (j + 1) * WIN] for t in (q, k, v))) for j in range(users)], axis=0
    )


def live_rows(mixed, length):
    at = lax.broadcasted_iota(jnp.int32, (WIN, 1), 0)
    return jnp.where(at < length, mixed, 0.0).astype(BF16)


def last_row(tile, length):
    pick = lax.broadcasted_iota(jnp.int32, (TILE, HEAD), 0) == (length - 1) % TILE
    return jnp.sum(jnp.where(pick, tile.astype(F32), 0.0), axis=0, keepdims=True).astype(BF16)


def w_out_copies(part, w_out_ref, w_out_s, sem):
    return [
        pltpu.make_async_copy(
            w_out_ref.at[pl.ds(h * HEAD, HEAD)], w_out_s.at[pl.ds(s * HEAD, HEAD)], sem.at[s]
        )
        for s, h in enumerate(head_order(part))
    ]


def layer_kernel(start_ref, len_ref, pos_ref, tokens_ref, half_hbm, att_hbm, gate_hbm, *rest):
    near, far = rest[: HEADS - 1], rest[HEADS - 1 : 2 * HEADS - 2]
    w_out_ref, out_ref, state_ref = rest[2 * HEADS - 2 : 2 * HEADS + 1]
    x_s, half_s, att_s, gate_s, w_out_s, out_s, sem_in, sem_w, sem_out = rest[2 * HEADS + 1 :]
    low_is_near = pos_ref[1] == 0

    def loads(i):
        first = start_ref[i]
        second = jnp.minimum(first + 1, BLK_DEV - 1)
        pairs = [
            (half_hbm.at[i], half_s.at[pl.ds(i * WIN, WIN)]),
            (att_hbm.at[i], att_s.at[pl.ds(i * WIN, WIN)]),
            (gate_hbm.at[i], gate_s.at[pl.ds(i * WIN, WIN)]),
            (tokens_ref.at[pl.ds(first * BLOCK, BLOCK)], x_s.at[pl.ds(i * WIN, BLOCK)]),
            (tokens_ref.at[pl.ds(second * BLOCK, BLOCK)], x_s.at[pl.ds(i * WIN + BLOCK, BLOCK)]),
        ]
        return [pltpu.make_async_copy(a, b, sem_in.at[i, j]) for j, (a, b) in enumerate(pairs)]

    weights = w_out_copies(pos_ref[0], w_out_ref, w_out_s, sem_w)

    def sends(i):
        at = (i % HALVES, slice(None), pl.ds((i // HALVES) * N_MP, N_MP))
        return pltpu.make_async_copy(out_s.at[at], out_ref.at[at], sem_out.at[i])

    for i in range(DONE):
        for copy in loads(i):
            copy.start()
        if i == GROUP - 1:
            for copy in weights:
                copy.start()

    def group(step, carry):
        first_user = step * GROUP
        for j in range(GROUP):
            for copy in loads(first_user + j):
                copy.wait()
        rows = pl.ds(pl.multiple_of(first_user * WIN, WIN), GROUP * WIN)

        def w_out_of():
            @pl.when(step == 0)
            def _():
                for copy in weights:
                    copy.wait()

            return w_out_s[...]

        both = mix(
            low_is_near,
            half_s[rows, :],
            (att_s[rows, :], gate_s[rows, :]),
            near,
            far,
            w_out_of,
            lambda: x_s[rows, :],
        )
        for j in range(GROUP):
            i = first_user + j
            length = len_ref[i]
            half_id = i % HALVES
            base = (i // HALVES) * N_MP
            mixed = live_rows(both[j * WIN : (j + 1) * WIN], length)
            for q in range(N_MP):
                out_s[half_id, :, base + q] = mixed[:, q * HEAD : (q + 1) * HEAD].reshape(
                    GROUPS, TILE, HEAD
                )
            sends(i).start()
            for q in range(N_MP):
                state_ref[i, :, q * HEAD : (q + 1) * HEAD] = last_row(
                    out_s[half_id, (length - 1) // TILE, base + q], length
                )
        return carry

    lax.fori_loop(0, DONE // GROUP, group, 0)
    for i in range(DONE):
        sends(i).wait()


def layer(tokens, starts, lengths, position, kept, near, far, w_out):
    message = (HALVES, GROUPS, MSG, TILE, HEAD)
    return pl.pallas_call(
        layer_kernel,
        grid_spec=pltpu.PrefetchScalarGridSpec(
            num_scalar_prefetch=3,
            grid=(1,),
            in_specs=[in_hbm()] * 4 + [in_vmem()] * (2 * HEADS - 2) + [in_hbm()],
            out_specs=[in_hbm(), in_vmem()],
            scratch_shapes=[
                pltpu.VMEM((DONE * WIN, D), BF16),
                pltpu.VMEM((DONE * WIN, D), BF16),
                pltpu.VMEM((DONE * WIN, HEAD), F32),
                pltpu.VMEM((DONE * WIN, HEAD), BF16),
                pltpu.VMEM((D, D), BF16),
                pltpu.VMEM((HALVES, GROUPS, ROUND * N_MP, TILE, HEAD), BF16),
                pltpu.SemaphoreType.DMA((DONE, 5)),
                pltpu.SemaphoreType.DMA((HEADS,)),
                pltpu.SemaphoreType.DMA((DONE,)),
            ],
        ),
        out_shape=[
            jax.ShapeDtypeStruct(message, BF16),
            jax.ShapeDtypeStruct((DONE, 1, D), BF16),
        ],
        name="layer",
    )(starts, lengths, position, tokens, *kept, *map(keep, near), *map(keep, far), w_out)


def raw_kernel(first_tile, len_ref, pos_ref, src_ref, w_own_ref, *rest):
    near, far = rest[: HEADS - 1], rest[HEADS - 1 : 2 * HEADS - 2]
    w_out_ref = rest[2 * HEADS - 2]
    pieces = rest[2 * HEADS - 1 : 2 * HEADS - 1 + N_MP]
    state_ref, x_s, w_out_s, mixed_s, sem_x, sem_w = rest[2 * HEADS - 1 + N_MP :]
    part = pos_ref[0]
    loads = [
        pltpu.make_async_copy(
            src_ref.at[pl.ds(k * GROUPS, GROUPS), pl.ds(first_tile, N_MP)], x_s.at[k], sem_x.at[k]
        )
        for k in range(RAW)
    ]
    weights = w_out_copies(part, w_out_ref, w_out_s, sem_w)
    for copy in loads + weights:
        copy.start()
    for copy in loads:
        copy.wait()

    def x_rows():
        return rows_of(x_s[...])

    x = x_rows().astype(F32)
    mean, inv = norm_stats(
        jnp.sum(x, axis=1, keepdims=True), jnp.sum(x * x, axis=1, keepdims=True)
    )
    half = ((x - mean) * (inv * 0.5)).astype(BF16)
    u, v, q, k = project([half], [w_own_ref[...]])

    def w_out_of():
        for copy in weights:
            copy.wait()
        return w_out_s[...]

    both = mix(
        pos_ref[1] == 0, half, (attend_users(RAW, q, k, v), u), near, far, w_out_of, x_rows
    )
    for k in range(RAW):
        mixed = live_rows(both[k * WIN : (k + 1) * WIN], len_ref[k])
        for q in range(N_MP):
            mixed_s[q, k] = mixed[:, q * HEAD : (q + 1) * HEAD].reshape(GROUPS, TILE, HEAD)
        for q in range(N_MP):
            state_ref[k, :, q * HEAD : (q + 1) * HEAD] = last_row(
                mixed_s[q, k, (len_ref[k] - 1) // TILE], len_ref[k]
            )
    for s in range(N_MP):
        pieces[s][...] = mixed_s[(part + s) % N_MP]


def raw_layer(source, first_tile, lengths, position, w_own, near, far, w_out):
    piece = jax.ShapeDtypeStruct((RAW, GROUPS, TILE, HEAD), BF16)
    outs = pl.pallas_call(
        lambda *refs: raw_kernel(first_tile, *refs),
        grid_spec=pltpu.PrefetchScalarGridSpec(
            num_scalar_prefetch=2,
            grid=(1,),
            in_specs=[in_hbm()] + [in_vmem()] * (2 * HEADS - 1) + [in_hbm()],
            out_specs=[in_vmem()] * (N_MP + 1),
            scratch_shapes=[
                pltpu.VMEM((RAW, GROUPS, N_MP, TILE, HEAD), BF16),
                pltpu.VMEM((D, D), BF16),
                pltpu.VMEM((N_MP, RAW, GROUPS, TILE, HEAD), BF16),
                pltpu.SemaphoreType.DMA((RAW,)),
                pltpu.SemaphoreType.DMA((HEADS,)),
            ],
        ),
        out_shape=[piece] * N_MP + [jax.ShapeDtypeStruct((RAW, 1, D), BF16)],
    )(lengths, position, source, w_own, *near, *far, w_out)
    return outs[:N_MP], outs[N_MP]


def merge_kernel(first_ref, in_ref, msg_ref, out_ref, sorted_s, table_v, table_s, sem):
    table = jnp.max(in_ref[:, N_MP].astype(F32), axis=1)
    table_v[...] = table.astype(jnp.int32)
    copy = pltpu.make_async_copy(table_v, table_s, sem.at[0])
    copy.start()
    copy.wait()
    first = first_ref[0]

    def one(d, carry):
        o = table_s[d, first]
        for q in range(N_MP):
            sorted_s[o, q] = in_ref[d, q]
        return carry

    lax.fori_loop(0, N_DP, one, 0, unroll=8)
    send = pltpu.make_async_copy(sorted_s, out_ref.at[:, pl.ds(ROUND * N_MP, N_MP)], sem.at[1])
    send.start()
    send.wait()


def merge(spread, first, message):
    return pl.pallas_call(
        merge_kernel,
        grid_spec=pltpu.PrefetchScalarGridSpec(
            num_scalar_prefetch=1,
            grid=(1,),
            in_specs=[in_vmem(), in_hbm()],
            out_specs=in_hbm(),
            scratch_shapes=[
                pltpu.VMEM((N_DP, N_MP, TILE, HEAD), BF16),
                pltpu.VMEM((N_DP, 128), jnp.int32),
                pltpu.SMEM((N_DP, 128), jnp.int32),
                pltpu.SemaphoreType.DMA((2,)),
            ],
        ),
        out_shape=jax.ShapeDtypeStruct((N_DP, MSG, TILE, HEAD), BF16),
        input_output_aliases={2: 0},
        name="merge",
    )(first, keep(spread), message)


def regroup_kernel(to_ref, in_ref, out_ref):
    def one(d, carry):
        for r in range(ROUND):
            o = to_ref[r * N_DP + d]
            for q in range(N_MP):
                out_ref[o, q, r] = in_ref[d, r * N_MP + q]
        return carry

    lax.fori_loop(0, N_DP, one, 0, unroll=8)


def regroup(spread, to):
    shape = (N_DP, N_MP, ROUND, TILE, HEAD)
    return pl.pallas_call(
        regroup_kernel,
        grid_spec=pltpu.PrefetchScalarGridSpec(
            num_scalar_prefetch=1,
            grid=(1,),
            in_specs=[in_vmem()],
            out_specs=pl.BlockSpec(shape, lambda i, s: (0, 0, 0, 0, 0)),
        ),
        out_shape=jax.ShapeDtypeStruct(shape, BF16),
        name="regroup",
    )(to, keep(spread))


def place_kernel(len_ref, off_ref, pos_ref, in_ref, *rest):
    pieces = rest[:N_MP]
    out_ref, zero_v, used_s, sem = rest[N_MP:]
    per_block = BLOCK // TILE
    zero_v[...] = jnp.zeros_like(zero_v)

    def clear(b, carry):
        used_s[b] = 0
        return carry

    lax.fori_loop(0, BLK_DEV, clear, 0, unroll=8)

    def send(u, source):
        def block(j):
            to = off_ref[u] + j
            used_s[to] = 1
            pltpu.make_async_copy(
                source(pl.ds(j * per_block, per_block)),
                out_ref.at[pl.ds(to * per_block, per_block)],
                sem,
            ).start()

        block(0)

        @pl.when(len_ref[u] > BLOCK)
        def _():
            block(1)

    for s in range(N_MP):
        m = (pos_ref[0] + N_MP - s) % N_MP
        for k in range(RAW):
            send(m * MINE + k, lambda rows: pieces[s].at[k, rows])

    def one(n, carry):
        m = n // DONE
        i = n % DONE
        send(m * MINE + RAW + i, lambda rows: in_ref.at[i % HALVES, rows, m, i // HALVES])
        return carry

    lax.fori_loop(0, N_MP * DONE, one, 0)

    def fill(b, carry):
        @pl.when(used_s[b] == 0)
        def _():
            pltpu.make_async_copy(zero_v, out_ref.at[pl.ds(b * per_block, per_block)], sem).start()

        return carry

    lax.fori_loop(0, BLK_DEV, fill, 0)
    pltpu.make_async_copy(out_ref, out_ref, sem).wait()


def place(arrived, pieces, lengths, offsets, position):
    rows = BLK_DEV * BLOCK
    return pl.pallas_call(
        place_kernel,
        grid_spec=pltpu.PrefetchScalarGridSpec(
            num_scalar_prefetch=3,
            grid=(1,),
            in_specs=[in_vmem()] * (1 + N_MP),
            out_specs=in_hbm(),
            scratch_shapes=[
                pltpu.VMEM((BLOCK // TILE, TILE, HEAD), BF16),
                pltpu.SMEM((BLK_DEV,), jnp.int32),
                pltpu.SemaphoreType.DMA,
            ],
        ),
        out_shape=jax.ShapeDtypeStruct((rows // TILE, TILE, HEAD), BF16),
        compiler_params=pltpu.CompilerParams(vmem_limit_bytes=32 * 1024 * 1024),
        name="place",
    )(lengths, offsets, position, keep(arrived), *map(keep, pieces)).reshape(rows, HEAD)


def along_mp(array, s):
    return lax.ppermute(array, "mp", [(i, (i + s) % N_MP) for i in range(N_MP)])


def per_device(tokens, w_uvqk, w_out, hist_len, owner, recv_offset, block_start):
    me = lax.axis_index("dp")
    part = lax.axis_index("mp")
    first = part * MINE
    core = me % 2
    half = me // GROUPS
    position = jnp.stack([part, core])

    starts = lax.dynamic_slice_in_dim(block_start[0], first, MINE, 0)
    lengths = lax.dynamic_slice_in_dim(hist_len[0], first, MINE, 0)
    table = jnp.concatenate([owner, hist_len, recv_offset, jnp.zeros((1, 56), jnp.int32)], axis=1)

    mine_rows = jnp.where(core == 0, w_uvqk[: D // 2], w_uvqk[D // 2 :])
    near, far = [], []
    for s in range(1, N_MP):
        near.append(along_mp(mine_rows, s))
    for s in range(1, N_MP):
        far.append(lax.ppermute(near[s - 1], "dp", [(i, i ^ 1) for i in range(N_DP)]))

    raw = pack(tokens, starts[:RAW], table)
    raw_in = lax.all_to_all(
        raw.reshape(N_DP, RAW_MSG * TILE, HEAD), "dp", 0, 0, tiled=True
    ).reshape(N_DP, RAW_MSG, TILE, HEAD)
    kept = own_head(tokens, starts[RAW:], w_uvqk)
    message, last = layer(
        tokens, starts[RAW:], lengths[RAW:], position, kept, near, far, w_out
    )
    message = merge(
        raw_in, (first + half)[None], message.reshape(N_DP, MSG, TILE, HEAD)
    )
    spread = lax.all_to_all(
        message.reshape(N_DP, MSG * TILE, HEAD), "dp", 0, 0, tiled=True
    ).reshape(N_DP, MSG, TILE, HEAD)
    _, raw_last = raw_layer(
        raw.reshape(N_DP, RAW_MSG, TILE, HEAD), 0, lengths[:RAW], position,
        w_uvqk, near, far, w_out,
    )

    table = raw_in[:, N_MP, 0, :].astype(jnp.int32)
    owners = table[:, :USERS]
    held = lax.dynamic_slice_in_dim(owners, first + RAW + half, HALVES * (ROUND - 1) + 1, 1)
    to = held[:, ::HALVES].T.reshape(-1)
    mine = owners == me
    recv_len = jnp.sum(jnp.where(mine, table[:, USERS : 2 * USERS], 0), axis=0)
    recv_off = jnp.sum(jnp.where(mine, table[:, 2 * USERS : 3 * USERS], 0), axis=0)

    sorted_rows = regroup(spread, to)
    arrived = lax.all_to_all(
        sorted_rows.reshape(N_DP * N_MP, ROUND * TILE, HEAD), ("dp", "mp"), 0, 0, tiled=True
    )
    pieces, _ = raw_layer(
        spread, ROUND * N_MP,
        lax.dynamic_slice_in_dim(recv_len, first, RAW, 0), position,
        w_uvqk, near, far, w_out,
    )
    pieces = [pieces[0]] + [along_mp(pieces[s], s) for s in range(1, N_MP)]
    packed = place(
        arrived.reshape(HALVES, GROUPS, N_MP, ROUND, TILE, HEAD),
        pieces, recv_len, recv_off, position,
    )

    columns = jnp.concatenate([raw_last, last], axis=0).reshape(MINE, N_MP, HEAD)
    state = jnp.zeros((N_MP, MINE, HEAD), BF16)
    for s in range(N_MP):
        to_part = (part + s) % N_MP
        piece = lax.dynamic_slice_in_dim(columns, to_part, 1, 1)[:, 0]
        if s:
            piece = along_mp(piece, s)
        state = lax.dynamic_update_slice_in_dim(state, piece[None], (part - s) % N_MP, 0)
    return packed, state.reshape(USERS, HEAD)


def solution(mesh):
    in_specs = (
        P("dp", None),
        P(None, "mp"),
        P(),
        P("dp", None),
        P("dp", None),
        P("dp", None),
        P("dp", None),
    )
    out_specs = (P("dp", "mp"), P("dp", "mp"))
    return jax.shard_map(
        per_device, mesh=mesh, in_specs=in_specs, out_specs=out_specs, check_vma=False
    )
```

```python
import jax
import jax.numpy as jnp
from jax import lax
from jax.experimental import pallas as pl
from jax.experimental.pallas import tpu as pltpu
from jax.sharding import PartitionSpec as P

D = 512
HEADS = 4
HEAD = D // HEADS
BLOCK = 128
MAXB = 2
BLK_DEV = 48
USERS = 24
N_DP = 64
N_MP = 4
WIN = MAXB * BLOCK
MINE = USERS // N_MP
RAW = 2
DONE = MINE - RAW
TILE = 8
GROUPS = WIN // TILE
HALVES = N_DP // GROUPS
GROUP = 2
OWN_GROUP = 2
RAW_MSG = N_MP + 1
ROUND = DONE // HALVES
MSG = (ROUND + 1) * N_MP
EPS = 1e-05
BF16 = jnp.bfloat16
F32 = jnp.float32


def silu_of_twice(h):
    return h + h * jnp.tanh(h)


def project(half_parts, w_parts):
    acc = jnp.dot(half_parts[0], w_parts[0], preferred_element_type=F32)
    for n, w in zip(half_parts[1:], w_parts[1:]):
        acc = acc + jnp.dot(n, w, preferred_element_type=F32)
    proj = silu_of_twice(acc).astype(BF16)
    return [proj[:, j * HEAD : (j + 1) * HEAD] for j in range(4)]


def attend(q, k, v):
    row = lax.broadcasted_iota(jnp.int32, (BLOCK, BLOCK), 0)
    col = lax.broadcasted_iota(jnp.int32, (BLOCK, BLOCK), 1)
    causal = col <= row
    scale = 0.5 * HEAD ** (-0.5)
    contract_last = (((1,), (1,)), ((), ()))
    s0 = lax.dot_general(q[:BLOCK], k[:BLOCK], contract_last, preferred_element_type=F32)
    s1 = lax.dot_general(q[BLOCK:], k, contract_last, preferred_element_type=F32)
    a0 = jnp.where(causal, silu_of_twice(s0 * scale), 0.0).astype(BF16)
    b = silu_of_twice(s1 * scale)
    a1 = jnp.concatenate(
        [b[:, :BLOCK].astype(BF16), jnp.where(causal, b[:, BLOCK:], 0.0).astype(BF16)], axis=1
    )
    return jnp.concatenate(
        [
            jnp.dot(a0, v[:BLOCK], preferred_element_type=F32),
            jnp.dot(a1, v, preferred_element_type=F32),
        ],
        axis=0,
    )


def norm_stats(total, squares, unit=1.0):
    mean = total * (1.0 / D)
    var = squares * (1.0 / D) - mean * mean
    return mean, lax.rsqrt(var * (unit * unit) + EPS) * unit


def token_copies(tokens_ref, block, x_ref, row, sem):
    second = jnp.minimum(block + 1, BLK_DEV - 1)
    return [
        pltpu.make_async_copy(
            tokens_ref.at[pl.ds(b * BLOCK, BLOCK)],
            x_ref.at[pl.ds(row + j * BLOCK, BLOCK)],
            sem.at[j],
        )
        for j, b in enumerate((block, second))
    ]


def norm_half(x):
    mean, inv = norm_stats(
        jnp.sum(x, axis=1, keepdims=True), jnp.sum(x * x, axis=1, keepdims=True)
    )
    return ((x - mean) * (inv * 0.5)).astype(BF16)


def own_head_kernel(
    start_ref, part_ref, tokens_ref, w_ref, half_ref, att_ref, gate_ref,
    x_s, half_s, att_s, gate_s, sem_in, sem_out,
):
    def loads(i):
        block = start_ref[0, part_ref[0] * MINE + RAW + i]
        return token_copies(tokens_ref, block, x_s, i * WIN, sem_in.at[i])

    def sends(step):
        rows = pl.ds(step * OWN_GROUP * WIN, OWN_GROUP * WIN)
        pairs = ((half_s, half_ref), (att_s, att_ref), (gate_s, gate_ref))
        return [
            pltpu.make_async_copy(a.at[rows], b.at[rows], sem_out.at[step, j])
            for j, (a, b) in enumerate(pairs)
        ]

    for i in range(DONE):
        for copy in loads(i):
            copy.start()

    def group(step, carry):
        for j in range(OWN_GROUP):
            for copy in loads(step * OWN_GROUP + j):
                copy.wait()
        rows = pl.ds(pl.multiple_of(step * OWN_GROUP * WIN, WIN), OWN_GROUP * WIN)
        half = norm_half(x_s[rows, :].astype(F32))
        half_s[rows, :] = half
        u, v, q, k = project([half], [w_ref[...]])
        gate_s[rows, :] = u
        att_s[rows, :] = attend_users(OWN_GROUP, q, k, v)
        for copy in sends(step):
            copy.start()
        return carry

    lax.fori_loop(0, DONE // OWN_GROUP, group, 0)
    for step in range(DONE // OWN_GROUP):
        for copy in sends(step):
            copy.wait()


def in_vmem():
    return pl.BlockSpec(memory_space=pltpu.VMEM)


def in_hbm():
    return pl.BlockSpec(memory_space=pltpu.HBM)


def keep(array):
    return pltpu.with_memory_space_constraint(array, pltpu.VMEM)


def own_head(tokens, starts, part, w_own):
    kept = [((DONE * WIN, D), BF16), ((DONE * WIN, HEAD), F32), ((DONE * WIN, HEAD), BF16)]
    return pl.pallas_call(
        own_head_kernel,
        grid_spec=pltpu.PrefetchScalarGridSpec(
            num_scalar_prefetch=2,
            grid=(1,),
            in_specs=[in_hbm(), in_vmem()],
            out_specs=[in_hbm()] * 3,
            scratch_shapes=[pltpu.VMEM((DONE * WIN, D), BF16)]
            + [pltpu.VMEM(*k) for k in kept]
            + [
                pltpu.SemaphoreType.DMA((DONE, MAXB)),
                pltpu.SemaphoreType.DMA((DONE // OWN_GROUP, 3)),
            ],
        ),
        out_shape=[jax.ShapeDtypeStruct(*k) for k in kept],
        cost_estimate=pl.CostEstimate(
            flops=DONE * WIN * D * D * 64, bytes_accessed=DONE * WIN * D * 8, transcendentals=0
        ),
        name="own_head",
    )(starts, part, tokens, w_own)


def rows_of(tiles):
    return jnp.concatenate(
        [tiles[..., q, :, :].reshape(-1, HEAD) for q in range(N_MP)], axis=1
    )


def pack_kernel(
    start_ref, part_ref, tokens_ref, owner_ref, len_ref, off_ref, out_ref, x_s, row_s, sem
):
    copies = []
    for k in range(RAW):
        block = start_ref[0, part_ref[0] * MINE + k]
        copies += token_copies(tokens_ref, block, x_s, k * WIN, sem.at[k])
    for copy in copies:
        copy.start()
    row_s[...] = jnp.zeros_like(row_s)
    for j, ref in enumerate((owner_ref, len_ref, off_ref)):
        row_s[:, j * USERS : (j + 1) * USERS] = ref[...]
    tile = jnp.broadcast_to(row_s[...], (TILE, 128)).astype(F32).astype(BF16)
    for k in range(RAW):
        out_ref[k, :, N_MP] = jnp.broadcast_to(tile[None], (GROUPS, TILE, 128))
    for copy in copies:
        copy.wait()
    for k in range(RAW):
        for q in range(N_MP):
            out_ref[k, :, q] = x_s[k * WIN : (k + 1) * WIN, q * HEAD : (q + 1) * HEAD].reshape(
                GROUPS, TILE, HEAD
            )


def pack(tokens, starts, part, owner, hist_len, recv_offset):
    shape = (RAW, GROUPS, RAW_MSG, TILE, HEAD)
    return pl.pallas_call(
        pack_kernel,
        grid_spec=pltpu.PrefetchScalarGridSpec(
            num_scalar_prefetch=2,
            grid=(1,),
            in_specs=[in_hbm()] + [in_vmem()] * 3,
            out_specs=pl.BlockSpec(shape, lambda i, *_: (0, 0, 0, 0, 0)),
            scratch_shapes=[
                pltpu.VMEM((RAW * WIN, D), BF16),
                pltpu.VMEM((1, 128), jnp.int32),
                pltpu.SemaphoreType.DMA((RAW, MAXB)),
            ],
        ),
        out_shape=jax.ShapeDtypeStruct(shape, BF16),
        name="pack",
    )(starts, part, tokens, owner, hist_len, recv_offset)


def head_order(part):
    return [part] + [(part + HEADS - s) % HEADS for s in range(1, HEADS)]


def mix(low_is_near, half_rows, first, near, far, w_out_of, x_rows):
    low = half_rows[:, : D // 2]
    high = half_rows[:, D // 2 :]
    parts = [jnp.where(low_is_near, low, high), jnp.where(low_is_near, high, low)]
    users = half_rows.shape[0] // WIN
    heads, gates = [first[0]], [first[1]]
    for near_ref, far_ref in zip(near, far):
        u, v, q, k = project(parts, [near_ref[...], far_ref[...]])
        gates.append(u)
        heads.append(attend_users(users, q, k, v))
    total = jnp.sum(heads[0] + heads[1] + (heads[2] + heads[3]), axis=1, keepdims=True)
    squares = jnp.sum(
        heads[0] * heads[0] + heads[1] * heads[1] + (heads[2] * heads[2] + heads[3] * heads[3]),
        axis=1,
        keepdims=True,
    )
    mean, inv = norm_stats(total, squares, 1.0 / WIN)
    gated = jnp.concatenate(
        [((a - mean) * inv * g.astype(F32)).astype(BF16) for a, g in zip(heads, gates)], axis=1
    )
    return jnp.dot(gated, w_out_of(), preferred_element_type=F32) + x_rows().astype(F32)


def attend_users(users, q, k, v):
    return jnp.concatenate(
        [attend(*(t[j * WIN : (j + 1) * WIN] for t in (q, k, v))) for j in range(users)], axis=0
    )


def live_rows(mixed, length):
    at = lax.broadcasted_iota(jnp.int32, (WIN, 1), 0)
    return jnp.where(at < length, mixed, 0.0).astype(BF16)


def last_row(tile, length):
    pick = lax.broadcasted_iota(jnp.int32, (TILE, HEAD), 0) == (length - 1) % TILE
    return jnp.sum(jnp.where(pick, tile.astype(F32), 0.0), axis=0, keepdims=True).astype(BF16)


def w_out_copies(part, w_out_ref, w_out_s, sem):
    return [
        pltpu.make_async_copy(
            w_out_ref.at[pl.ds(h * HEAD, HEAD)], w_out_s.at[pl.ds(s * HEAD, HEAD)], sem.at[s]
        )
        for s, h in enumerate(head_order(part))
    ]


def layer_kernel(
    start_ref, len_ref, part_ref, core_ref, tokens_ref, half_hbm, att_hbm, gate_hbm, *rest
):
    near, far = rest[: HEADS - 1], rest[HEADS - 1 : 2 * HEADS - 2]
    w_out_ref, out_ref, state_ref = rest[2 * HEADS - 2 : 2 * HEADS + 1]
    x_s, half_s, att_s, gate_s, w_out_s, out_s, sem_in, sem_w, sem_out = rest[2 * HEADS + 1 :]
    low_is_near = core_ref[0] == 0
    first_id = part_ref[0] * MINE + RAW

    def loads(i):
        rows = pl.ds(i * WIN, WIN)
        pairs = ((half_hbm, half_s), (att_hbm, att_s), (gate_hbm, gate_s))
        return [
            pltpu.make_async_copy(a.at[rows], b.at[rows], sem_in.at[i, MAXB + j])
            for j, (a, b) in enumerate(pairs)
        ] + token_copies(tokens_ref, start_ref[0, first_id + i], x_s, i * WIN, sem_in.at[i])

    weights = w_out_copies(part_ref[0], w_out_ref, w_out_s, sem_w)

    def sends(i):
        at = (i % HALVES, slice(None), pl.ds((i // HALVES) * N_MP, N_MP))
        return pltpu.make_async_copy(out_s.at[at], out_ref.at[at], sem_out.at[i])

    for i in range(DONE):
        for copy in loads(i):
            copy.start()
        if i == GROUP - 1:
            for copy in weights:
                copy.start()

    def group(step, carry):
        first_user = step * GROUP
        for j in range(GROUP):
            for copy in loads(first_user + j):
                copy.wait()
        rows = pl.ds(pl.multiple_of(first_user * WIN, WIN), GROUP * WIN)

        def w_out_of():
            @pl.when(step == 0)
            def _():
                for copy in weights:
                    copy.wait()

            return w_out_s[...]

        both = mix(
            low_is_near,
            half_s[rows, :],
            (att_s[rows, :], gate_s[rows, :]),
            near,
            far,
            w_out_of,
            lambda: x_s[rows, :],
        )
        for j in range(GROUP):
            i = first_user + j
            length = len_ref[0, first_id + i]
            half_id = i % HALVES
            base = (i // HALVES) * N_MP
            mixed = live_rows(both[j * WIN : (j + 1) * WIN], length)
            for q in range(N_MP):
                out_s[half_id, :, base + q] = mixed[:, q * HEAD : (q + 1) * HEAD].reshape(
                    GROUPS, TILE, HEAD
                )
            sends(i).start()
            for q in range(N_MP):
                state_ref[i, :, q * HEAD : (q + 1) * HEAD] = last_row(
                    out_s[half_id, (length - 1) // TILE, base + q], length
                )
        return carry

    lax.fori_loop(0, DONE // GROUP, group, 0)
    for i in range(DONE):
        sends(i).wait()


def layer(tokens, starts, lengths, part, core, kept, near, far, w_out):
    message = (HALVES, GROUPS, MSG, TILE, HEAD)
    return pl.pallas_call(
        layer_kernel,
        grid_spec=pltpu.PrefetchScalarGridSpec(
            num_scalar_prefetch=4,
            grid=(1,),
            in_specs=[in_hbm()] * 4 + [in_vmem()] * (2 * HEADS - 2) + [in_hbm()],
            out_specs=[in_hbm(), in_vmem()],
            scratch_shapes=[
                pltpu.VMEM((DONE * WIN, D), BF16),
                pltpu.VMEM((DONE * WIN, D), BF16),
                pltpu.VMEM((DONE * WIN, HEAD), F32),
                pltpu.VMEM((DONE * WIN, HEAD), BF16),
                pltpu.VMEM((D, D), BF16),
                pltpu.VMEM((HALVES, GROUPS, ROUND * N_MP, TILE, HEAD), BF16),
                pltpu.SemaphoreType.DMA((DONE, 5)),
                pltpu.SemaphoreType.DMA((HEADS,)),
                pltpu.SemaphoreType.DMA((DONE,)),
            ],
        ),
        out_shape=[
            jax.ShapeDtypeStruct(message, BF16),
            jax.ShapeDtypeStruct((DONE, 1, D), BF16),
        ],
        name="layer",
    )(starts, lengths, part, core, tokens, *kept, *map(keep, near), *map(keep, far), w_out)


def raw_kernel(first_tile, len_ref, part_ref, core_ref, src_ref, w_own_ref, *rest):
    near, far = rest[: HEADS - 1], rest[HEADS - 1 : 2 * HEADS - 2]
    w_out_ref = rest[2 * HEADS - 2]
    pieces = rest[2 * HEADS - 1 : 2 * HEADS - 1 + N_MP]
    state_ref, x_s, w_out_s, mixed_s, sem_x, sem_w = rest[2 * HEADS - 1 + N_MP :]
    part = part_ref[0]
    lengths = [len_ref[0, part * MINE + k] for k in range(RAW)]
    loads = [
        pltpu.make_async_copy(
            src_ref.at[pl.ds(k * GROUPS, GROUPS), pl.ds(first_tile, N_MP)], x_s.at[k], sem_x.at[k]
        )
        for k in range(RAW)
    ]
    weights = w_out_copies(part, w_out_ref, w_out_s, sem_w)
    for copy in loads + weights:
        copy.start()
    for copy in loads:
        copy.wait()

    def x_rows():
        return rows_of(x_s[...])

    half = norm_half(x_rows().astype(F32))
    u, v, q, k = project([half], [w_own_ref[...]])

    def w_out_of():
        for copy in weights:
            copy.wait()
        return w_out_s[...]

    both = mix(
        core_ref[0] == 0, half, (attend_users(RAW, q, k, v), u), near, far, w_out_of, x_rows
    )
    for k in range(RAW):
        mixed = live_rows(both[k * WIN : (k + 1) * WIN], lengths[k])
        for q in range(N_MP):
            mixed_s[q, k] = mixed[:, q * HEAD : (q + 1) * HEAD].reshape(GROUPS, TILE, HEAD)
        for q in range(N_MP):
            state_ref[k, :, q * HEAD : (q + 1) * HEAD] = last_row(
                mixed_s[q, k, (lengths[k] - 1) // TILE], lengths[k]
            )
    for s in range(N_MP):
        pieces[s][...] = mixed_s[(part + s) % N_MP]


def raw_layer(source, first_tile, lengths, part, core, w_own, near, far, w_out):
    piece = jax.ShapeDtypeStruct((RAW, GROUPS, TILE, HEAD), BF16)
    outs = pl.pallas_call(
        lambda *refs: raw_kernel(first_tile, *refs),
        grid_spec=pltpu.PrefetchScalarGridSpec(
            num_scalar_prefetch=3,
            grid=(1,),
            in_specs=[in_hbm()] + [in_vmem()] * (2 * HEADS - 1) + [in_hbm()],
            out_specs=[in_vmem()] * (N_MP + 1),
            scratch_shapes=[
                pltpu.VMEM((RAW, GROUPS, N_MP, TILE, HEAD), BF16),
                pltpu.VMEM((D, D), BF16),
                pltpu.VMEM((N_MP, RAW, GROUPS, TILE, HEAD), BF16),
                pltpu.SemaphoreType.DMA((RAW,)),
                pltpu.SemaphoreType.DMA((HEADS,)),
            ],
        ),
        out_shape=[piece] * N_MP + [jax.ShapeDtypeStruct((RAW, 1, D), BF16)],
    )(lengths, part, core, source, w_own, *near, *far, w_out)
    return outs[:N_MP], outs[N_MP]


def merge_kernel(first_ref, in_ref, msg_ref, out_ref, sorted_s, table_v, table_s, sem):
    table = jnp.max(in_ref[:, N_MP].astype(F32), axis=1)
    table_v[...] = table.astype(jnp.int32)
    copy = pltpu.make_async_copy(table_v, table_s, sem.at[0])
    copy.start()
    copy.wait()
    first = first_ref[0]

    def one(d, carry):
        o = table_s[d, first]
        for q in range(N_MP):
            sorted_s[o, q] = in_ref[d, q]
        return carry

    lax.fori_loop(0, N_DP, one, 0, unroll=8)
    send = pltpu.make_async_copy(sorted_s, out_ref.at[:, pl.ds(ROUND * N_MP, N_MP)], sem.at[1])
    send.start()
    send.wait()


def merge(spread, first, message):
    return pl.pallas_call(
        merge_kernel,
        grid_spec=pltpu.PrefetchScalarGridSpec(
            num_scalar_prefetch=1,
            grid=(1,),
            in_specs=[in_vmem(), in_hbm()],
            out_specs=in_hbm(),
            scratch_shapes=[
                pltpu.VMEM((N_DP, N_MP, TILE, HEAD), BF16),
                pltpu.VMEM((N_DP, 128), jnp.int32),
                pltpu.SMEM((N_DP, 128), jnp.int32),
                pltpu.SemaphoreType.DMA((2,)),
            ],
        ),
        out_shape=jax.ShapeDtypeStruct((N_DP, MSG, TILE, HEAD), BF16),
        input_output_aliases={2: 0},
        name="merge",
    )(first, keep(spread), message)


def regroup_kernel(to_ref, in_ref, out_ref):
    def one(d, carry):
        for r in range(ROUND):
            o = to_ref[r * N_DP + d]
            for q in range(N_MP):
                out_ref[o, q, r] = in_ref[d, r * N_MP + q]
        return carry

    lax.fori_loop(0, N_DP, one, 0, unroll=8)


def regroup(spread, to):
    shape = (N_DP, N_MP, ROUND, TILE, HEAD)
    return pl.pallas_call(
        regroup_kernel,
        grid_spec=pltpu.PrefetchScalarGridSpec(
            num_scalar_prefetch=1,
            grid=(1,),
            in_specs=[in_vmem()],
            out_specs=pl.BlockSpec(shape, lambda i, s: (0, 0, 0, 0, 0)),
        ),
        out_shape=jax.ShapeDtypeStruct(shape, BF16),
        name="regroup",
    )(to, keep(spread))


def place_kernel(len_ref, off_ref, part_ref, in_ref, own_ref, *rest):
    out_ref, zero_v, used_s, own_s, sem, sem_own = rest[N_MP - 1 :]
    pieces = (own_s, *rest[: N_MP - 1])
    load = pltpu.make_async_copy(own_ref, own_s, sem_own)
    load.start()
    per_block = BLOCK // TILE
    zero_v[...] = jnp.zeros_like(zero_v)

    def clear(b, carry):
        used_s[b] = 0
        return carry

    lax.fori_loop(0, BLK_DEV, clear, 0, unroll=8)

    def send(u, source):
        def block(j):
            to = off_ref[u] + j
            used_s[to] = 1
            pltpu.make_async_copy(
                source(pl.ds(j * per_block, per_block)),
                out_ref.at[pl.ds(to * per_block, per_block)],
                sem,
            ).start()

        block(0)

        @pl.when(len_ref[u] > BLOCK)
        def _():
            block(1)

    def send_piece(s):
        m = (part_ref[0] + N_MP - s) % N_MP
        for k in range(RAW):
            send(m * MINE + k, lambda rows: pieces[s].at[k, rows])

    for s in range(1, N_MP):
        send_piece(s)

    def one(n, carry):
        m = n // DONE
        i = n % DONE
        send(m * MINE + RAW + i, lambda rows: in_ref.at[i % HALVES, rows, m, i // HALVES])
        return carry

    lax.fori_loop(0, N_MP * DONE, one, 0)
    load.wait()
    send_piece(0)

    def fill(b, carry):
        @pl.when(used_s[b] == 0)
        def _():
            pltpu.make_async_copy(zero_v, out_ref.at[pl.ds(b * per_block, per_block)], sem).start()

        return carry

    lax.fori_loop(0, BLK_DEV, fill, 0)
    pltpu.make_async_copy(out_ref, out_ref, sem).wait()


def place(arrived, pieces, lengths, offsets, part):
    rows = BLK_DEV * BLOCK
    return pl.pallas_call(
        place_kernel,
        grid_spec=pltpu.PrefetchScalarGridSpec(
            num_scalar_prefetch=3,
            grid=(1,),
            in_specs=[in_vmem(), in_hbm()] + [in_vmem()] * (N_MP - 1),
            out_specs=in_hbm(),
            scratch_shapes=[
                pltpu.VMEM((BLOCK // TILE, TILE, HEAD), BF16),
                pltpu.SMEM((BLK_DEV,), jnp.int32),
                pltpu.VMEM((RAW, GROUPS, TILE, HEAD), BF16),
                pltpu.SemaphoreType.DMA,
                pltpu.SemaphoreType.DMA,
            ],
        ),
        out_shape=jax.ShapeDtypeStruct((rows // TILE, TILE, HEAD), BF16),
        compiler_params=pltpu.CompilerParams(vmem_limit_bytes=32 * 1024 * 1024),
        name="place",
    )(lengths, offsets, part, keep(arrived), pieces[0], *map(keep, pieces[1:])).reshape(rows, HEAD)


def along_mp(array, s):
    return lax.ppermute(array, "mp", [(i, (i + s) % N_MP) for i in range(N_MP)])


def per_device(tokens, w_uvqk, w_out, hist_len, owner, recv_offset, block_start):
    me = lax.axis_index("dp")
    part = lax.axis_index("mp")
    first = part * MINE
    core = me % 2
    half = me // GROUPS
    part_1, core_1 = part[None], core[None]

    mine_rows = jnp.where(core == 0, w_uvqk[: D // 2], w_uvqk[D // 2 :])
    near, far = [], []
    for s in range(1, N_MP):
        near.append(along_mp(mine_rows, s))
    for s in range(1, N_MP):
        far.append(lax.ppermute(near[s - 1], "dp", [(i, i ^ 1) for i in range(N_DP)]))

    raw = pack(tokens, block_start, part_1, owner, hist_len, recv_offset)
    raw_in = lax.all_to_all(
        raw.reshape(N_DP, RAW_MSG * TILE, HEAD), "dp", 0, 0, tiled=True
    ).reshape(N_DP, RAW_MSG, TILE, HEAD)
    kept = own_head(tokens, block_start, part_1, w_uvqk)
    message, last = layer(
        tokens, block_start, hist_len, part_1, core_1, kept, near, far, w_out
    )
    message = merge(
        raw_in, (first + half)[None], message.reshape(N_DP, MSG, TILE, HEAD)
    )
    spread = lax.all_to_all(
        message.reshape(N_DP, MSG * TILE, HEAD), "dp", 0, 0, tiled=True
    ).reshape(N_DP, MSG, TILE, HEAD)
    _, raw_last = raw_layer(
        raw.reshape(N_DP, RAW_MSG, TILE, HEAD), 0, hist_len, part_1, core_1,
        w_uvqk, near, far, w_out,
    )

    table = raw_in[:, N_MP, 0, :].astype(jnp.int32)
    owners = table[:, :USERS]
    held = lax.dynamic_slice_in_dim(owners, first + RAW + half, HALVES * (ROUND - 1) + 1, 1)
    to = held[:, ::HALVES].T.reshape(-1)
    mine = owners == me
    recv_len = jnp.sum(jnp.where(mine, table[:, USERS : 2 * USERS], 0), axis=0)
    recv_off = jnp.sum(jnp.where(mine, table[:, 2 * USERS : 3 * USERS], 0), axis=0)

    sorted_rows = regroup(spread, to)
    arrived = lax.all_to_all(
        sorted_rows.reshape(N_DP * N_MP, ROUND * TILE, HEAD), ("dp", "mp"), 0, 0, tiled=True
    )
    pieces, _ = raw_layer(
        spread, ROUND * N_MP, recv_len[None], part_1, core_1,
        w_uvqk, near, far, w_out,
    )
    pieces = [pieces[0]] + [along_mp(pieces[s], s) for s in range(1, N_MP)]
    packed = place(
        arrived.reshape(HALVES, GROUPS, N_MP, ROUND, TILE, HEAD),
        pieces, recv_len, recv_off, part_1,
    )

    columns = jnp.concatenate([raw_last, last], axis=0).reshape(MINE, N_MP, HEAD)
    state = jnp.zeros((N_MP, MINE, HEAD), BF16)
    for s in range(N_MP):
        to_part = (part + s) % N_MP
        piece = lax.dynamic_slice_in_dim(columns, to_part, 1, 1)[:, 0]
        if s:
            piece = along_mp(piece, s)
        state = lax.dynamic_update_slice_in_dim(state, piece[None], (part - s) % N_MP, 0)
    return packed, state.reshape(USERS, HEAD)


def solution(mesh):
    in_specs = (
        P("dp", None),
        P(None, "mp"),
        P(),
        P("dp", None),
        P("dp", None),
        P("dp", None),
        P("dp", None),
    )
    out_specs = (P("dp", "mp"), P("dp", "mp"))
    return jax.shard_map(
        per_device, mesh=mesh, in_specs=in_specs, out_specs=out_specs, check_vma=False
    )
```

```python
import jax
import jax.numpy as jnp
from jax import lax
from jax.experimental import pallas as pl
from jax.experimental.pallas import tpu as pltpu
from jax.sharding import PartitionSpec as P

D = 512
HEADS = 4
HEAD = D // HEADS
BLOCK = 128
MAXB = 2
BLK_DEV = 48
USERS = 24
N_DP = 64
N_MP = 4
WIN = MAXB * BLOCK
MINE = USERS // N_MP
RAW = 2
DONE = MINE - RAW
TILE = 8
GROUPS = WIN // TILE
HALVES = N_DP // GROUPS
GROUP = 2
OWN_GROUP = 2
CHUNKS = 4
RAW_MSG = N_MP + 1
ROUND = DONE // HALVES
MSG = (ROUND + 1) * N_MP
EPS = 1e-05
BF16 = jnp.bfloat16
F32 = jnp.float32


def silu_of_twice(h):
    return h + h * jnp.tanh(h)


def project(half_parts, w_parts):
    acc = jnp.dot(half_parts[0], w_parts[0], preferred_element_type=F32)
    for n, w in zip(half_parts[1:], w_parts[1:]):
        acc = acc + jnp.dot(n, w, preferred_element_type=F32)
    proj = silu_of_twice(acc).astype(BF16)
    return [proj[:, j * HEAD : (j + 1) * HEAD] for j in range(4)]


def attend(q, k, v):
    row = lax.broadcasted_iota(jnp.int32, (BLOCK, BLOCK), 0)
    col = lax.broadcasted_iota(jnp.int32, (BLOCK, BLOCK), 1)
    causal = col <= row
    scale = 0.5 * HEAD ** (-0.5)
    contract_last = (((1,), (1,)), ((), ()))
    s0 = lax.dot_general(q[:BLOCK], k[:BLOCK], contract_last, preferred_element_type=F32)
    s1 = lax.dot_general(q[BLOCK:], k, contract_last, preferred_element_type=F32)
    a0 = jnp.where(causal, silu_of_twice(s0 * scale), 0.0).astype(BF16)
    b = silu_of_twice(s1 * scale)
    a1 = jnp.concatenate(
        [b[:, :BLOCK].astype(BF16), jnp.where(causal, b[:, BLOCK:], 0.0).astype(BF16)], axis=1
    )
    return jnp.concatenate(
        [
            jnp.dot(a0, v[:BLOCK], preferred_element_type=F32),
            jnp.dot(a1, v, preferred_element_type=F32),
        ],
        axis=0,
    )


def norm_stats(total, squares, unit=1.0):
    mean = total * (1.0 / D)
    var = squares * (1.0 / D) - mean * mean
    return mean, lax.rsqrt(var * (unit * unit) + EPS) * unit


def token_copies(tokens_ref, block, x_ref, row, sem):
    second = jnp.minimum(block + 1, BLK_DEV - 1)
    return [
        pltpu.make_async_copy(
            tokens_ref.at[pl.ds(b * BLOCK, BLOCK)],
            x_ref.at[pl.ds(row + j * BLOCK, BLOCK)],
            sem.at[j],
        )
        for j, b in enumerate((block, second))
    ]


def norm_half(x):
    mean, inv = norm_stats(
        jnp.sum(x, axis=1, keepdims=True), jnp.sum(x * x, axis=1, keepdims=True)
    )
    return ((x - mean) * (inv * 0.5)).astype(BF16)


def own_head_kernel(
    start_ref, part_ref, tokens_ref, w_ref, half_ref, att_ref, gate_ref,
    x_s, half_s, att_s, gate_s, w_s, sem_in, sem_w, sem_out,
):
    load_w = pltpu.make_async_copy(w_ref, w_s, sem_w)

    def loads(i):
        block = start_ref[0, part_ref[0] * MINE + RAW + i]
        return token_copies(tokens_ref, block, x_s, i * WIN, sem_in.at[i])

    def sends(step):
        rows = pl.ds(step * OWN_GROUP * WIN, OWN_GROUP * WIN)
        pairs = ((half_s, half_ref), (att_s, att_ref), (gate_s, gate_ref))
        return [
            pltpu.make_async_copy(a.at[rows], b.at[rows], sem_out.at[step, j])
            for j, (a, b) in enumerate(pairs)
        ]

    for i in range(DONE):
        for copy in loads(i):
            copy.start()
        if i == OWN_GROUP - 1:
            load_w.start()

    def group(step, carry):
        for j in range(OWN_GROUP):
            for copy in loads(step * OWN_GROUP + j):
                copy.wait()
        rows = pl.ds(pl.multiple_of(step * OWN_GROUP * WIN, WIN), OWN_GROUP * WIN)
        half = norm_half(x_s[rows, :].astype(F32))
        half_s[rows, :] = half

        @pl.when(step == 0)
        def _():
            load_w.wait()

        u, v, q, k = project([half], [w_s[...]])
        gate_s[rows, :] = u
        att_s[rows, :] = attend_users(OWN_GROUP, q, k, v)
        for copy in sends(step):
            copy.start()
        return carry

    lax.fori_loop(0, DONE // OWN_GROUP, group, 0)
    for step in range(DONE // OWN_GROUP):
        for copy in sends(step):
            copy.wait()


def in_vmem():
    return pl.BlockSpec(memory_space=pltpu.VMEM)


def in_hbm():
    return pl.BlockSpec(memory_space=pltpu.HBM)


def keep(array):
    return pltpu.with_memory_space_constraint(array, pltpu.VMEM)


def own_head(tokens, starts, part, w_own):
    kept = [((DONE * WIN, D), BF16), ((DONE * WIN, HEAD), F32), ((DONE * WIN, HEAD), BF16)]
    return pl.pallas_call(
        own_head_kernel,
        grid_spec=pltpu.PrefetchScalarGridSpec(
            num_scalar_prefetch=2,
            grid=(1,),
            in_specs=[in_hbm()] * 2,
            out_specs=[in_hbm()] * 3,
            scratch_shapes=[pltpu.VMEM((DONE * WIN, D), BF16)]
            + [pltpu.VMEM(*k) for k in kept]
            + [
                pltpu.VMEM((D, D), BF16),
                pltpu.SemaphoreType.DMA((DONE, MAXB)),
                pltpu.SemaphoreType.DMA,
                pltpu.SemaphoreType.DMA((DONE // OWN_GROUP, 3)),
            ],
        ),
        out_shape=[jax.ShapeDtypeStruct(*k) for k in kept],
        cost_estimate=pl.CostEstimate(
            flops=DONE * WIN * D * D * 64, bytes_accessed=DONE * WIN * D * 8, transcendentals=0
        ),
        name="own_head",
    )(starts, part, tokens, w_own)


def rows_of(tiles):
    return jnp.concatenate(
        [tiles[..., q, :, :].reshape(-1, HEAD) for q in range(N_MP)], axis=1
    )


def pack_kernel(
    start_ref, part_ref, core_ref, tokens_ref, w_ref, owner_ref, len_ref, off_ref,
    out_ref, rows_ref, x_s, table_s, row_s, out_s, sem, sem_t, sem_w, sem_out,
):
    tables = [
        pltpu.make_async_copy(ref, table_s.at[j], sem_t.at[j])
        for j, ref in enumerate((owner_ref, len_ref, off_ref))
    ]
    half = D // 2
    weights = pltpu.make_async_copy(w_ref.at[pl.ds(core_ref[0] * half, half)], rows_ref, sem_w)
    loads = [
        token_copies(
            tokens_ref, start_ref[0, part_ref[0] * MINE + k], x_s, k * WIN, sem.at[k]
        )
        for k in range(RAW)
    ]
    for copy in tables + loads[0] + [weights] + loads[1]:
        copy.start()
    row_s[...] = jnp.zeros_like(row_s)
    for j, copy in enumerate(tables):
        copy.wait()
        row_s[:, j * USERS : (j + 1) * USERS] = table_s[j]
    tile = jnp.broadcast_to(row_s[...], (TILE, 128)).astype(F32).astype(BF16)
    for k in range(RAW):
        out_s[k, :, N_MP] = jnp.broadcast_to(tile[None], (GROUPS, TILE, 128))
    sends = [pltpu.make_async_copy(out_s.at[k], out_ref.at[k], sem_out.at[k]) for k in range(RAW)]
    for k in range(RAW):
        for copy in loads[k]:
            copy.wait()
        for q in range(N_MP):
            out_s[k, :, q] = x_s[k * WIN : (k + 1) * WIN, q * HEAD : (q + 1) * HEAD].reshape(
                GROUPS, TILE, HEAD
            )
        sends[k].start()
    weights.wait()
    for copy in sends:
        copy.wait()


def pack(tokens, starts, part, core, w_own, owner, hist_len, recv_offset):
    shape = (RAW, GROUPS, RAW_MSG, TILE, HEAD)
    return pl.pallas_call(
        pack_kernel,
        grid_spec=pltpu.PrefetchScalarGridSpec(
            num_scalar_prefetch=3,
            grid=(1,),
            in_specs=[in_hbm()] * 5,
            out_specs=[in_hbm(), in_vmem()],
            scratch_shapes=[
                pltpu.VMEM((RAW * WIN, D), BF16),
                pltpu.VMEM((3, 1, USERS), jnp.int32),
                pltpu.VMEM((1, 128), jnp.int32),
                pltpu.VMEM(shape, BF16),
                pltpu.SemaphoreType.DMA((RAW, MAXB)),
                pltpu.SemaphoreType.DMA((3,)),
                pltpu.SemaphoreType.DMA,
                pltpu.SemaphoreType.DMA((RAW,)),
            ],
        ),
        out_shape=[jax.ShapeDtypeStruct(shape, BF16), pltpu.VMEM((D // 2, D), BF16)],
        name="pack",
    )(starts, part, core, tokens, w_own, owner, hist_len, recv_offset)


def head_order(part):
    return [part] + [(part + HEADS - s) % HEADS for s in range(1, HEADS)]


def mix(low_is_near, half_rows, first, near, far, w_out_of, x_rows):
    low = half_rows[:, : D // 2]
    high = half_rows[:, D // 2 :]
    parts = [jnp.where(low_is_near, low, high), jnp.where(low_is_near, high, low)]
    users = half_rows.shape[0] // WIN
    heads, gates = [first[0]], [first[1]]
    for near_ref, far_ref in zip(near, far):
        u, v, q, k = project(parts, [near_ref[...], far_ref[...]])
        gates.append(u)
        heads.append(attend_users(users, q, k, v))
    total = jnp.sum(heads[0] + heads[1] + (heads[2] + heads[3]), axis=1, keepdims=True)
    squares = jnp.sum(
        heads[0] * heads[0] + heads[1] * heads[1] + (heads[2] * heads[2] + heads[3] * heads[3]),
        axis=1,
        keepdims=True,
    )
    mean, inv = norm_stats(total, squares, 1.0 / WIN)
    gated = jnp.concatenate(
        [((a - mean) * inv * g.astype(F32)).astype(BF16) for a, g in zip(heads, gates)], axis=1
    )
    return jnp.dot(gated, w_out_of(), preferred_element_type=F32) + x_rows().astype(F32)


def attend_users(users, q, k, v):
    return jnp.concatenate(
        [attend(*(t[j * WIN : (j + 1) * WIN] for t in (q, k, v))) for j in range(users)], axis=0
    )


def live_rows(mixed, length):
    at = lax.broadcasted_iota(jnp.int32, (WIN, 1), 0)
    return jnp.where(at < length, mixed, 0.0).astype(BF16)


def last_row(tile, length):
    pick = lax.broadcasted_iota(jnp.int32, (TILE, HEAD), 0) == (length - 1) % TILE
    return jnp.sum(jnp.where(pick, tile.astype(F32), 0.0), axis=0, keepdims=True).astype(BF16)


def w_out_copies(part, w_out_ref, w_out_s, sem):
    return [
        pltpu.make_async_copy(
            w_out_ref.at[pl.ds(h * HEAD, HEAD)], w_out_s.at[pl.ds(s * HEAD, HEAD)], sem.at[s]
        )
        for s, h in enumerate(head_order(part))
    ]


def layer_kernel(
    start_ref, len_ref, part_ref, core_ref, tokens_ref, half_hbm, att_hbm, gate_hbm, *rest
):
    near, far = rest[: HEADS - 1], rest[HEADS - 1 : 2 * HEADS - 2]
    w_out_ref, out_ref, state_ref = rest[2 * HEADS - 2 : 2 * HEADS + 1]
    x_s, half_s, att_s, gate_s, w_out_s, out_s, sem_in, sem_w, sem_out = rest[2 * HEADS + 1 :]
    low_is_near = core_ref[0] == 0
    first_id = part_ref[0] * MINE + RAW

    def loads(i):
        rows = pl.ds(i * WIN, WIN)
        pairs = ((half_hbm, half_s), (att_hbm, att_s), (gate_hbm, gate_s))
        return [
            pltpu.make_async_copy(a.at[rows], b.at[rows], sem_in.at[i, MAXB + j])
            for j, (a, b) in enumerate(pairs)
        ] + token_copies(tokens_ref, start_ref[0, first_id + i], x_s, i * WIN, sem_in.at[i])

    weights = w_out_copies(part_ref[0], w_out_ref, w_out_s, sem_w)

    def sends(i):
        at = (i % HALVES, slice(None), pl.ds((i // HALVES) * N_MP, N_MP))
        return pltpu.make_async_copy(out_s.at[at], out_ref.at[at], sem_out.at[i])

    for i in range(DONE):
        for copy in loads(i):
            copy.start()
        if i == GROUP - 1:
            for copy in weights:
                copy.start()

    def group(step, carry):
        first_user = step * GROUP
        for j in range(GROUP):
            for copy in loads(first_user + j):
                copy.wait()
        rows = pl.ds(pl.multiple_of(first_user * WIN, WIN), GROUP * WIN)

        def w_out_of():
            @pl.when(step == 0)
            def _():
                for copy in weights:
                    copy.wait()

            return w_out_s[...]

        both = mix(
            low_is_near,
            half_s[rows, :],
            (att_s[rows, :], gate_s[rows, :]),
            near,
            far,
            w_out_of,
            lambda: x_s[rows, :],
        )
        for j in range(GROUP):
            i = first_user + j
            length = len_ref[0, first_id + i]
            half_id = i % HALVES
            base = (i // HALVES) * N_MP
            mixed = live_rows(both[j * WIN : (j + 1) * WIN], length)
            for q in range(N_MP):
                out_s[half_id, :, base + q] = mixed[:, q * HEAD : (q + 1) * HEAD].reshape(
                    GROUPS, TILE, HEAD
                )
            sends(i).start()
            for q in range(N_MP):
                state_ref[i, :, q * HEAD : (q + 1) * HEAD] = last_row(
                    out_s[half_id, (length - 1) // TILE, base + q], length
                )
        return carry

    lax.fori_loop(0, DONE // GROUP, group, 0)
    for i in range(DONE):
        sends(i).wait()


def layer(tokens, starts, lengths, part, core, kept, near, far, w_out):
    message = (HALVES, GROUPS, MSG, TILE, HEAD)
    return pl.pallas_call(
        layer_kernel,
        grid_spec=pltpu.PrefetchScalarGridSpec(
            num_scalar_prefetch=4,
            grid=(1,),
            in_specs=[in_hbm()] * 4 + [in_vmem()] * (2 * HEADS - 2) + [in_hbm()],
            out_specs=[in_hbm(), in_vmem()],
            scratch_shapes=[
                pltpu.VMEM((DONE * WIN, D), BF16),
                pltpu.VMEM((DONE * WIN, D), BF16),
                pltpu.VMEM((DONE * WIN, HEAD), F32),
                pltpu.VMEM((DONE * WIN, HEAD), BF16),
                pltpu.VMEM((D, D), BF16),
                pltpu.VMEM((HALVES, GROUPS, ROUND * N_MP, TILE, HEAD), BF16),
                pltpu.SemaphoreType.DMA((DONE, 5)),
                pltpu.SemaphoreType.DMA((HEADS,)),
                pltpu.SemaphoreType.DMA((DONE,)),
            ],
        ),
        out_shape=[
            jax.ShapeDtypeStruct(message, BF16),
            jax.ShapeDtypeStruct((DONE, 1, D), BF16),
        ],
        name="layer",
    )(starts, lengths, part, core, tokens, *kept, *map(keep, near), *map(keep, far), w_out)


def raw_kernel(first_tile, len_ref, part_ref, core_ref, src_ref, w_own_ref, *rest):
    near, far = rest[: HEADS - 1], rest[HEADS - 1 : 2 * HEADS - 2]
    w_out_ref = rest[2 * HEADS - 2]
    pieces = rest[2 * HEADS - 1 : 2 * HEADS - 1 + N_MP]
    state_ref, x_s, w_out_s, mixed_s, sem_x, sem_w = rest[2 * HEADS - 1 + N_MP :]
    part = part_ref[0]
    lengths = [len_ref[0, part * MINE + k] for k in range(RAW)]
    loads = [
        pltpu.make_async_copy(
            src_ref.at[pl.ds(k * GROUPS, GROUPS), pl.ds(first_tile, N_MP)], x_s.at[k], sem_x.at[k]
        )
        for k in range(RAW)
    ]
    weights = w_out_copies(part, w_out_ref, w_out_s, sem_w)
    for copy in loads + weights:
        copy.start()
    for copy in loads:
        copy.wait()

    def x_rows():
        return rows_of(x_s[...])

    half = norm_half(x_rows().astype(F32))
    u, v, q, k = project([half], [w_own_ref[...]])

    def w_out_of():
        for copy in weights:
            copy.wait()
        return w_out_s[...]

    both = mix(
        core_ref[0] == 0, half, (attend_users(RAW, q, k, v), u), near, far, w_out_of, x_rows
    )
    for k in range(RAW):
        mixed = live_rows(both[k * WIN : (k + 1) * WIN], lengths[k])
        for q in range(N_MP):
            mixed_s[q, k] = mixed[:, q * HEAD : (q + 1) * HEAD].reshape(GROUPS, TILE, HEAD)
        for q in range(N_MP):
            state_ref[k, :, q * HEAD : (q + 1) * HEAD] = last_row(
                mixed_s[q, k, (lengths[k] - 1) // TILE], lengths[k]
            )
    for s in range(N_MP):
        pieces[s][...] = mixed_s[(part + s) % N_MP]


def raw_layer(source, first_tile, lengths, part, core, w_own, near, far, w_out):
    piece = jax.ShapeDtypeStruct((RAW, GROUPS, TILE, HEAD), BF16)
    outs = pl.pallas_call(
        lambda *refs: raw_kernel(first_tile, *refs),
        grid_spec=pltpu.PrefetchScalarGridSpec(
            num_scalar_prefetch=3,
            grid=(1,),
            in_specs=[in_hbm()] + [in_vmem()] * (2 * HEADS - 1) + [in_hbm()],
            out_specs=[in_vmem()] * (N_MP + 1),
            scratch_shapes=[
                pltpu.VMEM((RAW, GROUPS, N_MP, TILE, HEAD), BF16),
                pltpu.VMEM((D, D), BF16),
                pltpu.VMEM((N_MP, RAW, GROUPS, TILE, HEAD), BF16),
                pltpu.SemaphoreType.DMA((RAW,)),
                pltpu.SemaphoreType.DMA((HEADS,)),
            ],
        ),
        out_shape=[piece] * N_MP + [jax.ShapeDtypeStruct((RAW, 1, D), BF16)],
    )(lengths, part, core, source, w_own, *near, *far, w_out)
    return outs[:N_MP], outs[N_MP]


def merge_kernel(first_ref, in_ref, msg_ref, out_ref, sorted_s, table_v, table_s, sem):
    table = jnp.max(in_ref[:, N_MP].astype(F32), axis=1)
    table_v[...] = table.astype(jnp.int32)
    copy = pltpu.make_async_copy(table_v, table_s, sem.at[0])
    copy.start()
    copy.wait()
    first = first_ref[0]

    def one(d, carry):
        o = table_s[d, first]
        for q in range(N_MP):
            sorted_s[o, q] = in_ref[d, q]
        return carry

    lax.fori_loop(0, N_DP, one, 0, unroll=8)
    send = pltpu.make_async_copy(sorted_s, out_ref.at[:, pl.ds(ROUND * N_MP, N_MP)], sem.at[1])
    send.start()
    send.wait()


def merge(spread, first, message):
    return pl.pallas_call(
        merge_kernel,
        grid_spec=pltpu.PrefetchScalarGridSpec(
            num_scalar_prefetch=1,
            grid=(1,),
            in_specs=[in_vmem(), in_hbm()],
            out_specs=in_hbm(),
            scratch_shapes=[
                pltpu.VMEM((N_DP, N_MP, TILE, HEAD), BF16),
                pltpu.VMEM((N_DP, 128), jnp.int32),
                pltpu.SMEM((N_DP, 128), jnp.int32),
                pltpu.SemaphoreType.DMA((2,)),
            ],
        ),
        out_shape=jax.ShapeDtypeStruct((N_DP, MSG, TILE, HEAD), BF16),
        input_output_aliases={2: 0},
        name="merge",
    )(first, keep(spread), message)


def regroup_kernel(from_ref, in_ref, out_ref, out_s, sem):
    chunk = N_DP // CHUNKS

    def send(c):
        at = pl.ds(c * chunk, chunk)
        return pltpu.make_async_copy(out_s.at[at], out_ref.at[at], sem.at[c])

    def one(c, carry):
        for j in range(chunk):
            o = c * chunk + j
            for r in range(ROUND):
                d = from_ref[r * N_DP + o]
                for q in range(N_MP):
                    out_s[o, q, r] = in_ref[d, r * N_MP + q]
        send(c).start()
        return carry

    lax.fori_loop(0, CHUNKS, one, 0)
    for c in range(CHUNKS):
        send(c).wait()


def regroup(spread, source):
    shape = (N_DP, N_MP, ROUND, TILE, HEAD)
    return pl.pallas_call(
        regroup_kernel,
        grid_spec=pltpu.PrefetchScalarGridSpec(
            num_scalar_prefetch=1,
            grid=(1,),
            in_specs=[in_vmem()],
            out_specs=in_hbm(),
            scratch_shapes=[pltpu.VMEM(shape, BF16), pltpu.SemaphoreType.DMA((CHUNKS,))],
        ),
        out_shape=jax.ShapeDtypeStruct(shape, BF16),
        name="regroup",
    )(source, keep(spread))


def place_kernel(len_ref, off_ref, part_ref, in_ref, own_ref, *rest):
    out_ref, zero_v, used_s, own_s, sem, sem_own = rest[N_MP - 1 :]
    pieces = (own_s, *rest[: N_MP - 1])
    load = pltpu.make_async_copy(own_ref, own_s, sem_own)
    load.start()
    per_block = BLOCK // TILE
    zero_v[...] = jnp.zeros_like(zero_v)

    def clear(b, carry):
        used_s[b] = 0
        return carry

    lax.fori_loop(0, BLK_DEV, clear, 0, unroll=8)

    def send(u, source):
        def block(j):
            to = off_ref[u] + j
            used_s[to] = 1
            pltpu.make_async_copy(
                source(pl.ds(j * per_block, per_block)),
                out_ref.at[pl.ds(to * per_block, per_block)],
                sem,
            ).start()

        block(0)

        @pl.when(len_ref[u] > BLOCK)
        def _():
            block(1)

    def send_piece(s):
        m = (part_ref[0] + N_MP - s) % N_MP
        for k in range(RAW):
            send(m * MINE + k, lambda rows: pieces[s].at[k, rows])

    for s in range(1, N_MP):
        send_piece(s)

    def one(n, carry):
        m = n // DONE
        i = n % DONE
        send(m * MINE + RAW + i, lambda rows: in_ref.at[i % HALVES, rows, m, i // HALVES])
        return carry

    lax.fori_loop(0, N_MP * DONE, one, 0)
    load.wait()
    send_piece(0)

    def fill(b, carry):
        @pl.when(used_s[b] == 0)
        def _():
            pltpu.make_async_copy(zero_v, out_ref.at[pl.ds(b * per_block, per_block)], sem).start()

        return carry

    lax.fori_loop(0, BLK_DEV, fill, 0)
    pltpu.make_async_copy(out_ref, out_ref, sem).wait()


def place(arrived, pieces, lengths, offsets, part):
    rows = BLK_DEV * BLOCK
    return pl.pallas_call(
        place_kernel,
        grid_spec=pltpu.PrefetchScalarGridSpec(
            num_scalar_prefetch=3,
            grid=(1,),
            in_specs=[in_vmem(), in_hbm()] + [in_vmem()] * (N_MP - 1),
            out_specs=in_hbm(),
            scratch_shapes=[
                pltpu.VMEM((BLOCK // TILE, TILE, HEAD), BF16),
                pltpu.SMEM((BLK_DEV,), jnp.int32),
                pltpu.VMEM((RAW, GROUPS, TILE, HEAD), BF16),
                pltpu.SemaphoreType.DMA,
                pltpu.SemaphoreType.DMA,
            ],
        ),
        out_shape=jax.ShapeDtypeStruct((rows // TILE, TILE, HEAD), BF16),
        compiler_params=pltpu.CompilerParams(vmem_limit_bytes=32 * 1024 * 1024),
        name="place",
    )(lengths, offsets, part, keep(arrived), pltpu.with_memory_space_constraint(pieces[0], pltpu.HBM), *map(keep, pieces[1:])).reshape(rows, HEAD)


def along_mp(array, s):
    return lax.ppermute(array, "mp", [(i, (i + s) % N_MP) for i in range(N_MP)])


def per_device(tokens, w_uvqk, w_out, hist_len, owner, recv_offset, block_start):
    me = lax.axis_index("dp")
    part = lax.axis_index("mp")
    first = part * MINE
    core = me % 2
    half = me // GROUPS
    part_1, core_1 = part[None], core[None]

    raw, mine_rows = pack(
        tokens, block_start, part_1, core_1, w_uvqk, owner, hist_len, recv_offset
    )
    near, far = [], []
    for s in range(1, N_MP):
        near.append(along_mp(mine_rows, s))
    for s in range(1, N_MP):
        far.append(lax.ppermute(near[s - 1], "dp", [(i, i ^ 1) for i in range(N_DP)]))

    raw_in = lax.all_to_all(
        raw.reshape(N_DP, RAW_MSG * TILE, HEAD), "dp", 0, 0, tiled=True
    ).reshape(N_DP, RAW_MSG, TILE, HEAD)
    kept = own_head(tokens, block_start, part_1, w_uvqk)
    message, last = layer(
        tokens, block_start, hist_len, part_1, core_1, kept, near, far, w_out
    )
    message = merge(
        raw_in, (first + half)[None], message.reshape(N_DP, MSG, TILE, HEAD)
    )
    spread = lax.all_to_all(
        message.reshape(N_DP, MSG * TILE, HEAD), "dp", 0, 0, tiled=True
    ).reshape(N_DP, MSG, TILE, HEAD)
    _, raw_last = raw_layer(
        raw.reshape(N_DP, RAW_MSG, TILE, HEAD), 0, hist_len, part_1, core_1,
        w_uvqk, near, far, w_out,
    )

    table = raw_in[:, N_MP, 0, :].astype(jnp.int32)
    owners = table[:, :USERS]
    held = lax.dynamic_slice_in_dim(owners, first + RAW + half, HALVES * (ROUND - 1) + 1, 1)
    ids = jnp.arange(N_DP, dtype=jnp.int32)
    source = jnp.sum(
        jnp.where(held[:, ::HALVES].T[:, None, :] == ids[None, :, None], ids[None, None, :], 0), axis=2
    ).reshape(-1)
    mine = owners == me
    recv_len = jnp.sum(jnp.where(mine, table[:, USERS : 2 * USERS], 0), axis=0)
    recv_off = jnp.sum(jnp.where(mine, table[:, 2 * USERS : 3 * USERS], 0), axis=0)

    sorted_rows = regroup(spread, source)
    arrived = lax.all_to_all(
        sorted_rows.reshape(N_DP * N_MP, ROUND * TILE, HEAD), ("dp", "mp"), 0, 0, tiled=True
    )
    pieces, _ = raw_layer(
        spread, ROUND * N_MP, recv_len[None], part_1, core_1,
        w_uvqk, near, far, w_out,
    )
    pieces = [pieces[0]] + [along_mp(pieces[s], s) for s in range(1, N_MP)]
    packed = place(
        arrived.reshape(HALVES, GROUPS, N_MP, ROUND, TILE, HEAD),
        pieces, recv_len, recv_off, part_1,
    )

    columns = jnp.concatenate([raw_last, last], axis=0).reshape(MINE, N_MP, HEAD)
    state = jnp.zeros((N_MP, MINE, HEAD), BF16)
    for s in range(N_MP):
        to_part = (part + s) % N_MP
        piece = lax.dynamic_slice_in_dim(columns, to_part, 1, 1)[:, 0]
        if s:
            piece = along_mp(piece, s)
        state = lax.dynamic_update_slice_in_dim(state, piece[None], (part - s) % N_MP, 0)
    return packed, state.reshape(USERS, HEAD)


def solution(mesh):
    in_specs = (
        P("dp", None),
        P(None, "mp"),
        P(),
        P("dp", None),
        P("dp", None),
        P("dp", None),
        P("dp", None),
    )
    out_specs = (P("dp", "mp"), P("dp", "mp"))
    return jax.shard_map(
        per_device, mesh=mesh, in_specs=in_specs, out_specs=out_specs, check_vma=False
    )
```

```python
import jax
import jax.numpy as jnp
from jax import lax
from jax.experimental import pallas as pl
from jax.experimental.pallas import tpu as pltpu
from jax.sharding import PartitionSpec as P

D = 512
HEADS = 4
HEAD = D // HEADS
BLOCK = 128
MAXB = 2
BLK_DEV = 48
USERS = 24
N_DP = 64
N_MP = 4
WIN = MAXB * BLOCK
MINE = USERS // N_MP
RAW = 2
DONE = MINE - RAW
TILE = 8
GROUPS = WIN // TILE
HALVES = N_DP // GROUPS
GROUP = 2
OWN_GROUP = 2
CHUNKS = 4
SEATS = list(range(N_DP - 1, -1, -1))
RAW_MSG = N_MP + 1
ROUND = DONE // HALVES
MSG = (ROUND + 1) * N_MP
EPS = 1e-05
BF16 = jnp.bfloat16
F32 = jnp.float32


def silu_of_twice(h):
    return h + h * jnp.tanh(h)


def project(half_parts, w_parts):
    acc = jnp.dot(half_parts[0], w_parts[0], preferred_element_type=F32)
    for n, w in zip(half_parts[1:], w_parts[1:]):
        acc = acc + jnp.dot(n, w, preferred_element_type=F32)
    proj = silu_of_twice(acc).astype(BF16)
    return [proj[:, j * HEAD : (j + 1) * HEAD] for j in range(4)]


def attend(q, k, v):
    row = lax.broadcasted_iota(jnp.int32, (BLOCK, BLOCK), 0)
    col = lax.broadcasted_iota(jnp.int32, (BLOCK, BLOCK), 1)
    causal = col <= row
    scale = 0.5 * HEAD ** (-0.5)
    contract_last = (((1,), (1,)), ((), ()))
    s0 = lax.dot_general(q[:BLOCK], k[:BLOCK], contract_last, preferred_element_type=F32)
    s1 = lax.dot_general(q[BLOCK:], k, contract_last, preferred_element_type=F32)
    a0 = jnp.where(causal, silu_of_twice(s0 * scale), 0.0).astype(BF16)
    b = silu_of_twice(s1 * scale)
    a1 = jnp.concatenate(
        [b[:, :BLOCK].astype(BF16), jnp.where(causal, b[:, BLOCK:], 0.0).astype(BF16)], axis=1
    )
    return jnp.concatenate(
        [
            jnp.dot(a0, v[:BLOCK], preferred_element_type=F32),
            jnp.dot(a1, v, preferred_element_type=F32),
        ],
        axis=0,
    )


def norm_stats(total, squares, unit=1.0):
    mean = total * (1.0 / D)
    var = squares * (1.0 / D) - mean * mean
    return mean, lax.rsqrt(var * (unit * unit) + EPS) * unit


def token_copies(tokens_ref, block, x_ref, row, sem):
    second = jnp.minimum(block + 1, BLK_DEV - 1)
    return [
        pltpu.make_async_copy(
            tokens_ref.at[pl.ds(b * BLOCK, BLOCK)],
            x_ref.at[pl.ds(row + j * BLOCK, BLOCK)],
            sem.at[j],
        )
        for j, b in enumerate((block, second))
    ]


def norm_half(x):
    mean, inv = norm_stats(
        jnp.sum(x, axis=1, keepdims=True), jnp.sum(x * x, axis=1, keepdims=True)
    )
    return ((x - mean) * (inv * 0.5)).astype(BF16)


def own_head_kernel(
    start_ref, part_ref, tokens_ref, w_ref, half_ref, att_ref, gate_ref,
    x_s, half_s, att_s, gate_s, w_s, sem_in, sem_w, sem_out,
):
    load_w = pltpu.make_async_copy(w_ref, w_s, sem_w)

    def loads(i):
        block = start_ref[0, part_ref[0] * MINE + RAW + i]
        return token_copies(tokens_ref, block, x_s, i * WIN, sem_in.at[i])

    def sends(step):
        rows = pl.ds(step * OWN_GROUP * WIN, OWN_GROUP * WIN)
        pairs = ((half_s, half_ref), (att_s, att_ref), (gate_s, gate_ref))
        return [
            pltpu.make_async_copy(a.at[rows], b.at[rows], sem_out.at[step, j])
            for j, (a, b) in enumerate(pairs)
        ]

    for i in range(DONE):
        for copy in loads(i):
            copy.start()
        if i == OWN_GROUP - 1:
            load_w.start()

    def group(step, carry):
        for j in range(OWN_GROUP):
            for copy in loads(step * OWN_GROUP + j):
                copy.wait()
        rows = pl.ds(pl.multiple_of(step * OWN_GROUP * WIN, WIN), OWN_GROUP * WIN)
        half = norm_half(x_s[rows, :].astype(F32))
        half_s[rows, :] = half

        @pl.when(step == 0)
        def _():
            load_w.wait()

        u, v, q, k = project([half], [w_s[...]])
        gate_s[rows, :] = u
        att_s[rows, :] = attend_users(OWN_GROUP, q, k, v)
        for copy in sends(step):
            copy.start()
        return carry

    lax.fori_loop(0, DONE // OWN_GROUP, group, 0)
    for step in range(DONE // OWN_GROUP):
        for copy in sends(step):
            copy.wait()


def in_vmem():
    return pl.BlockSpec(memory_space=pltpu.VMEM)


def in_hbm():
    return pl.BlockSpec(memory_space=pltpu.HBM)


def keep(array):
    return pltpu.with_memory_space_constraint(array, pltpu.VMEM)


def own_head(tokens, starts, part, w_own):
    kept = [((DONE * WIN, D), BF16), ((DONE * WIN, HEAD), F32), ((DONE * WIN, HEAD), BF16)]
    return pl.pallas_call(
        own_head_kernel,
        grid_spec=pltpu.PrefetchScalarGridSpec(
            num_scalar_prefetch=2,
            grid=(1,),
            in_specs=[in_hbm()] * 2,
            out_specs=[in_hbm()] * 3,
            scratch_shapes=[pltpu.VMEM((DONE * WIN, D), BF16)]
            + [pltpu.VMEM(*k) for k in kept]
            + [
                pltpu.VMEM((D, D), BF16),
                pltpu.SemaphoreType.DMA((DONE, MAXB)),
                pltpu.SemaphoreType.DMA,
                pltpu.SemaphoreType.DMA((DONE // OWN_GROUP, 3)),
            ],
        ),
        out_shape=[jax.ShapeDtypeStruct(*k) for k in kept],
        cost_estimate=pl.CostEstimate(
            flops=DONE * WIN * D * D * 64, bytes_accessed=DONE * WIN * D * 8, transcendentals=0
        ),
        name="own_head",
    )(starts, part, tokens, w_own)


def rows_of(tiles):
    return jnp.concatenate(
        [tiles[..., q, :, :].reshape(-1, HEAD) for q in range(N_MP)], axis=1
    )


def pack_kernel(
    start_ref, part_ref, core_ref, tokens_ref, w_ref, owner_ref, len_ref, off_ref,
    out_ref, rows_ref, x_s, table_s, row_s, out_s, sem, sem_t, sem_w, sem_out,
):
    tables = [
        pltpu.make_async_copy(ref, table_s.at[j], sem_t.at[j])
        for j, ref in enumerate((owner_ref, len_ref, off_ref))
    ]
    half = D // 2
    weights = pltpu.make_async_copy(w_ref.at[pl.ds(core_ref[0] * half, half)], rows_ref, sem_w)
    loads = [
        token_copies(
            tokens_ref, start_ref[0, part_ref[0] * MINE + k], x_s, k * WIN, sem.at[k]
        )
        for k in range(RAW)
    ]
    for copy in tables + loads[0] + [weights] + loads[1]:
        copy.start()
    row_s[...] = jnp.zeros_like(row_s)
    for j, copy in enumerate(tables):
        copy.wait()
        row_s[:, j * USERS : (j + 1) * USERS] = table_s[j] if j else N_DP - 1 - table_s[j]
    tile = jnp.broadcast_to(row_s[...], (TILE, 128)).astype(F32).astype(BF16)
    for k in range(RAW):
        out_s[k, :, N_MP] = jnp.broadcast_to(tile[None], (GROUPS, TILE, 128))
    sends = [pltpu.make_async_copy(out_s.at[k], out_ref.at[k], sem_out.at[k]) for k in range(RAW)]
    for k in range(RAW):
        for copy in loads[k]:
            copy.wait()
        for q in range(N_MP):
            out_s[k, :, q] = x_s[k * WIN : (k + 1) * WIN, q * HEAD : (q + 1) * HEAD].reshape(
                GROUPS, TILE, HEAD
            )
        sends[k].start()
    weights.wait()
    for copy in sends:
        copy.wait()


def pack(tokens, starts, part, core, w_own, owner, hist_len, recv_offset):
    shape = (RAW, GROUPS, RAW_MSG, TILE, HEAD)
    return pl.pallas_call(
        pack_kernel,
        grid_spec=pltpu.PrefetchScalarGridSpec(
            num_scalar_prefetch=3,
            grid=(1,),
            in_specs=[in_hbm()] * 5,
            out_specs=[in_hbm(), in_vmem()],
            scratch_shapes=[
                pltpu.VMEM((RAW * WIN, D), BF16),
                pltpu.VMEM((3, 1, USERS), jnp.int32),
                pltpu.VMEM((1, 128), jnp.int32),
                pltpu.VMEM(shape, BF16),
                pltpu.SemaphoreType.DMA((RAW, MAXB)),
                pltpu.SemaphoreType.DMA((3,)),
                pltpu.SemaphoreType.DMA,
                pltpu.SemaphoreType.DMA((RAW,)),
            ],
        ),
        out_shape=[jax.ShapeDtypeStruct(shape, BF16), pltpu.VMEM((D // 2, D), BF16)],
        name="pack",
    )(starts, part, core, tokens, w_own, owner, hist_len, recv_offset)


def head_order(part):
    return [part] + [(part + HEADS - s) % HEADS for s in range(1, HEADS)]


def mix(low_is_near, half_rows, first, near, far, w_out_of, x_rows):
    low = half_rows[:, : D // 2]
    high = half_rows[:, D // 2 :]
    parts = [jnp.where(low_is_near, low, high), jnp.where(low_is_near, high, low)]
    users = half_rows.shape[0] // WIN
    heads, gates = [first[0]], [first[1]]
    for near_ref, far_ref in zip(near, far):
        u, v, q, k = project(parts, [near_ref[...], far_ref[...]])
        gates.append(u)
        heads.append(attend_users(users, q, k, v))
    total = jnp.sum(heads[0] + heads[1] + (heads[2] + heads[3]), axis=1, keepdims=True)
    squares = jnp.sum(
        heads[0] * heads[0] + heads[1] * heads[1] + (heads[2] * heads[2] + heads[3] * heads[3]),
        axis=1,
        keepdims=True,
    )
    mean, inv = norm_stats(total, squares, 1.0 / WIN)
    gated = jnp.concatenate(
        [((a - mean) * inv * g.astype(F32)).astype(BF16) for a, g in zip(heads, gates)], axis=1
    )
    return jnp.dot(gated, w_out_of(), preferred_element_type=F32) + x_rows().astype(F32)


def attend_users(users, q, k, v):
    return jnp.concatenate(
        [attend(*(t[j * WIN : (j + 1) * WIN] for t in (q, k, v))) for j in range(users)], axis=0
    )


def live_rows(mixed, length):
    at = lax.broadcasted_iota(jnp.int32, (WIN, 1), 0)
    return jnp.where(at < length, mixed, 0.0).astype(BF16)


def last_row(tile, length):
    pick = lax.broadcasted_iota(jnp.int32, (TILE, HEAD), 0) == (length - 1) % TILE
    return jnp.sum(jnp.where(pick, tile.astype(F32), 0.0), axis=0, keepdims=True).astype(BF16)


def w_out_copies(part, w_out_ref, w_out_s, sem):
    return [
        pltpu.make_async_copy(
            w_out_ref.at[pl.ds(h * HEAD, HEAD)], w_out_s.at[pl.ds(s * HEAD, HEAD)], sem.at[s]
        )
        for s, h in enumerate(head_order(part))
    ]


def layer_kernel(
    start_ref, len_ref, part_ref, core_ref, tokens_ref, half_hbm, att_hbm, gate_hbm, *rest
):
    near, far = rest[: HEADS - 1], rest[HEADS - 1 : 2 * HEADS - 2]
    w_out_ref, out_ref, state_ref = rest[2 * HEADS - 2 : 2 * HEADS + 1]
    x_s, half_s, att_s, gate_s, w_out_s, out_s, sem_in, sem_w, sem_out = rest[2 * HEADS + 1 :]
    low_is_near = core_ref[0] == 0
    first_id = part_ref[0] * MINE + RAW

    def loads(i):
        rows = pl.ds(i * WIN, WIN)
        pairs = ((half_hbm, half_s), (att_hbm, att_s), (gate_hbm, gate_s))
        return [
            pltpu.make_async_copy(a.at[rows], b.at[rows], sem_in.at[i, MAXB + j])
            for j, (a, b) in enumerate(pairs)
        ] + token_copies(tokens_ref, start_ref[0, first_id + i], x_s, i * WIN, sem_in.at[i])

    weights = w_out_copies(part_ref[0], w_out_ref, w_out_s, sem_w)

    def sends(i):
        at = (i % HALVES, slice(None), pl.ds((i // HALVES) * N_MP, N_MP))
        return pltpu.make_async_copy(out_s.at[at], out_ref.at[at], sem_out.at[i])

    for i in range(DONE):
        for copy in loads(i):
            copy.start()
        if i == GROUP - 1:
            for copy in weights:
                copy.start()

    def group(step, carry):
        first_user = step * GROUP
        for j in range(GROUP):
            for copy in loads(first_user + j):
                copy.wait()
        rows = pl.ds(pl.multiple_of(first_user * WIN, WIN), GROUP * WIN)

        def w_out_of():
            @pl.when(step == 0)
            def _():
                for copy in weights:
                    copy.wait()

            return w_out_s[...]

        both = mix(
            low_is_near,
            half_s[rows, :],
            (att_s[rows, :], gate_s[rows, :]),
            near,
            far,
            w_out_of,
            lambda: x_s[rows, :],
        )
        for j in range(GROUP):
            i = first_user + j
            length = len_ref[0, first_id + i]
            half_id = i % HALVES
            base = (i // HALVES) * N_MP
            mixed = live_rows(both[j * WIN : (j + 1) * WIN], length)
            for q in range(N_MP):
                out_s[half_id, :, base + q] = mixed[:, q * HEAD : (q + 1) * HEAD].reshape(
                    GROUPS, TILE, HEAD
                )
            sends(i).start()
            for q in range(N_MP):
                state_ref[i, :, q * HEAD : (q + 1) * HEAD] = last_row(
                    out_s[half_id, (length - 1) // TILE, base + q], length
                )
        return carry

    lax.fori_loop(0, DONE // GROUP, group, 0)
    for i in range(DONE):
        sends(i).wait()


def layer(tokens, starts, lengths, part, core, kept, near, far, w_out):
    message = (HALVES, GROUPS, MSG, TILE, HEAD)
    return pl.pallas_call(
        layer_kernel,
        grid_spec=pltpu.PrefetchScalarGridSpec(
            num_scalar_prefetch=4,
            grid=(1,),
            in_specs=[in_hbm()] * 4 + [in_vmem()] * (2 * HEADS - 2) + [in_hbm()],
            out_specs=[in_hbm(), in_vmem()],
            scratch_shapes=[
                pltpu.VMEM((DONE * WIN, D), BF16),
                pltpu.VMEM((DONE * WIN, D), BF16),
                pltpu.VMEM((DONE * WIN, HEAD), F32),
                pltpu.VMEM((DONE * WIN, HEAD), BF16),
                pltpu.VMEM((D, D), BF16),
                pltpu.VMEM((HALVES, GROUPS, ROUND * N_MP, TILE, HEAD), BF16),
                pltpu.SemaphoreType.DMA((DONE, 5)),
                pltpu.SemaphoreType.DMA((HEADS,)),
                pltpu.SemaphoreType.DMA((DONE,)),
            ],
        ),
        out_shape=[
            jax.ShapeDtypeStruct(message, BF16),
            jax.ShapeDtypeStruct((DONE, 1, D), BF16),
        ],
        name="layer",
    )(starts, lengths, part, core, tokens, *kept, *map(keep, near), *map(keep, far), w_out)


def raw_kernel(first_tile, len_ref, part_ref, core_ref, src_ref, w_own_ref, *rest):
    near, far = rest[: HEADS - 1], rest[HEADS - 1 : 2 * HEADS - 2]
    w_out_ref = rest[2 * HEADS - 2]
    pieces = rest[2 * HEADS - 1 : 2 * HEADS - 1 + N_MP]
    state_ref, x_s, w_out_s, mixed_s, sem_x, sem_w = rest[2 * HEADS - 1 + N_MP :]
    part = part_ref[0]
    lengths = [len_ref[0, part * MINE + k] for k in range(RAW)]
    loads = [
        pltpu.make_async_copy(
            src_ref.at[pl.ds(k * GROUPS, GROUPS), pl.ds(first_tile, N_MP)], x_s.at[k], sem_x.at[k]
        )
        for k in range(RAW)
    ]
    weights = w_out_copies(part, w_out_ref, w_out_s, sem_w)
    for copy in loads + weights:
        copy.start()
    for copy in loads:
        copy.wait()

    def x_rows():
        return rows_of(x_s[...])

    half = norm_half(x_rows().astype(F32))
    u, v, q, k = project([half], [w_own_ref[...]])

    def w_out_of():
        for copy in weights:
            copy.wait()
        return w_out_s[...]

    both = mix(
        core_ref[0] == 0, half, (attend_users(RAW, q, k, v), u), near, far, w_out_of, x_rows
    )
    for k in range(RAW):
        mixed = live_rows(both[k * WIN : (k + 1) * WIN], lengths[k])
        for q in range(N_MP):
            mixed_s[q, k] = mixed[:, q * HEAD : (q + 1) * HEAD].reshape(GROUPS, TILE, HEAD)
        for q in range(N_MP):
            state_ref[k, :, q * HEAD : (q + 1) * HEAD] = last_row(
                mixed_s[q, k, (lengths[k] - 1) // TILE], lengths[k]
            )
    for s in range(N_MP):
        pieces[s][...] = mixed_s[(part + s) % N_MP]


def raw_layer(source, first_tile, lengths, part, core, w_own, near, far, w_out):
    piece = jax.ShapeDtypeStruct((RAW, GROUPS, TILE, HEAD), BF16)
    outs = pl.pallas_call(
        lambda *refs: raw_kernel(first_tile, *refs),
        grid_spec=pltpu.PrefetchScalarGridSpec(
            num_scalar_prefetch=3,
            grid=(1,),
            in_specs=[in_hbm()] + [in_vmem()] * (2 * HEADS - 1) + [in_hbm()],
            out_specs=[in_vmem()] * (N_MP + 1),
            scratch_shapes=[
                pltpu.VMEM((RAW, GROUPS, N_MP, TILE, HEAD), BF16),
                pltpu.VMEM((D, D), BF16),
                pltpu.VMEM((N_MP, RAW, GROUPS, TILE, HEAD), BF16),
                pltpu.SemaphoreType.DMA((RAW,)),
                pltpu.SemaphoreType.DMA((HEADS,)),
            ],
        ),
        out_shape=[piece] * N_MP + [jax.ShapeDtypeStruct((RAW, 1, D), BF16)],
    )(lengths, part, core, source, w_own, *near, *far, w_out)
    return outs[:N_MP], outs[N_MP]


def merge_kernel(first_ref, in_ref, msg_ref, out_ref, sorted_s, table_v, table_s, sem):
    table = jnp.max(in_ref[:, N_MP].astype(F32), axis=1)
    table_v[...] = table.astype(jnp.int32)
    copy = pltpu.make_async_copy(table_v, table_s, sem.at[0])
    copy.start()
    copy.wait()
    first = first_ref[0]

    def one(d, carry):
        o = table_s[d, first]
        for q in range(N_MP):
            sorted_s[o, q] = in_ref[d, q]
        return carry

    lax.fori_loop(0, N_DP, one, 0, unroll=8)
    send = pltpu.make_async_copy(sorted_s, out_ref.at[:, pl.ds(ROUND * N_MP, N_MP)], sem.at[1])
    send.start()
    send.wait()


def merge(spread, first, message):
    return pl.pallas_call(
        merge_kernel,
        grid_spec=pltpu.PrefetchScalarGridSpec(
            num_scalar_prefetch=1,
            grid=(1,),
            in_specs=[in_vmem(), in_hbm()],
            out_specs=in_hbm(),
            scratch_shapes=[
                pltpu.VMEM((N_DP, N_MP, TILE, HEAD), BF16),
                pltpu.VMEM((N_DP, 128), jnp.int32),
                pltpu.SMEM((N_DP, 128), jnp.int32),
                pltpu.SemaphoreType.DMA((2,)),
            ],
        ),
        out_shape=jax.ShapeDtypeStruct((N_DP, MSG, TILE, HEAD), BF16),
        input_output_aliases={2: 0},
        name="merge",
    )(first, keep(spread), message)


def regroup_kernel(from_ref, in_ref, out_ref, out_s, sem):
    chunk = N_DP // CHUNKS

    def send(c):
        at = pl.ds(c * chunk, chunk)
        return pltpu.make_async_copy(out_s.at[at], out_ref.at[at], sem.at[c])

    def one(c, carry):
        for j in range(chunk):
            o = c * chunk + j
            for r in range(ROUND):
                d = from_ref[r * N_DP + o]
                for q in range(N_MP):
                    out_s[o, q, r] = in_ref[d, r * N_MP + q]
        send(c).start()
        return carry

    lax.fori_loop(0, CHUNKS, one, 0)
    for c in range(CHUNKS):
        send(c).wait()


def regroup(spread, source):
    shape = (N_DP, N_MP, ROUND, TILE, HEAD)
    return pl.pallas_call(
        regroup_kernel,
        grid_spec=pltpu.PrefetchScalarGridSpec(
            num_scalar_prefetch=1,
            grid=(1,),
            in_specs=[in_vmem()],
            out_specs=in_hbm(),
            scratch_shapes=[pltpu.VMEM(shape, BF16), pltpu.SemaphoreType.DMA((CHUNKS,))],
        ),
        out_shape=jax.ShapeDtypeStruct(shape, BF16),
        name="regroup",
    )(source, keep(spread))


def place_kernel(len_ref, off_ref, part_ref, in_ref, own_ref, *rest):
    out_ref, zero_v, used_s, own_s, sem, sem_own = rest[N_MP - 1 :]
    pieces = (own_s, *rest[: N_MP - 1])
    load = pltpu.make_async_copy(own_ref, own_s, sem_own)
    load.start()
    per_block = BLOCK // TILE
    zero_v[...] = jnp.zeros_like(zero_v)

    def clear(b, carry):
        used_s[b] = 0
        return carry

    lax.fori_loop(0, BLK_DEV, clear, 0, unroll=8)

    def send(u, source):
        def block(j):
            to = off_ref[u] + j
            used_s[to] = 1
            pltpu.make_async_copy(
                source(pl.ds(j * per_block, per_block)),
                out_ref.at[pl.ds(to * per_block, per_block)],
                sem,
            ).start()

        block(0)

        @pl.when(len_ref[u] > BLOCK)
        def _():
            block(1)

    def send_piece(s):
        m = (part_ref[0] + N_MP - s) % N_MP
        for k in range(RAW):
            send(m * MINE + k, lambda rows: pieces[s].at[k, rows])

    for s in range(1, N_MP):
        send_piece(s)

    def one(n, carry):
        m = n // DONE
        i = n % DONE
        send(m * MINE + RAW + i, lambda rows: in_ref.at[i % HALVES, rows, m, i // HALVES])
        return carry

    lax.fori_loop(0, N_MP * DONE, one, 0)
    load.wait()
    send_piece(0)

    def fill(b, carry):
        @pl.when(used_s[b] == 0)
        def _():
            pltpu.make_async_copy(zero_v, out_ref.at[pl.ds(b * per_block, per_block)], sem).start()

        return carry

    lax.fori_loop(0, BLK_DEV, fill, 0)
    pltpu.make_async_copy(out_ref, out_ref, sem).wait()


def place(arrived, pieces, lengths, offsets, part):
    rows = BLK_DEV * BLOCK
    return pl.pallas_call(
        place_kernel,
        grid_spec=pltpu.PrefetchScalarGridSpec(
            num_scalar_prefetch=3,
            grid=(1,),
            in_specs=[in_vmem(), in_hbm()] + [in_vmem()] * (N_MP - 1),
            out_specs=in_hbm(),
            scratch_shapes=[
                pltpu.VMEM((BLOCK // TILE, TILE, HEAD), BF16),
                pltpu.SMEM((BLK_DEV,), jnp.int32),
                pltpu.VMEM((RAW, GROUPS, TILE, HEAD), BF16),
                pltpu.SemaphoreType.DMA,
                pltpu.SemaphoreType.DMA,
            ],
        ),
        out_shape=jax.ShapeDtypeStruct((rows // TILE, TILE, HEAD), BF16),
        compiler_params=pltpu.CompilerParams(vmem_limit_bytes=32 * 1024 * 1024),
        name="place",
    )(lengths, offsets, part, keep(arrived), pltpu.with_memory_space_constraint(pieces[0], pltpu.HBM), *map(keep, pieces[1:])).reshape(rows, HEAD)


def along_mp(array, s):
    return lax.ppermute(array, "mp", [(i, (i + s) % N_MP) for i in range(N_MP)])


def per_device(tokens, w_uvqk, w_out, hist_len, owner, recv_offset, block_start):
    me = lax.axis_index("dp")
    part = lax.axis_index("mp")
    first = part * MINE
    core = me % 2
    seat = N_DP - 1 - me
    half = seat // GROUPS
    part_1, core_1 = part[None], core[None]

    raw, mine_rows = pack(
        tokens, block_start, part_1, core_1, w_uvqk, owner, hist_len, recv_offset
    )
    near, far = [], []
    for s in range(1, N_MP):
        near.append(along_mp(mine_rows, s))
    for s in range(1, N_MP):
        far.append(lax.ppermute(near[s - 1], "dp", [(i, i ^ 1) for i in range(N_DP)]))

    raw_in = lax.all_to_all(
        raw.reshape(N_DP, RAW_MSG * TILE, HEAD), "dp", 0, 0, axis_index_groups=[SEATS], tiled=True
    ).reshape(N_DP, RAW_MSG, TILE, HEAD)
    kept = own_head(tokens, block_start, part_1, w_uvqk)
    message, last = layer(
        tokens, block_start, hist_len, part_1, core_1, kept, near, far, w_out
    )
    message = merge(
        raw_in, (first + half)[None], message.reshape(N_DP, MSG, TILE, HEAD)
    )
    spread = lax.all_to_all(
        message.reshape(N_DP, MSG * TILE, HEAD), "dp", 0, 0, axis_index_groups=[SEATS], tiled=True
    ).reshape(N_DP, MSG, TILE, HEAD)
    _, raw_last = raw_layer(
        raw.reshape(N_DP, RAW_MSG, TILE, HEAD), 0, hist_len, part_1, core_1,
        w_uvqk, near, far, w_out,
    )

    table = raw_in[:, N_MP, 0, :].astype(jnp.int32)
    owners = table[:, :USERS]
    held = lax.dynamic_slice_in_dim(owners, first + RAW + half, HALVES * (ROUND - 1) + 1, 1)
    ids = jnp.arange(N_DP, dtype=jnp.int32)
    source = jnp.sum(
        jnp.where(held[:, ::HALVES].T[:, None, :] == ids[None, :, None], ids[None, None, :], 0), axis=2
    ).reshape(-1)
    mine = owners == seat
    recv_len = jnp.sum(jnp.where(mine, table[:, USERS : 2 * USERS], 0), axis=0)
    recv_off = jnp.sum(jnp.where(mine, table[:, 2 * USERS : 3 * USERS], 0), axis=0)

    sorted_rows = regroup(spread, source)
    arrived = lax.all_to_all(
        sorted_rows.reshape(N_DP * N_MP, ROUND * TILE, HEAD), ("dp", "mp"), 0, 0,
        axis_index_groups=[[d * N_MP + m for d in SEATS for m in range(N_MP)]], tiled=True
    )
    pieces, _ = raw_layer(
        spread, ROUND * N_MP, recv_len[None], part_1, core_1,
        w_uvqk, near, far, w_out,
    )
    pieces = [pieces[0]] + [along_mp(pieces[s], s) for s in range(1, N_MP)]
    packed = place(
        arrived.reshape(HALVES, GROUPS, N_MP, ROUND, TILE, HEAD),
        pieces, recv_len, recv_off, part_1,
    )

    columns = jnp.concatenate([raw_last, last], axis=0).reshape(MINE, N_MP, HEAD)
    state = jnp.zeros((N_MP, MINE, HEAD), BF16)
    for s in range(N_MP):
        to_part = (part + s) % N_MP
        piece = lax.dynamic_slice_in_dim(columns, to_part, 1, 1)[:, 0]
        if s:
            piece = along_mp(piece, s)
        state = lax.dynamic_update_slice_in_dim(state, piece[None], (part - s) % N_MP, 0)
    return packed, state.reshape(USERS, HEAD)


def solution(mesh):
    in_specs = (
        P("dp", None),
        P(None, "mp"),
        P(),
        P("dp", None),
        P("dp", None),
        P("dp", None),
        P("dp", None),
    )
    out_specs = (P("dp", "mp"), P("dp", "mp"))
    return jax.shard_map(
        per_device, mesh=mesh, in_specs=in_specs, out_specs=out_specs, check_vma=False
    )
```

```python
import jax
import jax.numpy as jnp
from jax import lax
from jax.experimental import pallas as pl
from jax.experimental.pallas import tpu as pltpu
from jax.sharding import PartitionSpec as P

D = 512
HEADS = 4
HEAD = D // HEADS
BLOCK = 128
MAXB = 2
BLK_DEV = 48
USERS = 24
N_DP = 64
N_MP = 4
WIN = MAXB * BLOCK
MINE = USERS // N_MP
RAW = 2
DONE = MINE - RAW
TILE = 8
GROUPS = WIN // TILE
HALVES = N_DP // GROUPS
GROUP = 2
OWN_GROUP = 2
CHUNKS = 4
SEATS = list(range(N_DP - 1, -1, -1))
RAW_MSG = N_MP + 1
ROUND = DONE // HALVES
MSG = (ROUND + 1) * N_MP
EPS = 1e-05
BF16 = jnp.bfloat16
F32 = jnp.float32


def silu_of_twice(h):
    return h + h * jnp.tanh(h)


def project(half_parts, w_parts):
    acc = jnp.dot(half_parts[0], w_parts[0], preferred_element_type=F32)
    for n, w in zip(half_parts[1:], w_parts[1:]):
        acc = acc + jnp.dot(n, w, preferred_element_type=F32)
    proj = silu_of_twice(acc).astype(BF16)
    return [proj[:, j * HEAD : (j + 1) * HEAD] for j in range(4)]


def attend(q, k, v):
    row = lax.broadcasted_iota(jnp.int32, (BLOCK, BLOCK), 0)
    col = lax.broadcasted_iota(jnp.int32, (BLOCK, BLOCK), 1)
    causal = col <= row
    scale = 0.5 * HEAD ** (-0.5)
    contract_last = (((1,), (1,)), ((), ()))
    s0 = lax.dot_general(q[:BLOCK], k[:BLOCK], contract_last, preferred_element_type=F32)
    s1 = lax.dot_general(q[BLOCK:], k, contract_last, preferred_element_type=F32)
    a0 = jnp.where(causal, silu_of_twice(s0 * scale), 0.0).astype(BF16)
    b = silu_of_twice(s1 * scale)
    a1 = jnp.concatenate(
        [b[:, :BLOCK].astype(BF16), jnp.where(causal, b[:, BLOCK:], 0.0).astype(BF16)], axis=1
    )
    return jnp.concatenate(
        [
            jnp.dot(a0, v[:BLOCK], preferred_element_type=F32),
            jnp.dot(a1, v, preferred_element_type=F32),
        ],
        axis=0,
    )


def norm_stats(total, squares, unit=1.0):
    mean = total * (1.0 / D)
    var = squares * (1.0 / D) - mean * mean
    return mean, lax.rsqrt(var * (unit * unit) + EPS) * unit


def token_copies(tokens_ref, block, x_ref, row, sem):
    second = jnp.minimum(block + 1, BLK_DEV - 1)
    return [
        pltpu.make_async_copy(
            tokens_ref.at[pl.ds(b * BLOCK, BLOCK)],
            x_ref.at[pl.ds(row + j * BLOCK, BLOCK)],
            sem.at[j],
        )
        for j, b in enumerate((block, second))
    ]


def norm_half(x):
    mean, inv = norm_stats(
        jnp.sum(x, axis=1, keepdims=True), jnp.sum(x * x, axis=1, keepdims=True)
    )
    return ((x - mean) * (inv * 0.5)).astype(BF16)


def own_head_kernel(
    start_ref, part_ref, tokens_ref, w_ref, half_ref, att_ref, gate_ref,
    x_s, half_s, att_s, gate_s, w_s, sem_in, sem_w, sem_out,
):
    load_w = pltpu.make_async_copy(w_ref, w_s, sem_w)

    def loads(i):
        block = start_ref[0, part_ref[0] * MINE + RAW + i]
        return token_copies(tokens_ref, block, x_s, i * WIN, sem_in.at[i])

    def sends(step):
        rows = pl.ds(step * OWN_GROUP * WIN, OWN_GROUP * WIN)
        pairs = ((half_s, half_ref), (att_s, att_ref), (gate_s, gate_ref))
        return [
            pltpu.make_async_copy(a.at[rows], b.at[rows], sem_out.at[step, j])
            for j, (a, b) in enumerate(pairs)
        ]

    for i in range(DONE):
        for copy in loads(i):
            copy.start()
        if i == OWN_GROUP - 1:
            load_w.start()

    def group(step, carry):
        for j in range(OWN_GROUP):
            for copy in loads(step * OWN_GROUP + j):
                copy.wait()
        rows = pl.ds(pl.multiple_of(step * OWN_GROUP * WIN, WIN), OWN_GROUP * WIN)
        half = norm_half(x_s[rows, :].astype(F32))
        half_s[rows, :] = half

        @pl.when(step == 0)
        def _():
            load_w.wait()

        u, v, q, k = project([half], [w_s[...]])
        gate_s[rows, :] = u
        att_s[rows, :] = attend_users(OWN_GROUP, q, k, v)
        for copy in sends(step):
            copy.start()
        return carry

    lax.fori_loop(0, DONE // OWN_GROUP, group, 0)
    for step in range(DONE // OWN_GROUP):
        for copy in sends(step):
            copy.wait()


def in_vmem():
    return pl.BlockSpec(memory_space=pltpu.VMEM)


def in_hbm():
    return pl.BlockSpec(memory_space=pltpu.HBM)


def keep(array):
    return pltpu.with_memory_space_constraint(array, pltpu.VMEM)


def own_head(tokens, starts, part, w_own):
    kept = [((DONE * WIN, D), BF16), ((DONE * WIN, HEAD), F32), ((DONE * WIN, HEAD), BF16)]
    return pl.pallas_call(
        own_head_kernel,
        grid_spec=pltpu.PrefetchScalarGridSpec(
            num_scalar_prefetch=2,
            grid=(1,),
            in_specs=[in_hbm()] * 2,
            out_specs=[in_hbm()] * 3,
            scratch_shapes=[pltpu.VMEM((DONE * WIN, D), BF16)]
            + [pltpu.VMEM(*k) for k in kept]
            + [
                pltpu.VMEM((D, D), BF16),
                pltpu.SemaphoreType.DMA((DONE, MAXB)),
                pltpu.SemaphoreType.DMA,
                pltpu.SemaphoreType.DMA((DONE // OWN_GROUP, 3)),
            ],
        ),
        out_shape=[jax.ShapeDtypeStruct(*k) for k in kept],
        cost_estimate=pl.CostEstimate(
            flops=DONE * WIN * D * D * 64, bytes_accessed=DONE * WIN * D * 8, transcendentals=0
        ),
        name="own_head",
    )(starts, part, tokens, w_own)


def rows_of(tiles):
    return jnp.concatenate(
        [tiles[..., q, :, :].reshape(-1, HEAD) for q in range(N_MP)], axis=1
    )


def pack_kernel(
    start_ref, part_ref, core_ref, tokens_ref, w_ref, owner_ref, len_ref, off_ref,
    out_ref, rows_ref, x_s, table_s, row_s, out_s, sem, sem_t, sem_w, sem_out,
):
    tables = [
        pltpu.make_async_copy(ref, table_s.at[j], sem_t.at[j])
        for j, ref in enumerate((owner_ref, len_ref, off_ref))
    ]
    half = D // 2
    weights = pltpu.make_async_copy(w_ref.at[pl.ds(core_ref[0] * half, half)], rows_ref, sem_w)
    loads = [
        token_copies(
            tokens_ref, start_ref[0, part_ref[0] * MINE + k], x_s, k * WIN, sem.at[k]
        )
        for k in range(RAW)
    ]
    for copy in tables + loads[0] + [weights] + loads[1]:
        copy.start()
    row_s[...] = jnp.zeros_like(row_s)
    for j, copy in enumerate(tables):
        copy.wait()
        row_s[:, j * USERS : (j + 1) * USERS] = table_s[j] if j else N_DP - 1 - table_s[j]
    tile = jnp.broadcast_to(row_s[...], (TILE, 128)).astype(F32).astype(BF16)
    for k in range(RAW):
        out_s[k, :, N_MP] = jnp.broadcast_to(tile[None], (GROUPS, TILE, 128))
    sends = [pltpu.make_async_copy(out_s.at[k], out_ref.at[k], sem_out.at[k]) for k in range(RAW)]
    for k in range(RAW):
        for copy in loads[k]:
            copy.wait()
        for q in range(N_MP):
            out_s[k, :, q] = x_s[k * WIN : (k + 1) * WIN, q * HEAD : (q + 1) * HEAD].reshape(
                GROUPS, TILE, HEAD
            )
        sends[k].start()
    weights.wait()
    for copy in sends:
        copy.wait()


def pack(tokens, starts, part, core, w_own, owner, hist_len, recv_offset):
    shape = (RAW, GROUPS, RAW_MSG, TILE, HEAD)
    return pl.pallas_call(
        pack_kernel,
        grid_spec=pltpu.PrefetchScalarGridSpec(
            num_scalar_prefetch=3,
            grid=(1,),
            in_specs=[in_hbm()] * 5,
            out_specs=[in_hbm(), in_vmem()],
            scratch_shapes=[
                pltpu.VMEM((RAW * WIN, D), BF16),
                pltpu.VMEM((3, 1, USERS), jnp.int32),
                pltpu.VMEM((1, 128), jnp.int32),
                pltpu.VMEM(shape, BF16),
                pltpu.SemaphoreType.DMA((RAW, MAXB)),
                pltpu.SemaphoreType.DMA((3,)),
                pltpu.SemaphoreType.DMA,
                pltpu.SemaphoreType.DMA((RAW,)),
            ],
        ),
        out_shape=[jax.ShapeDtypeStruct(shape, BF16), pltpu.VMEM((D // 2, D), BF16)],
        name="pack",
    )(starts, part, core, tokens, w_own, owner, hist_len, recv_offset)


def head_order(part, core):
    down, up = (part + HEADS - 1) % HEADS, (part + 1) % HEADS
    first = core == 0
    return [part, jnp.where(first, down, up), jnp.where(first, up, down), (part + 2) % HEADS]


def mix(low_is_near, half_rows, first, whole, halves, w_out_of, x_rows):
    low = half_rows[:, : D // 2]
    high = half_rows[:, D // 2 :]
    parts = [jnp.where(low_is_near, low, high), jnp.where(low_is_near, high, low)]
    users = half_rows.shape[0] // WIN
    heads, gates = [first[0]], [first[1]]
    for rows, refs in (([half_rows], whole[:1]), ([half_rows], whole[1:]), (parts, halves)):
        u, v, q, k = project(rows, [ref[...] for ref in refs])
        gates.append(u)
        heads.append(attend_users(users, q, k, v))
    total = jnp.sum(heads[0] + heads[1] + (heads[2] + heads[3]), axis=1, keepdims=True)
    squares = jnp.sum(
        heads[0] * heads[0] + heads[1] * heads[1] + (heads[2] * heads[2] + heads[3] * heads[3]),
        axis=1,
        keepdims=True,
    )
    mean, inv = norm_stats(total, squares, 1.0 / WIN)
    gated = jnp.concatenate(
        [((a - mean) * inv * g.astype(F32)).astype(BF16) for a, g in zip(heads, gates)], axis=1
    )
    return jnp.dot(gated, w_out_of(), preferred_element_type=F32) + x_rows().astype(F32)


def attend_users(users, q, k, v):
    return jnp.concatenate(
        [attend(*(t[j * WIN : (j + 1) * WIN] for t in (q, k, v))) for j in range(users)], axis=0
    )


def live_rows(mixed, length):
    at = lax.broadcasted_iota(jnp.int32, (WIN, 1), 0)
    return jnp.where(at < length, mixed, 0.0).astype(BF16)


def last_row(tile, length):
    pick = lax.broadcasted_iota(jnp.int32, (TILE, HEAD), 0) == (length - 1) % TILE
    return jnp.sum(jnp.where(pick, tile.astype(F32), 0.0), axis=0, keepdims=True).astype(BF16)


def w_out_copies(part, core, w_out_ref, w_out_s, sem):
    return [
        pltpu.make_async_copy(
            w_out_ref.at[pl.ds(h * HEAD, HEAD)], w_out_s.at[pl.ds(s * HEAD, HEAD)], sem.at[s]
        )
        for s, h in enumerate(head_order(part, core))
    ]


def layer_kernel(
    start_ref, len_ref, part_ref, core_ref, tokens_ref, half_hbm, att_hbm, gate_hbm, *rest
):
    whole, halves, (w_out_ref, out_ref, state_ref) = rest[:2], rest[2:4], rest[4:7]
    x_s, half_s, att_s, gate_s, w_out_s, out_s, sem_in, sem_w, sem_out = rest[7:]
    low_is_near = core_ref[0] == 0
    first_id = part_ref[0] * MINE + RAW

    def loads(i):
        rows = pl.ds(i * WIN, WIN)
        pairs = ((half_hbm, half_s), (att_hbm, att_s), (gate_hbm, gate_s))
        return [
            pltpu.make_async_copy(a.at[rows], b.at[rows], sem_in.at[i, MAXB + j])
            for j, (a, b) in enumerate(pairs)
        ] + token_copies(tokens_ref, start_ref[0, first_id + i], x_s, i * WIN, sem_in.at[i])

    weights = w_out_copies(part_ref[0], core_ref[0], w_out_ref, w_out_s, sem_w)

    def sends(i):
        at = (i % HALVES, slice(None), pl.ds((i // HALVES) * N_MP, N_MP))
        return pltpu.make_async_copy(out_s.at[at], out_ref.at[at], sem_out.at[i])

    for i in range(DONE):
        for copy in loads(i):
            copy.start()
        if i == GROUP - 1:
            for copy in weights:
                copy.start()

    def group(step, carry):
        first_user = step * GROUP
        for j in range(GROUP):
            for copy in loads(first_user + j):
                copy.wait()
        rows = pl.ds(pl.multiple_of(first_user * WIN, WIN), GROUP * WIN)

        def w_out_of():
            @pl.when(step == 0)
            def _():
                for copy in weights:
                    copy.wait()

            return w_out_s[...]

        both = mix(
            low_is_near,
            half_s[rows, :],
            (att_s[rows, :], gate_s[rows, :]),
            whole,
            halves,
            w_out_of,
            lambda: x_s[rows, :],
        )
        for j in range(GROUP):
            i = first_user + j
            length = len_ref[0, first_id + i]
            half_id = i % HALVES
            base = (i // HALVES) * N_MP
            mixed = live_rows(both[j * WIN : (j + 1) * WIN], length)
            for q in range(N_MP):
                out_s[half_id, :, base + q] = mixed[:, q * HEAD : (q + 1) * HEAD].reshape(
                    GROUPS, TILE, HEAD
                )
            sends(i).start()
            for q in range(N_MP):
                state_ref[i, :, q * HEAD : (q + 1) * HEAD] = last_row(
                    out_s[half_id, (length - 1) // TILE, base + q], length
                )
        return carry

    lax.fori_loop(0, DONE // GROUP, group, 0)
    for i in range(DONE):
        sends(i).wait()


def layer(tokens, starts, lengths, part, core, kept, weights, w_out):
    message = (HALVES, GROUPS, MSG, TILE, HEAD)
    return pl.pallas_call(
        layer_kernel,
        grid_spec=pltpu.PrefetchScalarGridSpec(
            num_scalar_prefetch=4,
            grid=(1,),
            in_specs=[in_hbm()] * 4 + [in_vmem()] * 4 + [in_hbm()],
            out_specs=[in_hbm(), in_vmem()],
            scratch_shapes=[
                pltpu.VMEM((DONE * WIN, D), BF16),
                pltpu.VMEM((DONE * WIN, D), BF16),
                pltpu.VMEM((DONE * WIN, HEAD), F32),
                pltpu.VMEM((DONE * WIN, HEAD), BF16),
                pltpu.VMEM((D, D), BF16),
                pltpu.VMEM((HALVES, GROUPS, ROUND * N_MP, TILE, HEAD), BF16),
                pltpu.SemaphoreType.DMA((DONE, 5)),
                pltpu.SemaphoreType.DMA((HEADS,)),
                pltpu.SemaphoreType.DMA((DONE,)),
            ],
        ),
        out_shape=[
            jax.ShapeDtypeStruct(message, BF16),
            jax.ShapeDtypeStruct((DONE, 1, D), BF16),
        ],
        name="layer",
    )(starts, lengths, part, core, tokens, *kept, *map(keep, weights), w_out)


def raw_kernel(first_tile, len_ref, part_ref, core_ref, src_ref, w_own_ref, *rest):
    whole, halves, w_out_ref = rest[:2], rest[2:4], rest[4]
    pieces = rest[5 : 5 + N_MP]
    state_ref, x_s, w_out_s, mixed_s, sem_x, sem_w = rest[5 + N_MP :]
    part = part_ref[0]
    lengths = [len_ref[0, part * MINE + k] for k in range(RAW)]
    loads = [
        pltpu.make_async_copy(
            src_ref.at[pl.ds(k * GROUPS, GROUPS), pl.ds(first_tile, N_MP)], x_s.at[k], sem_x.at[k]
        )
        for k in range(RAW)
    ]
    weights = w_out_copies(part, core_ref[0], w_out_ref, w_out_s, sem_w)
    for copy in loads + weights:
        copy.start()
    for copy in loads:
        copy.wait()

    def x_rows():
        return rows_of(x_s[...])

    half = norm_half(x_rows().astype(F32))
    u, v, q, k = project([half], [w_own_ref[...]])

    def w_out_of():
        for copy in weights:
            copy.wait()
        return w_out_s[...]

    both = mix(
        core_ref[0] == 0, half, (attend_users(RAW, q, k, v), u), whole, halves, w_out_of, x_rows
    )
    for k in range(RAW):
        mixed = live_rows(both[k * WIN : (k + 1) * WIN], lengths[k])
        for q in range(N_MP):
            mixed_s[q, k] = mixed[:, q * HEAD : (q + 1) * HEAD].reshape(GROUPS, TILE, HEAD)
        for q in range(N_MP):
            state_ref[k, :, q * HEAD : (q + 1) * HEAD] = last_row(
                mixed_s[q, k, (lengths[k] - 1) // TILE], lengths[k]
            )
    for s in range(N_MP):
        pieces[s][...] = mixed_s[(part + s) % N_MP]


def raw_layer(source, first_tile, lengths, part, core, w_own, weights, w_out):
    piece = jax.ShapeDtypeStruct((RAW, GROUPS, TILE, HEAD), BF16)
    outs = pl.pallas_call(
        lambda *refs: raw_kernel(first_tile, *refs),
        grid_spec=pltpu.PrefetchScalarGridSpec(
            num_scalar_prefetch=3,
            grid=(1,),
            in_specs=[in_hbm()] + [in_vmem()] * 5 + [in_hbm()],
            out_specs=[in_vmem()] * (N_MP + 1),
            scratch_shapes=[
                pltpu.VMEM((RAW, GROUPS, N_MP, TILE, HEAD), BF16),
                pltpu.VMEM((D, D), BF16),
                pltpu.VMEM((N_MP, RAW, GROUPS, TILE, HEAD), BF16),
                pltpu.SemaphoreType.DMA((RAW,)),
                pltpu.SemaphoreType.DMA((HEADS,)),
            ],
        ),
        out_shape=[piece] * N_MP + [jax.ShapeDtypeStruct((RAW, 1, D), BF16)],
    )(lengths, part, core, source, w_own, *weights, w_out)
    return outs[:N_MP], outs[N_MP]


def merge_kernel(first_ref, in_ref, msg_ref, out_ref, sorted_s, table_v, table_s, sem):
    table = jnp.max(in_ref[:, N_MP].astype(F32), axis=1)
    table_v[...] = table.astype(jnp.int32)
    copy = pltpu.make_async_copy(table_v, table_s, sem.at[0])
    copy.start()
    copy.wait()
    first = first_ref[0]

    def one(d, carry):
        o = table_s[d, first]
        for q in range(N_MP):
            sorted_s[o, q] = in_ref[d, q]
        return carry

    lax.fori_loop(0, N_DP, one, 0, unroll=8)
    send = pltpu.make_async_copy(sorted_s, out_ref.at[:, pl.ds(ROUND * N_MP, N_MP)], sem.at[1])
    send.start()
    send.wait()


def merge(spread, first, message):
    return pl.pallas_call(
        merge_kernel,
        grid_spec=pltpu.PrefetchScalarGridSpec(
            num_scalar_prefetch=1,
            grid=(1,),
            in_specs=[in_vmem(), in_hbm()],
            out_specs=in_hbm(),
            scratch_shapes=[
                pltpu.VMEM((N_DP, N_MP, TILE, HEAD), BF16),
                pltpu.VMEM((N_DP, 128), jnp.int32),
                pltpu.SMEM((N_DP, 128), jnp.int32),
                pltpu.SemaphoreType.DMA((2,)),
            ],
        ),
        out_shape=jax.ShapeDtypeStruct((N_DP, MSG, TILE, HEAD), BF16),
        input_output_aliases={2: 0},
        name="merge",
    )(first, keep(spread), message)


def regroup_kernel(from_ref, in_ref, out_ref, out_s, sem):
    chunk = N_DP // CHUNKS

    def send(c):
        at = pl.ds(c * chunk, chunk)
        return pltpu.make_async_copy(out_s.at[at], out_ref.at[at], sem.at[c])

    def one(c, carry):
        for j in range(chunk):
            o = c * chunk + j
            for r in range(ROUND):
                d = from_ref[r * N_DP + o]
                for q in range(N_MP):
                    out_s[o, q, r] = in_ref[d, r * N_MP + q]
        send(c).start()
        return carry

    lax.fori_loop(0, CHUNKS, one, 0)
    for c in range(CHUNKS):
        send(c).wait()


def regroup(spread, source):
    shape = (N_DP, N_MP, ROUND, TILE, HEAD)
    return pl.pallas_call(
        regroup_kernel,
        grid_spec=pltpu.PrefetchScalarGridSpec(
            num_scalar_prefetch=1,
            grid=(1,),
            in_specs=[in_vmem()],
            out_specs=in_hbm(),
            scratch_shapes=[pltpu.VMEM(shape, BF16), pltpu.SemaphoreType.DMA((CHUNKS,))],
        ),
        out_shape=jax.ShapeDtypeStruct(shape, BF16),
        name="regroup",
    )(source, keep(spread))


def place_kernel(len_ref, off_ref, part_ref, in_ref, own_ref, *rest):
    out_ref, zero_v, used_s, own_s, sem, sem_own = rest[N_MP - 1 :]
    pieces = (own_s, *rest[: N_MP - 1])
    load = pltpu.make_async_copy(own_ref, own_s, sem_own)
    load.start()
    per_block = BLOCK // TILE
    zero_v[...] = jnp.zeros_like(zero_v)

    def clear(b, carry):
        used_s[b] = 0
        return carry

    lax.fori_loop(0, BLK_DEV, clear, 0, unroll=8)

    def send(u, source):
        def block(j):
            to = off_ref[u] + j
            used_s[to] = 1
            pltpu.make_async_copy(
                source(pl.ds(j * per_block, per_block)),
                out_ref.at[pl.ds(to * per_block, per_block)],
                sem,
            ).start()

        block(0)

        @pl.when(len_ref[u] > BLOCK)
        def _():
            block(1)

    def send_piece(s):
        m = (part_ref[0] + N_MP - s) % N_MP
        for k in range(RAW):
            send(m * MINE + k, lambda rows: pieces[s].at[k, rows])

    for s in range(1, N_MP):
        send_piece(s)

    def one(n, carry):
        m = n // DONE
        i = n % DONE
        send(m * MINE + RAW + i, lambda rows: in_ref.at[i % HALVES, rows, m, i // HALVES])
        return carry

    lax.fori_loop(0, N_MP * DONE, one, 0)
    load.wait()
    send_piece(0)

    def fill(b, carry):
        @pl.when(used_s[b] == 0)
        def _():
            pltpu.make_async_copy(zero_v, out_ref.at[pl.ds(b * per_block, per_block)], sem).start()

        return carry

    lax.fori_loop(0, BLK_DEV, fill, 0)
    pltpu.make_async_copy(out_ref, out_ref, sem).wait()


def place(arrived, pieces, lengths, offsets, part):
    rows = BLK_DEV * BLOCK
    return pl.pallas_call(
        place_kernel,
        grid_spec=pltpu.PrefetchScalarGridSpec(
            num_scalar_prefetch=3,
            grid=(1,),
            in_specs=[in_vmem(), in_hbm()] + [in_vmem()] * (N_MP - 1),
            out_specs=in_hbm(),
            scratch_shapes=[
                pltpu.VMEM((BLOCK // TILE, TILE, HEAD), BF16),
                pltpu.SMEM((BLK_DEV,), jnp.int32),
                pltpu.VMEM((RAW, GROUPS, TILE, HEAD), BF16),
                pltpu.SemaphoreType.DMA,
                pltpu.SemaphoreType.DMA,
            ],
        ),
        out_shape=jax.ShapeDtypeStruct((rows // TILE, TILE, HEAD), BF16),
        compiler_params=pltpu.CompilerParams(vmem_limit_bytes=32 * 1024 * 1024),
        name="place",
    )(lengths, offsets, part, keep(arrived), pltpu.with_memory_space_constraint(pieces[0], pltpu.HBM), *map(keep, pieces[1:])).reshape(rows, HEAD)


def along_mp(array, s):
    return lax.ppermute(array, "mp", [(i, (i + s) % N_MP) for i in range(N_MP)])


def per_device(tokens, w_uvqk, w_out, hist_len, owner, recv_offset, block_start):
    me = lax.axis_index("dp")
    part = lax.axis_index("mp")
    first = part * MINE
    core = me % 2
    seat = N_DP - 1 - me
    half = seat // GROUPS
    part_1, core_1 = part[None], core[None]

    raw, mine_rows = pack(
        tokens, block_start, part_1, core_1, w_uvqk, owner, hist_len, recv_offset
    )
    swap = [(i, i ^ 1) for i in range(N_DP)]
    ring = [
        (d * N_MP + m, d * N_MP + (m + (1 if d % 2 == 0 else N_MP - 1)) % N_MP)
        for d in range(N_DP)
        for m in range(N_MP)
    ]
    side = lax.ppermute(w_uvqk, ("dp", "mp"), ring)
    across = along_mp(mine_rows, 2)
    other_side = lax.ppermute(side, "dp", swap)
    other_across = lax.ppermute(across, "dp", swap)
    weights = (side, other_side, across, other_across)
    raw_in = lax.all_to_all(
        raw.reshape(N_DP, RAW_MSG * TILE, HEAD), "dp", 0, 0, axis_index_groups=[SEATS], tiled=True
    ).reshape(N_DP, RAW_MSG, TILE, HEAD)
    kept = own_head(tokens, block_start, part_1, w_uvqk)
    message, last = layer(
        tokens, block_start, hist_len, part_1, core_1, kept, weights, w_out
    )
    message = merge(
        raw_in, (first + half)[None], message.reshape(N_DP, MSG, TILE, HEAD)
    )
    spread = lax.all_to_all(
        message.reshape(N_DP, MSG * TILE, HEAD), "dp", 0, 0, axis_index_groups=[SEATS], tiled=True
    ).reshape(N_DP, MSG, TILE, HEAD)
    _, raw_last = raw_layer(
        raw.reshape(N_DP, RAW_MSG, TILE, HEAD), 0, hist_len, part_1, core_1,
        w_uvqk, weights, w_out,
    )

    table = raw_in[:, N_MP, 0, :].astype(jnp.int32)
    owners = table[:, :USERS]
    held = lax.dynamic_slice_in_dim(owners, first + RAW + half, HALVES * (ROUND - 1) + 1, 1)
    ids = jnp.arange(N_DP, dtype=jnp.int32)
    source = jnp.sum(
        jnp.where(held[:, ::HALVES].T[:, None, :] == ids[None, :, None], ids[None, None, :], 0), axis=2
    ).reshape(-1)
    mine = owners == seat
    recv_len = jnp.sum(jnp.where(mine, table[:, USERS : 2 * USERS], 0), axis=0)
    recv_off = jnp.sum(jnp.where(mine, table[:, 2 * USERS : 3 * USERS], 0), axis=0)

    sorted_rows = regroup(spread, source)
    arrived = lax.all_to_all(
        sorted_rows.reshape(N_DP * N_MP, ROUND * TILE, HEAD), ("dp", "mp"), 0, 0,
        axis_index_groups=[[d * N_MP + m for d in SEATS for m in range(N_MP)]], tiled=True
    )
    pieces, _ = raw_layer(
        spread, ROUND * N_MP, recv_len[None], part_1, core_1,
        w_uvqk, weights, w_out,
    )
    pieces = [pieces[0]] + [along_mp(pieces[s], s) for s in range(1, N_MP)]
    packed = place(
        arrived.reshape(HALVES, GROUPS, N_MP, ROUND, TILE, HEAD),
        pieces, recv_len, recv_off, part_1,
    )

    columns = jnp.concatenate([raw_last, last], axis=0).reshape(MINE, N_MP, HEAD)
    state = jnp.zeros((N_MP, MINE, HEAD), BF16)
    for s in range(N_MP):
        to_part = (part + s) % N_MP
        piece = lax.dynamic_slice_in_dim(columns, to_part, 1, 1)[:, 0]
        if s:
            piece = along_mp(piece, s)
        state = lax.dynamic_update_slice_in_dim(state, piece[None], (part - s) % N_MP, 0)
    return packed, state.reshape(USERS, HEAD)


def solution(mesh):
    in_specs = (
        P("dp", None),
        P(None, "mp"),
        P(),
        P("dp", None),
        P("dp", None),
        P("dp", None),
        P("dp", None),
    )
    out_specs = (P("dp", "mp"), P("dp", "mp"))
    return jax.shard_map(
        per_device, mesh=mesh, in_specs=in_specs, out_specs=out_specs, check_vma=False
    )
```

```python
import jax
import jax.numpy as jnp
from jax import lax
from jax.experimental import pallas as pl
from jax.experimental.pallas import tpu as pltpu
from jax.sharding import PartitionSpec as P

D = 512
HEADS = 4
HEAD = D // HEADS
BLOCK = 128
MAXB = 2
BLK_DEV = 48
USERS = 24
N_DP = 64
N_MP = 4
WIN = MAXB * BLOCK
MINE = USERS // N_MP
RAW = 2
DONE = MINE - RAW
TILE = 8
GROUPS = WIN // TILE
HALVES = N_DP // GROUPS
GROUP = 2
OWN_GROUP = 2
CHUNKS = 4


def seat_of(dp):
    return ((dp & 7) << 3) | ((3 * (dp >> 3)) & 7)


SEATS = sorted(range(N_DP), key=seat_of)
RAW_MSG = N_MP + 1
ROUND = DONE // HALVES
MSG = (ROUND + 1) * N_MP
EPS = 1e-05
BF16 = jnp.bfloat16
F32 = jnp.float32


def silu_of_twice(h):
    return h + h * jnp.tanh(h)


def project(half_parts, w_parts):
    acc = jnp.dot(half_parts[0], w_parts[0], preferred_element_type=F32)
    for n, w in zip(half_parts[1:], w_parts[1:]):
        acc = acc + jnp.dot(n, w, preferred_element_type=F32)
    proj = silu_of_twice(acc).astype(BF16)
    return [proj[:, j * HEAD : (j + 1) * HEAD] for j in range(4)]


def attend(q, k, v):
    row = lax.broadcasted_iota(jnp.int32, (BLOCK, BLOCK), 0)
    col = lax.broadcasted_iota(jnp.int32, (BLOCK, BLOCK), 1)
    causal = col <= row
    scale = 0.5 * HEAD ** (-0.5)
    contract_last = (((1,), (1,)), ((), ()))
    s0 = lax.dot_general(q[:BLOCK], k[:BLOCK], contract_last, preferred_element_type=F32)
    s1 = lax.dot_general(q[BLOCK:], k, contract_last, preferred_element_type=F32)
    a0 = jnp.where(causal, silu_of_twice(s0 * scale), 0.0).astype(BF16)
    b = silu_of_twice(s1 * scale)
    a1 = jnp.concatenate(
        [b[:, :BLOCK].astype(BF16), jnp.where(causal, b[:, BLOCK:], 0.0).astype(BF16)], axis=1
    )
    return jnp.concatenate(
        [
            jnp.dot(a0, v[:BLOCK], preferred_element_type=F32),
            jnp.dot(a1, v, preferred_element_type=F32),
        ],
        axis=0,
    )


def norm_stats(total, squares, unit=1.0):
    mean = total * (1.0 / D)
    var = squares * (1.0 / D) - mean * mean
    return mean, lax.rsqrt(var * (unit * unit) + EPS) * unit


def token_copies(tokens_ref, block, x_ref, row, sem):
    second = jnp.minimum(block + 1, BLK_DEV - 1)
    return [
        pltpu.make_async_copy(
            tokens_ref.at[pl.ds(b * BLOCK, BLOCK)],
            x_ref.at[pl.ds(row + j * BLOCK, BLOCK)],
            sem.at[j],
        )
        for j, b in enumerate((block, second))
    ]


def norm_half(x):
    mean, inv = norm_stats(
        jnp.sum(x, axis=1, keepdims=True), jnp.sum(x * x, axis=1, keepdims=True)
    )
    return ((x - mean) * (inv * 0.5)).astype(BF16)


def own_head_kernel(
    start_ref, part_ref, tokens_ref, w_ref, half_ref, att_ref, gate_ref,
    x_s, half_s, att_s, gate_s, w_s, sem_in, sem_w, sem_out,
):
    load_w = pltpu.make_async_copy(w_ref, w_s, sem_w)

    def loads(i):
        block = start_ref[0, part_ref[0] * MINE + RAW + i]
        return token_copies(tokens_ref, block, x_s, i * WIN, sem_in.at[i])

    def sends(step):
        rows = pl.ds(step * OWN_GROUP * WIN, OWN_GROUP * WIN)
        pairs = ((half_s, half_ref), (att_s, att_ref), (gate_s, gate_ref))
        return [
            pltpu.make_async_copy(a.at[rows], b.at[rows], sem_out.at[step, j])
            for j, (a, b) in enumerate(pairs)
        ]

    for i in range(DONE):
        for copy in loads(i):
            copy.start()
        if i == OWN_GROUP - 1:
            load_w.start()

    def group(step, carry):
        for j in range(OWN_GROUP):
            for copy in loads(step * OWN_GROUP + j):
                copy.wait()
        rows = pl.ds(pl.multiple_of(step * OWN_GROUP * WIN, WIN), OWN_GROUP * WIN)
        half = norm_half(x_s[rows, :].astype(F32))
        half_s[rows, :] = half

        @pl.when(step == 0)
        def _():
            load_w.wait()

        u, v, q, k = project([half], [w_s[...]])
        gate_s[rows, :] = u
        att_s[rows, :] = attend_users(OWN_GROUP, q, k, v)
        for copy in sends(step):
            copy.start()
        return carry

    lax.fori_loop(0, DONE // OWN_GROUP, group, 0)
    for step in range(DONE // OWN_GROUP):
        for copy in sends(step):
            copy.wait()


def in_vmem():
    return pl.BlockSpec(memory_space=pltpu.VMEM)


def in_hbm():
    return pl.BlockSpec(memory_space=pltpu.HBM)


def keep(array):
    return pltpu.with_memory_space_constraint(array, pltpu.VMEM)


def own_head(tokens, starts, part, w_own):
    kept = [((DONE * WIN, D), BF16), ((DONE * WIN, HEAD), F32), ((DONE * WIN, HEAD), BF16)]
    return pl.pallas_call(
        own_head_kernel,
        grid_spec=pltpu.PrefetchScalarGridSpec(
            num_scalar_prefetch=2,
            grid=(1,),
            in_specs=[in_hbm()] * 2,
            out_specs=[in_hbm()] * 3,
            scratch_shapes=[pltpu.VMEM((DONE * WIN, D), BF16)]
            + [pltpu.VMEM(*k) for k in kept]
            + [
                pltpu.VMEM((D, D), BF16),
                pltpu.SemaphoreType.DMA((DONE, MAXB)),
                pltpu.SemaphoreType.DMA,
                pltpu.SemaphoreType.DMA((DONE // OWN_GROUP, 3)),
            ],
        ),
        out_shape=[jax.ShapeDtypeStruct(*k) for k in kept],
        cost_estimate=pl.CostEstimate(
            flops=DONE * WIN * D * D * 64, bytes_accessed=DONE * WIN * D * 8, transcendentals=0
        ),
        name="own_head",
    )(starts, part, tokens, w_own)


def rows_of(tiles):
    return jnp.concatenate(
        [tiles[..., q, :, :].reshape(-1, HEAD) for q in range(N_MP)], axis=1
    )


def pack_kernel(
    start_ref, part_ref, core_ref, tokens_ref, w_ref, owner_ref, len_ref, off_ref,
    out_ref, rows_ref, x_s, table_s, row_s, out_s, sem, sem_t, sem_w, sem_out,
):
    tables = [
        pltpu.make_async_copy(ref, table_s.at[j], sem_t.at[j])
        for j, ref in enumerate((owner_ref, len_ref, off_ref))
    ]
    half = D // 2
    weights = pltpu.make_async_copy(w_ref.at[pl.ds(core_ref[0] * half, half)], rows_ref, sem_w)
    loads = [
        token_copies(
            tokens_ref, start_ref[0, part_ref[0] * MINE + k], x_s, k * WIN, sem.at[k]
        )
        for k in range(RAW)
    ]
    for copy in tables + loads[0] + [weights] + loads[1]:
        copy.start()
    row_s[...] = jnp.zeros_like(row_s)
    for j, copy in enumerate(tables):
        copy.wait()
        row_s[:, j * USERS : (j + 1) * USERS] = table_s[j] if j else seat_of(table_s[j])
    tile = jnp.broadcast_to(row_s[...], (TILE, 128)).astype(F32).astype(BF16)
    for k in range(RAW):
        out_s[k, :, N_MP] = jnp.broadcast_to(tile[None], (GROUPS, TILE, 128))
    sends = [pltpu.make_async_copy(out_s.at[k], out_ref.at[k], sem_out.at[k]) for k in range(RAW)]
    for k in range(RAW):
        for copy in loads[k]:
            copy.wait()
        for q in range(N_MP):
            out_s[k, :, q] = x_s[k * WIN : (k + 1) * WIN, q * HEAD : (q + 1) * HEAD].reshape(
                GROUPS, TILE, HEAD
            )
        sends[k].start()
    weights.wait()
    for copy in sends:
        copy.wait()


def pack(tokens, starts, part, core, w_own, owner, hist_len, recv_offset):
    shape = (RAW, GROUPS, RAW_MSG, TILE, HEAD)
    return pl.pallas_call(
        pack_kernel,
        grid_spec=pltpu.PrefetchScalarGridSpec(
            num_scalar_prefetch=3,
            grid=(1,),
            in_specs=[in_hbm()] * 5,
            out_specs=[in_hbm(), in_vmem()],
            scratch_shapes=[
                pltpu.VMEM((RAW * WIN, D), BF16),
                pltpu.VMEM((3, 1, USERS), jnp.int32),
                pltpu.VMEM((1, 128), jnp.int32),
                pltpu.VMEM(shape, BF16),
                pltpu.SemaphoreType.DMA((RAW, MAXB)),
                pltpu.SemaphoreType.DMA((3,)),
                pltpu.SemaphoreType.DMA,
                pltpu.SemaphoreType.DMA((RAW,)),
            ],
        ),
        out_shape=[jax.ShapeDtypeStruct(shape, BF16), pltpu.VMEM((D // 2, D), BF16)],
        name="pack",
    )(starts, part, core, tokens, w_own, owner, hist_len, recv_offset)


def head_order(part, core):
    down, up = (part + HEADS - 1) % HEADS, (part + 1) % HEADS
    first = core == 0
    return [part, jnp.where(first, down, up), jnp.where(first, up, down), (part + 2) % HEADS]


def mix(low_is_near, half_rows, first, whole, halves, w_out_of, x_rows):
    low = half_rows[:, : D // 2]
    high = half_rows[:, D // 2 :]
    parts = [jnp.where(low_is_near, low, high), jnp.where(low_is_near, high, low)]
    users = half_rows.shape[0] // WIN
    heads, gates = [first[0]], [first[1]]
    for rows, refs in (([half_rows], whole[:1]), ([half_rows], whole[1:]), (parts, halves)):
        u, v, q, k = project(rows, [ref[...] for ref in refs])
        gates.append(u)
        heads.append(attend_users(users, q, k, v))
    total = jnp.sum(heads[0] + heads[1] + (heads[2] + heads[3]), axis=1, keepdims=True)
    squares = jnp.sum(
        heads[0] * heads[0] + heads[1] * heads[1] + (heads[2] * heads[2] + heads[3] * heads[3]),
        axis=1,
        keepdims=True,
    )
    mean, inv = norm_stats(total, squares, 1.0 / WIN)
    gated = jnp.concatenate(
        [((a - mean) * inv * g.astype(F32)).astype(BF16) for a, g in zip(heads, gates)], axis=1
    )
    return jnp.dot(gated, w_out_of(), preferred_element_type=F32) + x_rows().astype(F32)


def attend_users(users, q, k, v):
    return jnp.concatenate(
        [attend(*(t[j * WIN : (j + 1) * WIN] for t in (q, k, v))) for j in range(users)], axis=0
    )


def live_rows(mixed, length):
    at = lax.broadcasted_iota(jnp.int32, (WIN, 1), 0)
    return jnp.where(at < length, mixed, 0.0).astype(BF16)


def last_row(tile, length):
    pick = lax.broadcasted_iota(jnp.int32, (TILE, HEAD), 0) == (length - 1) % TILE
    return jnp.sum(jnp.where(pick, tile.astype(F32), 0.0), axis=0, keepdims=True).astype(BF16)


def w_out_copies(part, core, w_out_ref, w_out_s, sem):
    return [
        pltpu.make_async_copy(
            w_out_ref.at[pl.ds(h * HEAD, HEAD)], w_out_s.at[pl.ds(s * HEAD, HEAD)], sem.at[s]
        )
        for s, h in enumerate(head_order(part, core))
    ]


def layer_kernel(
    start_ref, len_ref, part_ref, core_ref, tokens_ref, half_hbm, att_hbm, gate_hbm, *rest
):
    whole, halves, (w_out_ref, out_ref, state_ref) = rest[:2], rest[2:4], rest[4:7]
    x_s, half_s, att_s, gate_s, w_out_s, out_s, sem_in, sem_w, sem_out = rest[7:]
    low_is_near = core_ref[0] == 0
    first_id = part_ref[0] * MINE + RAW

    def loads(i):
        rows = pl.ds(i * WIN, WIN)
        pairs = ((half_hbm, half_s), (att_hbm, att_s), (gate_hbm, gate_s))
        return [
            pltpu.make_async_copy(a.at[rows], b.at[rows], sem_in.at[i, MAXB + j])
            for j, (a, b) in enumerate(pairs)
        ] + token_copies(tokens_ref, start_ref[0, first_id + i], x_s, i * WIN, sem_in.at[i])

    weights = w_out_copies(part_ref[0], core_ref[0], w_out_ref, w_out_s, sem_w)

    def sends(i):
        at = (i % HALVES, slice(None), pl.ds((i // HALVES) * N_MP, N_MP))
        return pltpu.make_async_copy(out_s.at[at], out_ref.at[at], sem_out.at[i])

    for i in range(DONE):
        for copy in loads(i):
            copy.start()
        if i == GROUP - 1:
            for copy in weights:
                copy.start()

    def group(step, carry):
        first_user = step * GROUP
        for j in range(GROUP):
            for copy in loads(first_user + j):
                copy.wait()
        rows = pl.ds(pl.multiple_of(first_user * WIN, WIN), GROUP * WIN)

        def w_out_of():
            @pl.when(step == 0)
            def _():
                for copy in weights:
                    copy.wait()

            return w_out_s[...]

        both = mix(
            low_is_near,
            half_s[rows, :],
            (att_s[rows, :], gate_s[rows, :]),
            whole,
            halves,
            w_out_of,
            lambda: x_s[rows, :],
        )
        for j in range(GROUP):
            i = first_user + j
            length = len_ref[0, first_id + i]
            half_id = i % HALVES
            base = (i // HALVES) * N_MP
            mixed = live_rows(both[j * WIN : (j + 1) * WIN], length)
            for q in range(N_MP):
                out_s[half_id, :, base + q] = mixed[:, q * HEAD : (q + 1) * HEAD].reshape(
                    GROUPS, TILE, HEAD
                )
            sends(i).start()
            for q in range(N_MP):
                state_ref[i, :, q * HEAD : (q + 1) * HEAD] = last_row(
                    out_s[half_id, (length - 1) // TILE, base + q], length
                )
        return carry

    lax.fori_loop(0, DONE // GROUP, group, 0)
    for i in range(DONE):
        sends(i).wait()


def layer(tokens, starts, lengths, part, core, kept, weights, w_out):
    message = (HALVES, GROUPS, MSG, TILE, HEAD)
    return pl.pallas_call(
        layer_kernel,
        grid_spec=pltpu.PrefetchScalarGridSpec(
            num_scalar_prefetch=4,
            grid=(1,),
            in_specs=[in_hbm()] * 4 + [in_vmem()] * 4 + [in_hbm()],
            out_specs=[in_hbm(), in_vmem()],
            scratch_shapes=[
                pltpu.VMEM((DONE * WIN, D), BF16),
                pltpu.VMEM((DONE * WIN, D), BF16),
                pltpu.VMEM((DONE * WIN, HEAD), F32),
                pltpu.VMEM((DONE * WIN, HEAD), BF16),
                pltpu.VMEM((D, D), BF16),
                pltpu.VMEM((HALVES, GROUPS, ROUND * N_MP, TILE, HEAD), BF16),
                pltpu.SemaphoreType.DMA((DONE, 5)),
                pltpu.SemaphoreType.DMA((HEADS,)),
                pltpu.SemaphoreType.DMA((DONE,)),
            ],
        ),
        out_shape=[
            jax.ShapeDtypeStruct(message, BF16),
            jax.ShapeDtypeStruct((DONE, 1, D), BF16),
        ],
        name="layer",
    )(starts, lengths, part, core, tokens, *kept, *map(keep, weights), w_out)


def raw_kernel(first_tile, len_ref, part_ref, core_ref, src_ref, w_own_ref, *rest):
    whole, halves, w_out_ref = rest[:2], rest[2:4], rest[4]
    pieces = rest[5 : 5 + N_MP]
    state_ref, x_s, w_out_s, mixed_s, sem_x, sem_w = rest[5 + N_MP :]
    part = part_ref[0]
    lengths = [len_ref[0, part * MINE + k] for k in range(RAW)]
    loads = [
        pltpu.make_async_copy(
            src_ref.at[pl.ds(k * GROUPS, GROUPS), pl.ds(first_tile, N_MP)], x_s.at[k], sem_x.at[k]
        )
        for k in range(RAW)
    ]
    weights = w_out_copies(part, core_ref[0], w_out_ref, w_out_s, sem_w)
    for copy in loads + weights:
        copy.start()
    for copy in loads:
        copy.wait()

    def x_rows():
        return rows_of(x_s[...])

    half = norm_half(x_rows().astype(F32))
    u, v, q, k = project([half], [w_own_ref[...]])

    def w_out_of():
        for copy in weights:
            copy.wait()
        return w_out_s[...]

    both = mix(
        core_ref[0] == 0, half, (attend_users(RAW, q, k, v), u), whole, halves, w_out_of, x_rows
    )
    for k in range(RAW):
        mixed = live_rows(both[k * WIN : (k + 1) * WIN], lengths[k])
        for q in range(N_MP):
            mixed_s[q, k] = mixed[:, q * HEAD : (q + 1) * HEAD].reshape(GROUPS, TILE, HEAD)
        for q in range(N_MP):
            state_ref[k, :, q * HEAD : (q + 1) * HEAD] = last_row(
                mixed_s[q, k, (lengths[k] - 1) // TILE], lengths[k]
            )
    for s in range(N_MP):
        pieces[s][...] = mixed_s[(part + s) % N_MP]


def raw_layer(source, first_tile, lengths, part, core, w_own, weights, w_out):
    piece = jax.ShapeDtypeStruct((RAW, GROUPS, TILE, HEAD), BF16)
    outs = pl.pallas_call(
        lambda *refs: raw_kernel(first_tile, *refs),
        grid_spec=pltpu.PrefetchScalarGridSpec(
            num_scalar_prefetch=3,
            grid=(1,),
            in_specs=[in_hbm()] + [in_vmem()] * 5 + [in_hbm()],
            out_specs=[in_vmem()] * (N_MP + 1),
            scratch_shapes=[
                pltpu.VMEM((RAW, GROUPS, N_MP, TILE, HEAD), BF16),
                pltpu.VMEM((D, D), BF16),
                pltpu.VMEM((N_MP, RAW, GROUPS, TILE, HEAD), BF16),
                pltpu.SemaphoreType.DMA((RAW,)),
                pltpu.SemaphoreType.DMA((HEADS,)),
            ],
        ),
        out_shape=[piece] * N_MP + [jax.ShapeDtypeStruct((RAW, 1, D), BF16)],
    )(lengths, part, core, source, w_own, *weights, w_out)
    return outs[:N_MP], outs[N_MP]


def merge_kernel(first_ref, in_ref, msg_ref, out_ref, sorted_s, table_v, table_s, sem):
    lane = lax.broadcasted_iota(jnp.int32, (TILE, 128), 1)
    column = (lane == first_ref[0]).astype(F32).astype(BF16)
    tiles = in_ref[:, N_MP].reshape(N_DP * TILE, 128)
    seats = lax.dot_general(column, tiles, (((1,), (1,)), ((), ())), preferred_element_type=F32)
    table_v[...] = seats.astype(jnp.int32)
    copy = pltpu.make_async_copy(table_v.at[pl.ds(0, 1)], table_s, sem.at[0])
    copy.start()
    copy.wait()

    def one(d, carry):
        o = table_s[0, d * TILE]
        for q in range(N_MP):
            sorted_s[o, q] = in_ref[d, q]
        return carry

    lax.fori_loop(0, N_DP, one, 0, unroll=8)
    send = pltpu.make_async_copy(sorted_s, out_ref.at[:, pl.ds(ROUND * N_MP, N_MP)], sem.at[1])
    send.start()
    send.wait()


def merge(spread, first, message):
    return pl.pallas_call(
        merge_kernel,
        grid_spec=pltpu.PrefetchScalarGridSpec(
            num_scalar_prefetch=1,
            grid=(1,),
            in_specs=[in_vmem(), in_hbm()],
            out_specs=in_hbm(),
            scratch_shapes=[
                pltpu.VMEM((N_DP, N_MP, TILE, HEAD), BF16),
                pltpu.VMEM((TILE, N_DP * TILE), jnp.int32),
                pltpu.SMEM((1, N_DP * TILE), jnp.int32),
                pltpu.SemaphoreType.DMA((2,)),
            ],
        ),
        out_shape=jax.ShapeDtypeStruct((N_DP, MSG, TILE, HEAD), BF16),
        input_output_aliases={2: 0},
        name="merge",
    )(first, keep(spread), message)


def regroup_kernel(from_ref, in_ref, out_ref, out_s, sem):
    chunk = N_DP // CHUNKS

    def send(c):
        at = pl.ds(c * chunk, chunk)
        return pltpu.make_async_copy(out_s.at[at], out_ref.at[at], sem.at[c])

    def one(c, carry):
        for j in range(chunk):
            o = c * chunk + j
            for r in range(ROUND):
                d = from_ref[r * N_DP + o]
                for q in range(N_MP):
                    out_s[o, q, r] = in_ref[d, r * N_MP + q]
        send(c).start()
        return carry

    lax.fori_loop(0, CHUNKS, one, 0)
    for c in range(CHUNKS):
        send(c).wait()


def regroup(spread, source):
    shape = (N_DP, N_MP, ROUND, TILE, HEAD)
    return pl.pallas_call(
        regroup_kernel,
        grid_spec=pltpu.PrefetchScalarGridSpec(
            num_scalar_prefetch=1,
            grid=(1,),
            in_specs=[in_vmem()],
            out_specs=in_hbm(),
            scratch_shapes=[pltpu.VMEM(shape, BF16), pltpu.SemaphoreType.DMA((CHUNKS,))],
        ),
        out_shape=jax.ShapeDtypeStruct(shape, BF16),
        name="regroup",
    )(source, keep(spread))


def place_raw_kernel(len_ref, off_ref, part_ref, own_ref, *rest):
    out_ref, zero_v, used_s, own_s, sem, sem_zero, sem_own = rest[N_MP - 1 :]
    pieces = (own_s, *rest[: N_MP - 1])
    per_block = BLOCK // TILE
    load = pltpu.make_async_copy(own_ref, own_s, sem_own)
    load.start()
    zero_v[...] = jnp.zeros_like(zero_v)

    def clear(b, carry):
        used_s[b] = 0
        return carry

    lax.fori_loop(0, BLK_DEV, clear, 0, unroll=8)

    def mark(u, carry):
        used_s[off_ref[u]] = 1

        @pl.when(len_ref[u] > BLOCK)
        def _():
            used_s[off_ref[u] + 1] = 1

        return carry

    lax.fori_loop(0, USERS, mark, 0)

    def fill(b, carry):
        @pl.when(used_s[b] == 0)
        def _():
            pltpu.make_async_copy(
                zero_v, out_ref.at[pl.ds(b * per_block, per_block)], sem_zero
            ).start()

        return carry

    lax.fori_loop(0, BLK_DEV, fill, 0)

    def copies(s, k, blocks):
        u = (part_ref[0] + N_MP - s) % N_MP * MINE + k
        tiles = blocks * per_block
        copy = pltpu.make_async_copy(
            pieces[s].at[k, pl.ds(0, tiles)],
            out_ref.at[pl.ds(off_ref[u] * per_block, tiles)],
            sem.at[s, k],
        )
        return (len_ref[u] > BLOCK) == (blocks == MAXB), copy

    def each(act):
        for s in (1, 2, 3, 0):
            for k in range(RAW):
                for blocks in (1, MAXB):
                    when, copy = copies(s, k, blocks)
                    pl.when(when)(lambda copy=copy: act(copy))

    load.wait()
    each(lambda copy: copy.start())
    each(lambda copy: copy.wait())

    def filled(b, carry):
        @pl.when(used_s[b] == 0)
        def _():
            pltpu.make_async_copy(
                zero_v, out_ref.at[pl.ds(b * per_block, per_block)], sem_zero
            ).wait()

        return carry

    lax.fori_loop(0, BLK_DEV, filled, 0)


OUT_SHAPE = (BLK_DEV * BLOCK // TILE, TILE, HEAD)


def place_raw(pieces, lengths, offsets, part):
    return pl.pallas_call(
        place_raw_kernel,
        grid_spec=pltpu.PrefetchScalarGridSpec(
            num_scalar_prefetch=3,
            grid=(1,),
            in_specs=[in_hbm()] + [in_vmem()] * (N_MP - 1),
            out_specs=in_hbm(),
            scratch_shapes=[
                pltpu.VMEM((BLOCK // TILE, TILE, HEAD), BF16),
                pltpu.SMEM((BLK_DEV,), jnp.int32),
                pltpu.VMEM((RAW, GROUPS, TILE, HEAD), BF16),
                pltpu.SemaphoreType.DMA((N_MP, RAW)),
                pltpu.SemaphoreType.DMA,
                pltpu.SemaphoreType.DMA,
            ],
        ),
        out_shape=jax.ShapeDtypeStruct(OUT_SHAPE, BF16),
        compiler_params=pltpu.CompilerParams(vmem_limit_bytes=32 * 1024 * 1024),
        name="place_raw",
    )(lengths, offsets, part, pltpu.with_memory_space_constraint(pieces[0], pltpu.HBM), *pieces[1:])


def place_kernel(len_ref, off_ref, in_ref, partial_ref, out_ref, sem):
    per_block = BLOCK // TILE

    def each(act):
        def one(n, carry):
            m = n // DONE
            i = n % DONE
            u = m * MINE + RAW + i
            for blocks in (1, MAXB):
                tiles = blocks * per_block
                copy = pltpu.make_async_copy(
                    in_ref.at[i % HALVES, pl.ds(0, tiles), m, i // HALVES],
                    out_ref.at[pl.ds(off_ref[u] * per_block, tiles)],
                    sem.at[n],
                )
                pl.when((len_ref[u] > BLOCK) == (blocks == MAXB))(lambda copy=copy: act(copy))
            return carry

        lax.fori_loop(0, N_MP * DONE, one, 0)

    each(lambda copy: copy.start())
    each(lambda copy: copy.wait())


def place(arrived, partial, lengths, offsets):
    return pl.pallas_call(
        place_kernel,
        grid_spec=pltpu.PrefetchScalarGridSpec(
            num_scalar_prefetch=2,
            grid=(1,),
            in_specs=[in_vmem(), in_hbm()],
            out_specs=in_hbm(),
            scratch_shapes=[pltpu.SemaphoreType.DMA((N_MP * DONE,))],
        ),
        out_shape=jax.ShapeDtypeStruct(OUT_SHAPE, BF16),
        input_output_aliases={3: 0},
        compiler_params=pltpu.CompilerParams(vmem_limit_bytes=56 * 1024 * 1024),
        name="place",
    )(lengths, offsets, keep(arrived), partial).reshape(BLK_DEV * BLOCK, HEAD)


def along_mp(array, s):
    return lax.ppermute(array, "mp", [(i, (i + s) % N_MP) for i in range(N_MP)])


def per_device(tokens, w_uvqk, w_out, hist_len, owner, recv_offset, block_start):
    me = lax.axis_index("dp")
    part = lax.axis_index("mp")
    first = part * MINE
    core = me % 2
    seat = seat_of(me)
    half = seat // GROUPS
    part_1, core_1 = part[None], core[None]

    raw, mine_rows = pack(
        tokens, block_start, part_1, core_1, w_uvqk, owner, hist_len, recv_offset
    )
    swap = [(i, i ^ 1) for i in range(N_DP)]
    ring = [
        (d * N_MP + m, d * N_MP + (m + (1 if d % 2 == 0 else N_MP - 1)) % N_MP)
        for d in range(N_DP)
        for m in range(N_MP)
    ]
    side = lax.ppermute(w_uvqk, ("dp", "mp"), ring)
    across = along_mp(mine_rows, 2)
    other_side = lax.ppermute(side, "dp", swap)
    other_across = lax.ppermute(across, "dp", swap)
    weights = (side, other_side, across, other_across)
    raw_in = lax.all_to_all(
        raw.reshape(N_DP, RAW_MSG * TILE, HEAD), "dp", 0, 0, axis_index_groups=[SEATS], tiled=True
    ).reshape(N_DP, RAW_MSG, TILE, HEAD)
    kept = own_head(tokens, block_start, part_1, w_uvqk)
    message, last = layer(
        tokens, block_start, hist_len, part_1, core_1, kept, weights, w_out
    )
    message = merge(
        raw_in, (first + half)[None], message.reshape(N_DP, MSG, TILE, HEAD)
    )
    spread = lax.all_to_all(
        message.reshape(N_DP, MSG * TILE, HEAD), "dp", 0, 0, axis_index_groups=[SEATS], tiled=True
    ).reshape(N_DP, MSG, TILE, HEAD)
    _, raw_last = raw_layer(
        raw.reshape(N_DP, RAW_MSG, TILE, HEAD), 0, hist_len, part_1, core_1,
        w_uvqk, weights, w_out,
    )

    table = raw_in[:, N_MP, 0, :].astype(jnp.int32)
    owners = table[:, :USERS]
    held = lax.dynamic_slice_in_dim(owners, first + RAW + half, HALVES * (ROUND - 1) + 1, 1)
    ids = jnp.arange(N_DP, dtype=jnp.int32)
    source = jnp.sum(
        jnp.where(held[:, ::HALVES].T[:, None, :] == ids[None, :, None], ids[None, None, :], 0), axis=2
    ).reshape(-1)
    mine = owners == seat
    recv_len = jnp.sum(jnp.where(mine, table[:, USERS : 2 * USERS], 0), axis=0)
    recv_off = jnp.sum(jnp.where(mine, table[:, 2 * USERS : 3 * USERS], 0), axis=0)

    sorted_rows = regroup(spread, source)
    arrived = lax.all_to_all(
        sorted_rows.reshape(N_DP * N_MP, ROUND * TILE, HEAD), ("dp", "mp"), 0, 0,
        axis_index_groups=[[d * N_MP + m for d in SEATS for m in range(N_MP)]], tiled=True
    )
    pieces, _ = raw_layer(
        spread, ROUND * N_MP, recv_len[None], part_1, core_1,
        w_uvqk, weights, w_out,
    )
    pieces = [pieces[0]] + [along_mp(pieces[s], s) for s in range(1, N_MP)]
    partial = place_raw(pieces, recv_len, recv_off, part_1)
    packed = place(
        arrived.reshape(HALVES, GROUPS, N_MP, ROUND, TILE, HEAD), partial, recv_len, recv_off
    )

    columns = jnp.concatenate([raw_last, last], axis=0).reshape(MINE, N_MP, HEAD)
    state = jnp.zeros((N_MP, MINE, HEAD), BF16)
    for s in range(N_MP):
        to_part = (part + s) % N_MP
        piece = lax.dynamic_slice_in_dim(columns, to_part, 1, 1)[:, 0]
        if s:
            piece = along_mp(piece, s)
        state = lax.dynamic_update_slice_in_dim(state, piece[None], (part - s) % N_MP, 0)
    return packed, state.reshape(USERS, HEAD)


def solution(mesh):
    in_specs = (
        P("dp", None),
        P(None, "mp"),
        P(),
        P("dp", None),
        P("dp", None),
        P("dp", None),
        P("dp", None),
    )
    out_specs = (P("dp", "mp"), P("dp", "mp"))
    return jax.shard_map(
        per_device, mesh=mesh, in_specs=in_specs, out_specs=out_specs, check_vma=False
    )
```

```python
import jax
import jax.numpy as jnp
from jax import lax
from jax.experimental import pallas as pl
from jax.experimental.pallas import tpu as pltpu
from jax.sharding import PartitionSpec as P

D = 512
HEADS = 4
HEAD = D // HEADS
BLOCK = 128
MAXB = 2
BLK_DEV = 48
USERS = 24
N_DP = 64
N_MP = 4
WIN = MAXB * BLOCK
MINE = USERS // N_MP
RAW = 2
DONE = MINE - RAW
TILE = 8
GROUPS = WIN // TILE
HALVES = N_DP // GROUPS
GROUP = 2
OWN_GROUP = 2
CHUNKS = 4
SEATS = list(range(N_DP - 1, -1, -1))
RAW_MSG = N_MP + 1
ROUND = DONE // HALVES
MSG = (ROUND + 1) * N_MP
EPS = 1e-05
BF16 = jnp.bfloat16
F32 = jnp.float32


def silu_of_twice(h):
    return h + h * jnp.tanh(h)


def project(half_parts, w_parts):
    acc = jnp.dot(half_parts[0], w_parts[0], preferred_element_type=F32)
    for n, w in zip(half_parts[1:], w_parts[1:]):
        acc = acc + jnp.dot(n, w, preferred_element_type=F32)
    proj = silu_of_twice(acc).astype(BF16)
    return [proj[:, j * HEAD : (j + 1) * HEAD] for j in range(4)]


def attend(q, k, v):
    row = lax.broadcasted_iota(jnp.int32, (BLOCK, BLOCK), 0)
    col = lax.broadcasted_iota(jnp.int32, (BLOCK, BLOCK), 1)
    causal = col <= row
    scale = 0.5 * HEAD ** (-0.5)
    contract_last = (((1,), (1,)), ((), ()))
    s0 = lax.dot_general(q[:BLOCK], k[:BLOCK], contract_last, preferred_element_type=F32)
    s1 = lax.dot_general(q[BLOCK:], k, contract_last, preferred_element_type=F32)
    a0 = jnp.where(causal, silu_of_twice(s0 * scale), 0.0).astype(BF16)
    b = silu_of_twice(s1 * scale)
    a1 = jnp.concatenate(
        [b[:, :BLOCK].astype(BF16), jnp.where(causal, b[:, BLOCK:], 0.0).astype(BF16)], axis=1
    )
    return jnp.concatenate(
        [
            jnp.dot(a0, v[:BLOCK], preferred_element_type=F32),
            jnp.dot(a1, v, preferred_element_type=F32),
        ],
        axis=0,
    )


def norm_stats(total, squares, unit=1.0):
    mean = total * (1.0 / D)
    var = squares * (1.0 / D) - mean * mean
    return mean, lax.rsqrt(var * (unit * unit) + EPS) * unit


def token_copies(tokens_ref, block, x_ref, row, sem):
    second = jnp.minimum(block + 1, BLK_DEV - 1)
    return [
        pltpu.make_async_copy(
            tokens_ref.at[pl.ds(b * BLOCK, BLOCK)],
            x_ref.at[pl.ds(row + j * BLOCK, BLOCK)],
            sem.at[j],
        )
        for j, b in enumerate((block, second))
    ]


def norm_half(x):
    mean, inv = norm_stats(
        jnp.sum(x, axis=1, keepdims=True), jnp.sum(x * x, axis=1, keepdims=True)
    )
    return ((x - mean) * (inv * 0.5)).astype(BF16)


def own_head_kernel(
    start_ref, part_ref, tokens_ref, w_ref, half_ref, att_ref, gate_ref,
    x_s, half_s, att_s, gate_s, w_s, sem_in, sem_w, sem_out,
):
    load_w = pltpu.make_async_copy(w_ref, w_s, sem_w)

    def loads(i):
        block = start_ref[0, part_ref[0] * MINE + RAW + i]
        return token_copies(tokens_ref, block, x_s, i * WIN, sem_in.at[i])

    def sends(step):
        rows = pl.ds(step * OWN_GROUP * WIN, OWN_GROUP * WIN)
        pairs = ((half_s, half_ref), (att_s, att_ref), (gate_s, gate_ref))
        return [
            pltpu.make_async_copy(a.at[rows], b.at[rows], sem_out.at[step, j])
            for j, (a, b) in enumerate(pairs)
        ]

    for i in range(DONE):
        for copy in loads(i):
            copy.start()
        if i == OWN_GROUP - 1:
            load_w.start()

    def group(step, carry):
        for j in range(OWN_GROUP):
            for copy in loads(step * OWN_GROUP + j):
                copy.wait()
        rows = pl.ds(pl.multiple_of(step * OWN_GROUP * WIN, WIN), OWN_GROUP * WIN)
        half = norm_half(x_s[rows, :].astype(F32))
        half_s[rows, :] = half

        @pl.when(step == 0)
        def _():
            load_w.wait()

        u, v, q, k = project([half], [w_s[...]])
        gate_s[rows, :] = u
        att_s[rows, :] = attend_users(OWN_GROUP, q, k, v)
        for copy in sends(step):
            copy.start()
        return carry

    lax.fori_loop(0, DONE // OWN_GROUP, group, 0)
    for step in range(DONE // OWN_GROUP):
        for copy in sends(step):
            copy.wait()


def in_vmem():
    return pl.BlockSpec(memory_space=pltpu.VMEM)


def in_hbm():
    return pl.BlockSpec(memory_space=pltpu.HBM)


def keep(array):
    return pltpu.with_memory_space_constraint(array, pltpu.VMEM)


def own_head(tokens, starts, part, w_own):
    kept = [((DONE * WIN, D), BF16), ((DONE * WIN, HEAD), F32), ((DONE * WIN, HEAD), BF16)]
    return pl.pallas_call(
        own_head_kernel,
        grid_spec=pltpu.PrefetchScalarGridSpec(
            num_scalar_prefetch=2,
            grid=(1,),
            in_specs=[in_hbm()] * 2,
            out_specs=[in_hbm()] * 3,
            scratch_shapes=[pltpu.VMEM((DONE * WIN, D), BF16)]
            + [pltpu.VMEM(*k) for k in kept]
            + [
                pltpu.VMEM((D, D), BF16),
                pltpu.SemaphoreType.DMA((DONE, MAXB)),
                pltpu.SemaphoreType.DMA,
                pltpu.SemaphoreType.DMA((DONE // OWN_GROUP, 3)),
            ],
        ),
        out_shape=[jax.ShapeDtypeStruct(*k) for k in kept],
        cost_estimate=pl.CostEstimate(
            flops=DONE * WIN * D * D * 64, bytes_accessed=DONE * WIN * D * 8, transcendentals=0
        ),
        name="own_head",
    )(starts, part, tokens, w_own)


def rows_of(tiles):
    return jnp.concatenate(
        [tiles[..., q, :, :].reshape(-1, HEAD) for q in range(N_MP)], axis=1
    )


def pack_kernel(
    start_ref, part_ref, core_ref, tokens_ref, w_ref, owner_ref, len_ref, off_ref,
    out_ref, rows_ref, x_s, table_s, row_s, out_s, sem, sem_t, sem_w, sem_out,
):
    tables = [
        pltpu.make_async_copy(ref, table_s.at[j], sem_t.at[j])
        for j, ref in enumerate((owner_ref, len_ref, off_ref))
    ]
    half = D // 2
    weights = pltpu.make_async_copy(w_ref.at[pl.ds(core_ref[0] * half, half)], rows_ref, sem_w)
    loads = [
        token_copies(
            tokens_ref, start_ref[0, part_ref[0] * MINE + k], x_s, k * WIN, sem.at[k]
        )
        for k in range(RAW)
    ]
    for copy in tables + loads[0] + [weights] + loads[1]:
        copy.start()
    row_s[...] = jnp.zeros_like(row_s)
    for j, copy in enumerate(tables):
        copy.wait()
        row_s[:, j * USERS : (j + 1) * USERS] = table_s[j] if j else N_DP - 1 - table_s[j]
    tile = jnp.broadcast_to(row_s[...], (TILE, 128)).astype(F32).astype(BF16)
    for k in range(RAW):
        out_s[k, :, N_MP] = jnp.broadcast_to(tile[None], (GROUPS, TILE, 128))
    sends = [pltpu.make_async_copy(out_s.at[k], out_ref.at[k], sem_out.at[k]) for k in range(RAW)]
    for k in range(RAW):
        for copy in loads[k]:
            copy.wait()
        for q in range(N_MP):
            out_s[k, :, q] = x_s[k * WIN : (k + 1) * WIN, q * HEAD : (q + 1) * HEAD].reshape(
                GROUPS, TILE, HEAD
            )
        sends[k].start()
    weights.wait()
    for copy in sends:
        copy.wait()


def pack(tokens, starts, part, core, w_own, owner, hist_len, recv_offset):
    shape = (RAW, GROUPS, RAW_MSG, TILE, HEAD)
    return pl.pallas_call(
        pack_kernel,
        grid_spec=pltpu.PrefetchScalarGridSpec(
            num_scalar_prefetch=3,
            grid=(1,),
            in_specs=[in_hbm()] * 5,
            out_specs=[in_hbm(), in_vmem()],
            scratch_shapes=[
                pltpu.VMEM((RAW * WIN, D), BF16),
                pltpu.VMEM((3, 1, USERS), jnp.int32),
                pltpu.VMEM((1, 128), jnp.int32),
                pltpu.VMEM(shape, BF16),
                pltpu.SemaphoreType.DMA((RAW, MAXB)),
                pltpu.SemaphoreType.DMA((3,)),
                pltpu.SemaphoreType.DMA,
                pltpu.SemaphoreType.DMA((RAW,)),
            ],
        ),
        out_shape=[jax.ShapeDtypeStruct(shape, BF16), pltpu.VMEM((D // 2, D), BF16)],
        name="pack",
    )(starts, part, core, tokens, w_own, owner, hist_len, recv_offset)


def head_order(part, core):
    down, up = (part + HEADS - 1) % HEADS, (part + 1) % HEADS
    first = core == 0
    return [part, jnp.where(first, down, up), jnp.where(first, up, down), (part + 2) % HEADS]


def mix(low_is_near, half_rows, first, whole, halves, w_out_of, x_rows):
    low = half_rows[:, : D // 2]
    high = half_rows[:, D // 2 :]
    parts = [jnp.where(low_is_near, low, high), jnp.where(low_is_near, high, low)]
    users = half_rows.shape[0] // WIN
    heads, gates = [first[0]], [first[1]]
    for rows, refs in (([half_rows], whole[:1]), ([half_rows], whole[1:]), (parts, halves)):
        u, v, q, k = project(rows, [ref[...] for ref in refs])
        gates.append(u)
        heads.append(attend_users(users, q, k, v))
    total = jnp.sum(heads[0] + heads[1] + (heads[2] + heads[3]), axis=1, keepdims=True)
    squares = jnp.sum(
        heads[0] * heads[0] + heads[1] * heads[1] + (heads[2] * heads[2] + heads[3] * heads[3]),
        axis=1,
        keepdims=True,
    )
    mean, inv = norm_stats(total, squares, 1.0 / WIN)
    gated = jnp.concatenate(
        [((a - mean) * inv * g.astype(F32)).astype(BF16) for a, g in zip(heads, gates)], axis=1
    )
    return jnp.dot(gated, w_out_of(), preferred_element_type=F32) + x_rows().astype(F32)


def attend_users(users, q, k, v):
    return jnp.concatenate(
        [attend(*(t[j * WIN : (j + 1) * WIN] for t in (q, k, v))) for j in range(users)], axis=0
    )


def live_rows(mixed, length):
    at = lax.broadcasted_iota(jnp.int32, (WIN, 1), 0)
    return jnp.where(at < length, mixed, 0.0).astype(BF16)


def last_row(tile, length):
    pick = lax.broadcasted_iota(jnp.int32, (TILE, HEAD), 0) == (length - 1) % TILE
    return jnp.sum(jnp.where(pick, tile.astype(F32), 0.0), axis=0, keepdims=True).astype(BF16)


def w_out_copies(part, core, w_out_ref, w_out_s, sem):
    return [
        pltpu.make_async_copy(
            w_out_ref.at[pl.ds(h * HEAD, HEAD)], w_out_s.at[pl.ds(s * HEAD, HEAD)], sem.at[s]
        )
        for s, h in enumerate(head_order(part, core))
    ]


def layer_kernel(
    start_ref, len_ref, part_ref, core_ref, tokens_ref, half_hbm, att_hbm, gate_hbm, *rest
):
    whole, halves, (w_out_ref, out_ref, state_ref) = rest[:2], rest[2:4], rest[4:7]
    x_s, half_s, att_s, gate_s, w_out_s, out_s, sem_in, sem_w, sem_out = rest[7:]
    low_is_near = core_ref[0] == 0
    first_id = part_ref[0] * MINE + RAW

    def loads(i):
        rows = pl.ds(i * WIN, WIN)
        pairs = ((half_hbm, half_s), (att_hbm, att_s), (gate_hbm, gate_s))
        return [
            pltpu.make_async_copy(a.at[rows], b.at[rows], sem_in.at[i, MAXB + j])
            for j, (a, b) in enumerate(pairs)
        ] + token_copies(tokens_ref, start_ref[0, first_id + i], x_s, i * WIN, sem_in.at[i])

    weights = w_out_copies(part_ref[0], core_ref[0], w_out_ref, w_out_s, sem_w)

    def sends(i):
        at = (i % HALVES, slice(None), pl.ds((i // HALVES) * N_MP, N_MP))
        return pltpu.make_async_copy(out_s.at[at], out_ref.at[at], sem_out.at[i])

    for i in range(DONE):
        for copy in loads(i):
            copy.start()
        if i == GROUP - 1:
            for copy in weights:
                copy.start()

    def group(step, carry):
        first_user = step * GROUP
        for j in range(GROUP):
            for copy in loads(first_user + j):
                copy.wait()
        rows = pl.ds(pl.multiple_of(first_user * WIN, WIN), GROUP * WIN)

        def w_out_of():
            @pl.when(step == 0)
            def _():
                for copy in weights:
                    copy.wait()

            return w_out_s[...]

        both = mix(
            low_is_near,
            half_s[rows, :],
            (att_s[rows, :], gate_s[rows, :]),
            whole,
            halves,
            w_out_of,
            lambda: x_s[rows, :],
        )
        for j in range(GROUP):
            i = first_user + j
            length = len_ref[0, first_id + i]
            half_id = i % HALVES
            base = (i // HALVES) * N_MP
            mixed = live_rows(both[j * WIN : (j + 1) * WIN], length)
            for q in range(N_MP):
                out_s[half_id, :, base + q] = mixed[:, q * HEAD : (q + 1) * HEAD].reshape(
                    GROUPS, TILE, HEAD
                )
            sends(i).start()
            for q in range(N_MP):
                state_ref[i, :, q * HEAD : (q + 1) * HEAD] = last_row(
                    out_s[half_id, (length - 1) // TILE, base + q], length
                )
        return carry

    lax.fori_loop(0, DONE // GROUP, group, 0)
    for i in range(DONE):
        sends(i).wait()


def layer(tokens, starts, lengths, part, core, kept, weights, w_out):
    message = (HALVES, GROUPS, MSG, TILE, HEAD)
    return pl.pallas_call(
        layer_kernel,
        grid_spec=pltpu.PrefetchScalarGridSpec(
            num_scalar_prefetch=4,
            grid=(1,),
            in_specs=[in_hbm()] * 4 + [in_vmem()] * 4 + [in_hbm()],
            out_specs=[in_hbm(), in_vmem()],
            scratch_shapes=[
                pltpu.VMEM((DONE * WIN, D), BF16),
                pltpu.VMEM((DONE * WIN, D), BF16),
                pltpu.VMEM((DONE * WIN, HEAD), F32),
                pltpu.VMEM((DONE * WIN, HEAD), BF16),
                pltpu.VMEM((D, D), BF16),
                pltpu.VMEM((HALVES, GROUPS, ROUND * N_MP, TILE, HEAD), BF16),
                pltpu.SemaphoreType.DMA((DONE, 5)),
                pltpu.SemaphoreType.DMA((HEADS,)),
                pltpu.SemaphoreType.DMA((DONE,)),
            ],
        ),
        out_shape=[
            jax.ShapeDtypeStruct(message, BF16),
            jax.ShapeDtypeStruct((DONE, 1, D), BF16),
        ],
        name="layer",
    )(starts, lengths, part, core, tokens, *kept, *map(keep, weights), w_out)


def raw_kernel(first_tile, len_ref, part_ref, core_ref, src_ref, w_own_ref, *rest):
    whole, halves, w_out_ref = rest[:2], rest[2:4], rest[4]
    pieces = rest[5 : 5 + N_MP]
    state_ref, x_s, w_out_s, mixed_s, sem_x, sem_w = rest[5 + N_MP :]
    part = part_ref[0]
    lengths = [len_ref[0, part * MINE + k] for k in range(RAW)]
    loads = [
        pltpu.make_async_copy(
            src_ref.at[pl.ds(k * GROUPS, GROUPS), pl.ds(first_tile, N_MP)], x_s.at[k], sem_x.at[k]
        )
        for k in range(RAW)
    ]
    weights = w_out_copies(part, core_ref[0], w_out_ref, w_out_s, sem_w)
    for copy in loads + weights:
        copy.start()
    for copy in loads:
        copy.wait()

    def x_rows():
        return rows_of(x_s[...])

    half = norm_half(x_rows().astype(F32))
    u, v, q, k = project([half], [w_own_ref[...]])

    def w_out_of():
        for copy in weights:
            copy.wait()
        return w_out_s[...]

    both = mix(
        core_ref[0] == 0, half, (attend_users(RAW, q, k, v), u), whole, halves, w_out_of, x_rows
    )
    for k in range(RAW):
        mixed = live_rows(both[k * WIN : (k + 1) * WIN], lengths[k])
        for q in range(N_MP):
            mixed_s[q, k] = mixed[:, q * HEAD : (q + 1) * HEAD].reshape(GROUPS, TILE, HEAD)
        for q in range(N_MP):
            state_ref[k, :, q * HEAD : (q + 1) * HEAD] = last_row(
                mixed_s[q, k, (lengths[k] - 1) // TILE], lengths[k]
            )
    for s in range(N_MP):
        pieces[s][...] = mixed_s[(part + s) % N_MP]


def raw_layer(source, first_tile, lengths, part, core, w_own, weights, w_out):
    piece = jax.ShapeDtypeStruct((RAW, GROUPS, TILE, HEAD), BF16)
    outs = pl.pallas_call(
        lambda *refs: raw_kernel(first_tile, *refs),
        grid_spec=pltpu.PrefetchScalarGridSpec(
            num_scalar_prefetch=3,
            grid=(1,),
            in_specs=[in_hbm()] + [in_vmem()] * 5 + [in_hbm()],
            out_specs=[in_vmem()] * (N_MP + 1),
            scratch_shapes=[
                pltpu.VMEM((RAW, GROUPS, N_MP, TILE, HEAD), BF16),
                pltpu.VMEM((D, D), BF16),
                pltpu.VMEM((N_MP, RAW, GROUPS, TILE, HEAD), BF16),
                pltpu.SemaphoreType.DMA((RAW,)),
                pltpu.SemaphoreType.DMA((HEADS,)),
            ],
        ),
        out_shape=[piece] * N_MP + [jax.ShapeDtypeStruct((RAW, 1, D), BF16)],
    )(lengths, part, core, source, w_own, *weights, w_out)
    return outs[:N_MP], outs[N_MP]


def merge_kernel(first_ref, in_ref, msg_ref, out_ref, sorted_s, table_v, table_s, sem):
    lane = lax.broadcasted_iota(jnp.int32, (TILE, 128), 1)
    column = (lane == first_ref[0]).astype(F32).astype(BF16)
    tiles = in_ref[:, N_MP].reshape(N_DP * TILE, 128)
    seats = lax.dot_general(column, tiles, (((1,), (1,)), ((), ())), preferred_element_type=F32)
    table_v[...] = seats.astype(jnp.int32)
    copy = pltpu.make_async_copy(table_v.at[pl.ds(0, 1)], table_s, sem.at[0])
    copy.start()
    copy.wait()

    def one(d, carry):
        o = table_s[0, d * TILE]
        for q in range(N_MP):
            sorted_s[o, q] = in_ref[d, q]
        return carry

    lax.fori_loop(0, N_DP, one, 0, unroll=8)
    send = pltpu.make_async_copy(sorted_s, out_ref.at[:, pl.ds(ROUND * N_MP, N_MP)], sem.at[1])
    send.start()
    send.wait()


def merge(spread, first, message):
    return pl.pallas_call(
        merge_kernel,
        grid_spec=pltpu.PrefetchScalarGridSpec(
            num_scalar_prefetch=1,
            grid=(1,),
            in_specs=[in_vmem(), in_hbm()],
            out_specs=in_hbm(),
            scratch_shapes=[
                pltpu.VMEM((N_DP, N_MP, TILE, HEAD), BF16),
                pltpu.VMEM((TILE, N_DP * TILE), jnp.int32),
                pltpu.SMEM((1, N_DP * TILE), jnp.int32),
                pltpu.SemaphoreType.DMA((2,)),
            ],
        ),
        out_shape=jax.ShapeDtypeStruct((N_DP, MSG, TILE, HEAD), BF16),
        input_output_aliases={2: 0},
        name="merge",
    )(first, keep(spread), message)


def regroup_kernel(from_ref, in_ref, out_ref, out_s, sem):
    chunk = N_DP // CHUNKS

    def send(c):
        at = (slice(None), pl.ds(c * chunk, chunk))
        return pltpu.make_async_copy(out_s.at[at], out_ref.at[at], sem.at[c])

    def one(c, carry):
        for j in range(chunk):
            o = c * chunk + j
            for r in range(ROUND):
                d = from_ref[r * N_DP + o]
                for q in range(N_MP):
                    out_s[q, o, r] = in_ref[d, r * N_MP + q]
        send(c).start()
        return carry

    lax.fori_loop(0, CHUNKS, one, 0)
    for c in range(CHUNKS):
        send(c).wait()


def regroup(spread, source):
    shape = (N_MP, N_DP, ROUND, TILE, HEAD)
    return pl.pallas_call(
        regroup_kernel,
        grid_spec=pltpu.PrefetchScalarGridSpec(
            num_scalar_prefetch=1,
            grid=(1,),
            in_specs=[in_vmem()],
            out_specs=in_hbm(),
            scratch_shapes=[pltpu.VMEM(shape, BF16), pltpu.SemaphoreType.DMA((CHUNKS,))],
        ),
        out_shape=jax.ShapeDtypeStruct(shape, BF16),
        name="regroup",
    )(source, keep(spread))


def place_raw_kernel(len_ref, off_ref, part_ref, own_ref, *rest):
    out_ref, zero_v, used_s, own_s, sem, sem_zero, sem_own = rest[N_MP - 1 :]
    pieces = (own_s, *rest[: N_MP - 1])
    per_block = BLOCK // TILE
    load = pltpu.make_async_copy(own_ref, own_s, sem_own)
    load.start()
    zero_v[...] = jnp.zeros_like(zero_v)

    def clear(b, carry):
        used_s[b] = 0
        return carry

    lax.fori_loop(0, BLK_DEV, clear, 0, unroll=8)

    def mark(u, carry):
        used_s[off_ref[u]] = 1

        @pl.when(len_ref[u] > BLOCK)
        def _():
            used_s[off_ref[u] + 1] = 1

        return carry

    lax.fori_loop(0, USERS, mark, 0)

    def fill(b, carry):
        @pl.when(used_s[b] == 0)
        def _():
            pltpu.make_async_copy(
                zero_v, out_ref.at[pl.ds(b * per_block, per_block)], sem_zero
            ).start()

        return carry

    lax.fori_loop(0, BLK_DEV, fill, 0)

    def copies(s, k, blocks):
        u = (part_ref[0] + N_MP - s) % N_MP * MINE + k
        tiles = blocks * per_block
        copy = pltpu.make_async_copy(
            pieces[s].at[k, pl.ds(0, tiles)],
            out_ref.at[pl.ds(off_ref[u] * per_block, tiles)],
            sem.at[s, k],
        )
        return (len_ref[u] > BLOCK) == (blocks == MAXB), copy

    def each(act):
        for s in (1, 2, 3, 0):
            for k in range(RAW):
                for blocks in (1, MAXB):
                    when, copy = copies(s, k, blocks)
                    pl.when(when)(lambda copy=copy: act(copy))

    load.wait()
    each(lambda copy: copy.start())
    each(lambda copy: copy.wait())

    def filled(b, carry):
        @pl.when(used_s[b] == 0)
        def _():
            pltpu.make_async_copy(
                zero_v, out_ref.at[pl.ds(b * per_block, per_block)], sem_zero
            ).wait()

        return carry

    lax.fori_loop(0, BLK_DEV, filled, 0)


OUT_SHAPE = (BLK_DEV * BLOCK // TILE, TILE, HEAD)


def place_raw(pieces, lengths, offsets, part):
    return pl.pallas_call(
        place_raw_kernel,
        grid_spec=pltpu.PrefetchScalarGridSpec(
            num_scalar_prefetch=3,
            grid=(1,),
            in_specs=[in_hbm()] + [in_vmem()] * (N_MP - 1),
            out_specs=in_hbm(),
            scratch_shapes=[
                pltpu.VMEM((BLOCK // TILE, TILE, HEAD), BF16),
                pltpu.SMEM((BLK_DEV,), jnp.int32),
                pltpu.VMEM((RAW, GROUPS, TILE, HEAD), BF16),
                pltpu.SemaphoreType.DMA((N_MP, RAW)),
                pltpu.SemaphoreType.DMA,
                pltpu.SemaphoreType.DMA,
            ],
        ),
        out_shape=jax.ShapeDtypeStruct(OUT_SHAPE, BF16),
        compiler_params=pltpu.CompilerParams(vmem_limit_bytes=32 * 1024 * 1024),
        name="place_raw",
    )(lengths, offsets, part, pltpu.with_memory_space_constraint(pieces[0], pltpu.HBM), *pieces[1:])


def place_kernel(len_ref, off_ref, in_ref, partial_ref, out_ref, sem):
    per_block = BLOCK // TILE

    def each(act):
        def one(n, carry):
            m = n // DONE
            i = n % DONE
            u = m * MINE + RAW + i
            for blocks in (1, MAXB):
                tiles = blocks * per_block
                copy = pltpu.make_async_copy(
                    in_ref.at[m, i % HALVES, pl.ds(0, tiles), i // HALVES],
                    out_ref.at[pl.ds(off_ref[u] * per_block, tiles)],
                    sem.at[n],
                )
                pl.when((len_ref[u] > BLOCK) == (blocks == MAXB))(lambda copy=copy: act(copy))
            return carry

        lax.fori_loop(0, N_MP * DONE, one, 0)

    each(lambda copy: copy.start())
    each(lambda copy: copy.wait())


def place(arrived, partial, lengths, offsets):
    return pl.pallas_call(
        place_kernel,
        grid_spec=pltpu.PrefetchScalarGridSpec(
            num_scalar_prefetch=2,
            grid=(1,),
            in_specs=[in_vmem(), in_hbm()],
            out_specs=in_hbm(),
            scratch_shapes=[pltpu.SemaphoreType.DMA((N_MP * DONE,))],
        ),
        out_shape=jax.ShapeDtypeStruct(OUT_SHAPE, BF16),
        input_output_aliases={3: 0},
        compiler_params=pltpu.CompilerParams(vmem_limit_bytes=56 * 1024 * 1024),
        name="place",
    )(lengths, offsets, keep(arrived), partial).reshape(BLK_DEV * BLOCK, HEAD)


def along_mp(array, s):
    return lax.ppermute(array, "mp", [(i, (i + s) % N_MP) for i in range(N_MP)])


def per_device(tokens, w_uvqk, w_out, hist_len, owner, recv_offset, block_start):
    me = lax.axis_index("dp")
    part = lax.axis_index("mp")
    first = part * MINE
    core = me % 2
    seat = N_DP - 1 - me
    half = seat // GROUPS
    part_1, core_1 = part[None], core[None]

    raw, mine_rows = pack(
        tokens, block_start, part_1, core_1, w_uvqk, owner, hist_len, recv_offset
    )
    swap = [(i, i ^ 1) for i in range(N_DP)]
    ring = [
        (d * N_MP + m, d * N_MP + (m + (1 if d % 2 == 0 else N_MP - 1)) % N_MP)
        for d in range(N_DP)
        for m in range(N_MP)
    ]
    side = lax.ppermute(w_uvqk, ("dp", "mp"), ring)
    across = along_mp(mine_rows, 2)
    other_side = lax.ppermute(side, "dp", swap)
    other_across = lax.ppermute(across, "dp", swap)
    weights = (side, other_side, across, other_across)
    raw_in = lax.all_to_all(
        raw.reshape(N_DP, RAW_MSG * TILE, HEAD), "dp", 0, 0, axis_index_groups=[SEATS], tiled=True
    ).reshape(N_DP, RAW_MSG, TILE, HEAD)
    kept = own_head(tokens, block_start, part_1, w_uvqk)
    message, last = layer(
        tokens, block_start, hist_len, part_1, core_1, kept, weights, w_out
    )
    message = merge(
        raw_in, (first + half)[None], message.reshape(N_DP, MSG, TILE, HEAD)
    )
    spread = lax.all_to_all(
        message.reshape(N_DP, MSG * TILE, HEAD), "dp", 0, 0, axis_index_groups=[SEATS], tiled=True
    ).reshape(N_DP, MSG, TILE, HEAD)
    _, raw_last = raw_layer(
        raw.reshape(N_DP, RAW_MSG, TILE, HEAD), 0, hist_len, part_1, core_1,
        w_uvqk, weights, w_out,
    )

    table = raw_in[:, N_MP, 0, :].astype(jnp.int32)
    owners = table[:, :USERS]
    held = lax.dynamic_slice_in_dim(owners, first + RAW + half, HALVES * (ROUND - 1) + 1, 1)
    ids = jnp.arange(N_DP, dtype=jnp.int32)
    source = jnp.sum(
        jnp.where(held[:, ::HALVES].T[:, None, :] == ids[None, :, None], ids[None, None, :], 0), axis=2
    ).reshape(-1)
    mine = owners == seat
    recv_len = jnp.sum(jnp.where(mine, table[:, USERS : 2 * USERS], 0), axis=0)
    recv_off = jnp.sum(jnp.where(mine, table[:, 2 * USERS : 3 * USERS], 0), axis=0)

    sorted_rows = regroup(spread, source)
    arrived = lax.all_to_all(
        sorted_rows.reshape(N_DP * N_MP, ROUND * TILE, HEAD), ("dp", "mp"), 0, 0,
        axis_index_groups=[[d * N_MP + m for m in range(N_MP) for d in SEATS]], tiled=True
    )
    pieces, _ = raw_layer(
        spread, ROUND * N_MP, recv_len[None], part_1, core_1,
        w_uvqk, weights, w_out,
    )
    pieces = [pieces[0]] + [along_mp(pieces[s], s) for s in range(1, N_MP)]
    partial = place_raw(pieces, recv_len, recv_off, part_1)
    packed = place(
        arrived.reshape(N_MP, HALVES, GROUPS, ROUND, TILE, HEAD), partial, recv_len, recv_off
    )

    columns = jnp.concatenate([raw_last, last], axis=0).reshape(MINE, N_MP, HEAD)
    state = jnp.zeros((N_MP, MINE, HEAD), BF16)
    for s in range(N_MP):
        to_part = (part + s) % N_MP
        piece = lax.dynamic_slice_in_dim(columns, to_part, 1, 1)[:, 0]
        if s:
            piece = along_mp(piece, s)
        state = lax.dynamic_update_slice_in_dim(state, piece[None], (part - s) % N_MP, 0)
    return packed, state.reshape(USERS, HEAD)


def solution(mesh):
    in_specs = (
        P("dp", None),
        P(None, "mp"),
        P(),
        P("dp", None),
        P("dp", None),
        P("dp", None),
        P("dp", None),
    )
    out_specs = (P("dp", "mp"), P("dp", "mp"))
    return jax.shard_map(
        per_device, mesh=mesh, in_specs=in_specs, out_specs=out_specs, check_vma=False
    )
```

```python
import jax
import jax.numpy as jnp
from jax import lax
from jax.experimental import pallas as pl
from jax.experimental.pallas import tpu as pltpu
from jax.sharding import PartitionSpec as P

D = 512
HEADS = 4
HEAD = D // HEADS
BLOCK = 128
MAXB = 2
BLK_DEV = 48
USERS = 24
N_DP = 64
N_MP = 4
WIN = MAXB * BLOCK
MINE = USERS // N_MP
RAW = 2
DONE = MINE - RAW
TILE = 8
GROUPS = WIN // TILE
HALVES = N_DP // GROUPS
GROUP = 2
OWN_GROUP = 2
CHUNKS = 8
SEATS = list(range(N_DP - 1, -1, -1))
RAW_MSG = N_MP + 1
ROUND = DONE // HALVES
MSG = (ROUND + 1) * N_MP
EPS = 1e-05
BF16 = jnp.bfloat16
F32 = jnp.float32


def silu_of_twice(h):
    return h + h * jnp.tanh(h)


def project(half_parts, w_parts):
    acc = jnp.dot(half_parts[0], w_parts[0], preferred_element_type=F32)
    for n, w in zip(half_parts[1:], w_parts[1:]):
        acc = acc + jnp.dot(n, w, preferred_element_type=F32)
    proj = silu_of_twice(acc).astype(BF16)
    return [proj[:, j * HEAD : (j + 1) * HEAD] for j in range(4)]


def attend(q, k, v):
    row = lax.broadcasted_iota(jnp.int32, (BLOCK, BLOCK), 0)
    col = lax.broadcasted_iota(jnp.int32, (BLOCK, BLOCK), 1)
    causal = col <= row
    scale = 0.5 * HEAD ** (-0.5)
    contract_last = (((1,), (1,)), ((), ()))
    s0 = lax.dot_general(q[:BLOCK], k[:BLOCK], contract_last, preferred_element_type=F32)
    s1 = lax.dot_general(q[BLOCK:], k, contract_last, preferred_element_type=F32)
    a0 = jnp.where(causal, silu_of_twice(s0 * scale), 0.0).astype(BF16)
    b = silu_of_twice(s1 * scale)
    a1 = jnp.concatenate(
        [b[:, :BLOCK].astype(BF16), jnp.where(causal, b[:, BLOCK:], 0.0).astype(BF16)], axis=1
    )
    return jnp.concatenate(
        [
            jnp.dot(a0, v[:BLOCK], preferred_element_type=F32),
            jnp.dot(a1, v, preferred_element_type=F32),
        ],
        axis=0,
    )


def norm_stats(total, squares, unit=1.0):
    mean = total * (1.0 / D)
    var = squares * (1.0 / D) - mean * mean
    return mean, lax.rsqrt(var * (unit * unit) + EPS) * unit


def token_copies(tokens_ref, block, x_ref, row, sem):
    second = jnp.minimum(block + 1, BLK_DEV - 1)
    return [
        pltpu.make_async_copy(
            tokens_ref.at[pl.ds(b * BLOCK, BLOCK)],
            x_ref.at[pl.ds(row + j * BLOCK, BLOCK)],
            sem.at[j],
        )
        for j, b in enumerate((block, second))
    ]


def norm_half(x):
    mean, inv = norm_stats(
        jnp.sum(x, axis=1, keepdims=True), jnp.sum(x * x, axis=1, keepdims=True)
    )
    return ((x - mean) * (inv * 0.5)).astype(BF16)


def own_head_kernel(
    start_ref, part_ref, tokens_ref, w_ref, half_ref, att_ref, gate_ref,
    x_s, half_s, att_s, gate_s, w_s, sem_in, sem_w, sem_out,
):
    load_w = pltpu.make_async_copy(w_ref, w_s, sem_w)

    def loads(i):
        block = start_ref[0, part_ref[0] * MINE + RAW + i]
        return token_copies(tokens_ref, block, x_s, i * WIN, sem_in.at[i])

    def sends(step):
        rows = pl.ds(step * OWN_GROUP * WIN, OWN_GROUP * WIN)
        pairs = ((half_s, half_ref), (att_s, att_ref), (gate_s, gate_ref))
        return [
            pltpu.make_async_copy(a.at[rows], b.at[rows], sem_out.at[step, j])
            for j, (a, b) in enumerate(pairs)
        ]

    for i in range(DONE):
        for copy in loads(i):
            copy.start()
        if i == OWN_GROUP - 1:
            load_w.start()

    def group(step, carry):
        for j in range(OWN_GROUP):
            for copy in loads(step * OWN_GROUP + j):
                copy.wait()
        rows = pl.ds(pl.multiple_of(step * OWN_GROUP * WIN, WIN), OWN_GROUP * WIN)
        half = norm_half(x_s[rows, :].astype(F32))
        half_s[rows, :] = half

        @pl.when(step == 0)
        def _():
            load_w.wait()

        u, v, q, k = project([half], [w_s[...]])
        gate_s[rows, :] = u
        att_s[rows, :] = attend_users(OWN_GROUP, q, k, v)
        for copy in sends(step):
            copy.start()
        return carry

    lax.fori_loop(0, DONE // OWN_GROUP, group, 0)
    for step in range(DONE // OWN_GROUP):
        for copy in sends(step):
            copy.wait()


def in_vmem():
    return pl.BlockSpec(memory_space=pltpu.VMEM)


def in_hbm():
    return pl.BlockSpec(memory_space=pltpu.HBM)


def keep(array):
    return pltpu.with_memory_space_constraint(array, pltpu.VMEM)


def own_head(tokens, starts, part, w_own):
    kept = [((DONE * WIN, D), BF16), ((DONE * WIN, HEAD), F32), ((DONE * WIN, HEAD), BF16)]
    return pl.pallas_call(
        own_head_kernel,
        grid_spec=pltpu.PrefetchScalarGridSpec(
            num_scalar_prefetch=2,
            grid=(1,),
            in_specs=[in_hbm()] * 2,
            out_specs=[in_hbm()] * 3,
            scratch_shapes=[pltpu.VMEM((DONE * WIN, D), BF16)]
            + [pltpu.VMEM(*k) for k in kept]
            + [
                pltpu.VMEM((D, D), BF16),
                pltpu.SemaphoreType.DMA((DONE, MAXB)),
                pltpu.SemaphoreType.DMA,
                pltpu.SemaphoreType.DMA((DONE // OWN_GROUP, 3)),
            ],
        ),
        out_shape=[jax.ShapeDtypeStruct(*k) for k in kept],
        cost_estimate=pl.CostEstimate(
            flops=DONE * WIN * D * D * 64, bytes_accessed=DONE * WIN * D * 8, transcendentals=0
        ),
        name="own_head",
    )(starts, part, tokens, w_own)


def rows_of(tiles):
    return jnp.concatenate(
        [tiles[..., q, :, :].reshape(-1, HEAD) for q in range(N_MP)], axis=1
    )


def pack_kernel(
    start_ref, part_ref, core_ref, tokens_ref, w_ref, owner_ref, len_ref, off_ref,
    out_ref, rows_ref, x_s, table_s, row_s, out_s, sem, sem_t, sem_w, sem_out,
):
    tables = [
        pltpu.make_async_copy(ref, table_s.at[j], sem_t.at[j])
        for j, ref in enumerate((owner_ref, len_ref, off_ref))
    ]
    half = D // 2
    weights = pltpu.make_async_copy(w_ref.at[pl.ds(core_ref[0] * half, half)], rows_ref, sem_w)
    loads = [
        token_copies(
            tokens_ref, start_ref[0, part_ref[0] * MINE + k], x_s, k * WIN, sem.at[k]
        )
        for k in range(RAW)
    ]
    for copy in tables + loads[0] + [weights] + loads[1]:
        copy.start()
    row_s[...] = jnp.zeros_like(row_s)
    for j, copy in enumerate(tables):
        copy.wait()
        row_s[:, j * USERS : (j + 1) * USERS] = table_s[j] if j else N_DP - 1 - table_s[j]
    tile = jnp.broadcast_to(row_s[...], (TILE, 128)).astype(F32).astype(BF16)
    for k in range(RAW):
        out_s[k, :, N_MP] = jnp.broadcast_to(tile[None], (GROUPS, TILE, 128))
    sends = [pltpu.make_async_copy(out_s.at[k], out_ref.at[k], sem_out.at[k]) for k in range(RAW)]
    for k in range(RAW):
        for copy in loads[k]:
            copy.wait()
        for q in range(N_MP):
            out_s[k, :, q] = x_s[k * WIN : (k + 1) * WIN, q * HEAD : (q + 1) * HEAD].reshape(
                GROUPS, TILE, HEAD
            )
        sends[k].start()
    weights.wait()
    for copy in sends:
        copy.wait()


def pack(tokens, starts, part, core, w_own, owner, hist_len, recv_offset):
    shape = (RAW, GROUPS, RAW_MSG, TILE, HEAD)
    return pl.pallas_call(
        pack_kernel,
        grid_spec=pltpu.PrefetchScalarGridSpec(
            num_scalar_prefetch=3,
            grid=(1,),
            in_specs=[in_hbm()] * 5,
            out_specs=[in_hbm(), in_vmem()],
            scratch_shapes=[
                pltpu.VMEM((RAW * WIN, D), BF16),
                pltpu.VMEM((3, 1, USERS), jnp.int32),
                pltpu.VMEM((1, 128), jnp.int32),
                pltpu.VMEM(shape, BF16),
                pltpu.SemaphoreType.DMA((RAW, MAXB)),
                pltpu.SemaphoreType.DMA((3,)),
                pltpu.SemaphoreType.DMA,
                pltpu.SemaphoreType.DMA((RAW,)),
            ],
        ),
        out_shape=[jax.ShapeDtypeStruct(shape, BF16), pltpu.VMEM((D // 2, D), BF16)],
        name="pack",
    )(starts, part, core, tokens, w_own, owner, hist_len, recv_offset)


def head_order(part, core):
    down, up = (part + HEADS - 1) % HEADS, (part + 1) % HEADS
    first = core == 0
    return [part, jnp.where(first, down, up), jnp.where(first, up, down), (part + 2) % HEADS]


def mix(low_is_near, half_rows, first, whole, halves, w_out_of, x_rows):
    low = half_rows[:, : D // 2]
    high = half_rows[:, D // 2 :]
    parts = [jnp.where(low_is_near, low, high), jnp.where(low_is_near, high, low)]
    users = half_rows.shape[0] // WIN
    heads, gates = [first[0]], [first[1]]
    for rows, refs in (([half_rows], whole[:1]), ([half_rows], whole[1:]), (parts, halves)):
        u, v, q, k = project(rows, [ref[...] for ref in refs])
        gates.append(u)
        heads.append(attend_users(users, q, k, v))
    total = jnp.sum(heads[0] + heads[1] + (heads[2] + heads[3]), axis=1, keepdims=True)
    squares = jnp.sum(
        heads[0] * heads[0] + heads[1] * heads[1] + (heads[2] * heads[2] + heads[3] * heads[3]),
        axis=1,
        keepdims=True,
    )
    mean, inv = norm_stats(total, squares, 1.0 / WIN)
    gated = jnp.concatenate(
        [((a - mean) * inv * g.astype(F32)).astype(BF16) for a, g in zip(heads, gates)], axis=1
    )
    return jnp.dot(gated, w_out_of(), preferred_element_type=F32) + x_rows().astype(F32)


def attend_users(users, q, k, v):
    return jnp.concatenate(
        [attend(*(t[j * WIN : (j + 1) * WIN] for t in (q, k, v))) for j in range(users)], axis=0
    )


def live_rows(mixed, length):
    at = lax.broadcasted_iota(jnp.int32, (WIN, 1), 0)
    return jnp.where(at < length, mixed, 0.0).astype(BF16)


def last_row(tile, length):
    pick = lax.broadcasted_iota(jnp.int32, (TILE, HEAD), 0) == (length - 1) % TILE
    return jnp.sum(jnp.where(pick, tile.astype(F32), 0.0), axis=0, keepdims=True).astype(BF16)


def w_out_copies(part, core, w_out_ref, w_out_s, sem):
    return [
        pltpu.make_async_copy(
            w_out_ref.at[pl.ds(h * HEAD, HEAD)], w_out_s.at[pl.ds(s * HEAD, HEAD)], sem.at[s]
        )
        for s, h in enumerate(head_order(part, core))
    ]


def layer_kernel(
    start_ref, len_ref, part_ref, core_ref, tokens_ref, half_hbm, att_hbm, gate_hbm, *rest
):
    whole, halves, (w_out_ref, out_ref, state_ref) = rest[:2], rest[2:4], rest[4:7]
    x_s, half_s, att_s, gate_s, w_out_s, out_s, sem_in, sem_w, sem_out = rest[7:]
    low_is_near = core_ref[0] == 0
    first_id = part_ref[0] * MINE + RAW

    def loads(i):
        rows = pl.ds(i * WIN, WIN)
        pairs = ((half_hbm, half_s), (att_hbm, att_s), (gate_hbm, gate_s))
        return [
            pltpu.make_async_copy(a.at[rows], b.at[rows], sem_in.at[i, MAXB + j])
            for j, (a, b) in enumerate(pairs)
        ] + token_copies(tokens_ref, start_ref[0, first_id + i], x_s, i * WIN, sem_in.at[i])

    weights = w_out_copies(part_ref[0], core_ref[0], w_out_ref, w_out_s, sem_w)

    def sends(i):
        at = (i % HALVES, slice(None), pl.ds((i // HALVES) * N_MP, N_MP))
        return pltpu.make_async_copy(out_s.at[at], out_ref.at[at], sem_out.at[i])

    for i in range(DONE):
        for copy in loads(i):
            copy.start()
        if i == GROUP - 1:
            for copy in weights:
                copy.start()

    def group(step, carry):
        first_user = step * GROUP
        for j in range(GROUP):
            for copy in loads(first_user + j):
                copy.wait()
        rows = pl.ds(pl.multiple_of(first_user * WIN, WIN), GROUP * WIN)

        def w_out_of():
            @pl.when(step == 0)
            def _():
                for copy in weights:
                    copy.wait()

            return w_out_s[...]

        both = mix(
            low_is_near,
            half_s[rows, :],
            (att_s[rows, :], gate_s[rows, :]),
            whole,
            halves,
            w_out_of,
            lambda: x_s[rows, :],
        )
        for j in range(GROUP):
            i = first_user + j
            length = len_ref[0, first_id + i]
            half_id = i % HALVES
            base = (i // HALVES) * N_MP
            mixed = live_rows(both[j * WIN : (j + 1) * WIN], length)
            for q in range(N_MP):
                out_s[half_id, :, base + q] = mixed[:, q * HEAD : (q + 1) * HEAD].reshape(
                    GROUPS, TILE, HEAD
                )
            sends(i).start()
            for q in range(N_MP):
                state_ref[i, :, q * HEAD : (q + 1) * HEAD] = last_row(
                    out_s[half_id, (length - 1) // TILE, base + q], length
                )
        return carry

    lax.fori_loop(0, DONE // GROUP, group, 0)
    for i in range(DONE):
        sends(i).wait()


def layer(tokens, starts, lengths, part, core, kept, weights, w_out):
    message = (HALVES, GROUPS, MSG, TILE, HEAD)
    return pl.pallas_call(
        layer_kernel,
        grid_spec=pltpu.PrefetchScalarGridSpec(
            num_scalar_prefetch=4,
            grid=(1,),
            in_specs=[in_hbm()] * 4 + [in_vmem()] * 4 + [in_hbm()],
            out_specs=[in_hbm(), in_vmem()],
            scratch_shapes=[
                pltpu.VMEM((DONE * WIN, D), BF16),
                pltpu.VMEM((DONE * WIN, D), BF16),
                pltpu.VMEM((DONE * WIN, HEAD), F32),
                pltpu.VMEM((DONE * WIN, HEAD), BF16),
                pltpu.VMEM((D, D), BF16),
                pltpu.VMEM((HALVES, GROUPS, ROUND * N_MP, TILE, HEAD), BF16),
                pltpu.SemaphoreType.DMA((DONE, 5)),
                pltpu.SemaphoreType.DMA((HEADS,)),
                pltpu.SemaphoreType.DMA((DONE,)),
            ],
        ),
        out_shape=[
            jax.ShapeDtypeStruct(message, BF16),
            jax.ShapeDtypeStruct((DONE, 1, D), BF16),
        ],
        name="layer",
    )(starts, lengths, part, core, tokens, *kept, *map(keep, weights), w_out)


def raw_kernel(first_tile, len_ref, part_ref, core_ref, src_ref, w_own_ref, *rest):
    whole, halves, w_out_ref = rest[:2], rest[2:4], rest[4]
    pieces = rest[5 : 5 + N_MP]
    state_ref, x_s, w_out_s, mixed_s, sem_x, sem_w = rest[5 + N_MP :]
    part = part_ref[0]
    lengths = [len_ref[0, part * MINE + k] for k in range(RAW)]
    loads = [
        pltpu.make_async_copy(
            src_ref.at[pl.ds(k * GROUPS, GROUPS), pl.ds(first_tile, N_MP)], x_s.at[k], sem_x.at[k]
        )
        for k in range(RAW)
    ]
    weights = w_out_copies(part, core_ref[0], w_out_ref, w_out_s, sem_w)
    for copy in loads + weights:
        copy.start()
    for copy in loads:
        copy.wait()

    def x_rows():
        return rows_of(x_s[...])

    half = norm_half(x_rows().astype(F32))
    u, v, q, k = project([half], [w_own_ref[...]])

    def w_out_of():
        for copy in weights:
            copy.wait()
        return w_out_s[...]

    both = mix(
        core_ref[0] == 0, half, (attend_users(RAW, q, k, v), u), whole, halves, w_out_of, x_rows
    )
    for k in range(RAW):
        mixed = live_rows(both[k * WIN : (k + 1) * WIN], lengths[k])
        for q in range(N_MP):
            mixed_s[q, k] = mixed[:, q * HEAD : (q + 1) * HEAD].reshape(GROUPS, TILE, HEAD)
        for q in range(N_MP):
            state_ref[k, :, q * HEAD : (q + 1) * HEAD] = last_row(
                mixed_s[q, k, (lengths[k] - 1) // TILE], lengths[k]
            )
    for s in range(N_MP):
        pieces[s][...] = mixed_s[(part + s) % N_MP]


def raw_layer(source, first_tile, lengths, part, core, w_own, weights, w_out):
    piece = jax.ShapeDtypeStruct((RAW, GROUPS, TILE, HEAD), BF16)
    outs = pl.pallas_call(
        lambda *refs: raw_kernel(first_tile, *refs),
        grid_spec=pltpu.PrefetchScalarGridSpec(
            num_scalar_prefetch=3,
            grid=(1,),
            in_specs=[in_hbm()] + [in_vmem()] * 5 + [in_hbm()],
            out_specs=[in_vmem()] * (N_MP + 1),
            scratch_shapes=[
                pltpu.VMEM((RAW, GROUPS, N_MP, TILE, HEAD), BF16),
                pltpu.VMEM((D, D), BF16),
                pltpu.VMEM((N_MP, RAW, GROUPS, TILE, HEAD), BF16),
                pltpu.SemaphoreType.DMA((RAW,)),
                pltpu.SemaphoreType.DMA((HEADS,)),
            ],
        ),
        out_shape=[piece] * N_MP + [jax.ShapeDtypeStruct((RAW, 1, D), BF16)],
    )(lengths, part, core, source, w_own, *weights, w_out)
    return outs[:N_MP], outs[N_MP]


def merge_kernel(first_ref, in_ref, msg_ref, out_ref, sorted_s, table_v, table_s, sem):
    lane = lax.broadcasted_iota(jnp.int32, (TILE, 128), 1)
    column = (lane == first_ref[0]).astype(F32).astype(BF16)
    tiles = in_ref[:, N_MP].reshape(N_DP * TILE, 128)
    seats = lax.dot_general(column, tiles, (((1,), (1,)), ((), ())), preferred_element_type=F32)
    table_v[...] = seats.astype(jnp.int32)
    copy = pltpu.make_async_copy(table_v.at[pl.ds(0, 1)], table_s, sem.at[0])
    copy.start()
    copy.wait()

    def one(d, carry):
        o = table_s[0, d * TILE]
        for q in range(N_MP):
            sorted_s[o, q] = in_ref[d, q]
        return carry

    lax.fori_loop(0, N_DP, one, 0, unroll=8)
    send = pltpu.make_async_copy(sorted_s, out_ref.at[:, pl.ds(ROUND * N_MP, N_MP)], sem.at[1])
    send.start()
    send.wait()


def merge(spread, first, message):
    return pl.pallas_call(
        merge_kernel,
        grid_spec=pltpu.PrefetchScalarGridSpec(
            num_scalar_prefetch=1,
            grid=(1,),
            in_specs=[in_vmem(), in_hbm()],
            out_specs=in_hbm(),
            scratch_shapes=[
                pltpu.VMEM((N_DP, N_MP, TILE, HEAD), BF16),
                pltpu.VMEM((TILE, N_DP * TILE), jnp.int32),
                pltpu.SMEM((1, N_DP * TILE), jnp.int32),
                pltpu.SemaphoreType.DMA((2,)),
            ],
        ),
        out_shape=jax.ShapeDtypeStruct((N_DP, MSG, TILE, HEAD), BF16),
        input_output_aliases={2: 0},
        name="merge",
    )(first, keep(spread), message)


def regroup_kernel(from_ref, in_ref, out_ref, out_s, sem):
    chunk = N_DP // CHUNKS

    def send(c):
        at = pl.ds(c * chunk, chunk)
        return pltpu.make_async_copy(out_s.at[at], out_ref.at[at], sem.at[c])

    def one(c, carry):
        for j in range(chunk):
            o = c * chunk + j
            for r in range(ROUND):
                d = from_ref[r * N_DP + o]
                for q in range(N_MP):
                    out_s[o, q, r] = in_ref[d, r * N_MP + q]
        send(c).start()
        return carry

    lax.fori_loop(0, CHUNKS, one, 0)
    for c in range(CHUNKS):
        send(c).wait()


def regroup(spread, source):
    shape = (N_DP, N_MP, ROUND, TILE, HEAD)
    return pl.pallas_call(
        regroup_kernel,
        grid_spec=pltpu.PrefetchScalarGridSpec(
            num_scalar_prefetch=1,
            grid=(1,),
            in_specs=[in_vmem()],
            out_specs=in_hbm(),
            scratch_shapes=[pltpu.VMEM(shape, BF16), pltpu.SemaphoreType.DMA((CHUNKS,))],
        ),
        out_shape=jax.ShapeDtypeStruct(shape, BF16),
        name="regroup",
    )(source, keep(spread))


def place_raw_kernel(len_ref, off_ref, part_ref, own_ref, *rest):
    out_ref, zero_v, used_s, own_s, sem, sem_zero, sem_own = rest[N_MP - 1 :]
    pieces = (own_s, *rest[: N_MP - 1])
    per_block = BLOCK // TILE
    load = pltpu.make_async_copy(own_ref, own_s, sem_own)
    load.start()
    zero_v[...] = jnp.zeros_like(zero_v)

    def clear(b, carry):
        used_s[b] = 0
        return carry

    lax.fori_loop(0, BLK_DEV, clear, 0, unroll=8)

    def mark(u, carry):
        used_s[off_ref[u]] = 1

        @pl.when(len_ref[u] > BLOCK)
        def _():
            used_s[off_ref[u] + 1] = 1

        return carry

    lax.fori_loop(0, USERS, mark, 0)

    def fill(b, carry):
        @pl.when(used_s[b] == 0)
        def _():
            pltpu.make_async_copy(
                zero_v, out_ref.at[pl.ds(b * per_block, per_block)], sem_zero
            ).start()

        return carry

    lax.fori_loop(0, BLK_DEV, fill, 0)

    def copies(s, k, blocks):
        u = (part_ref[0] + N_MP - s) % N_MP * MINE + k
        tiles = blocks * per_block
        copy = pltpu.make_async_copy(
            pieces[s].at[k, pl.ds(0, tiles)],
            out_ref.at[pl.ds(off_ref[u] * per_block, tiles)],
            sem.at[s, k],
        )
        return (len_ref[u] > BLOCK) == (blocks == MAXB), copy

    def each(act):
        for s in (1, 2, 3, 0):
            for k in range(RAW):
                for blocks in (1, MAXB):
                    when, copy = copies(s, k, blocks)
                    pl.when(when)(lambda copy=copy: act(copy))

    load.wait()
    each(lambda copy: copy.start())
    each(lambda copy: copy.wait())

    def filled(b, carry):
        @pl.when(used_s[b] == 0)
        def _():
            pltpu.make_async_copy(
                zero_v, out_ref.at[pl.ds(b * per_block, per_block)], sem_zero
            ).wait()

        return carry

    lax.fori_loop(0, BLK_DEV, filled, 0)


OUT_SHAPE = (BLK_DEV * BLOCK // TILE, TILE, HEAD)


def place_raw(pieces, lengths, offsets, part):
    return pl.pallas_call(
        place_raw_kernel,
        grid_spec=pltpu.PrefetchScalarGridSpec(
            num_scalar_prefetch=3,
            grid=(1,),
            in_specs=[in_hbm()] + [in_vmem()] * (N_MP - 1),
            out_specs=in_hbm(),
            scratch_shapes=[
                pltpu.VMEM((BLOCK // TILE, TILE, HEAD), BF16),
                pltpu.SMEM((BLK_DEV,), jnp.int32),
                pltpu.VMEM((RAW, GROUPS, TILE, HEAD), BF16),
                pltpu.SemaphoreType.DMA((N_MP, RAW)),
                pltpu.SemaphoreType.DMA,
                pltpu.SemaphoreType.DMA,
            ],
        ),
        out_shape=jax.ShapeDtypeStruct(OUT_SHAPE, BF16),
        compiler_params=pltpu.CompilerParams(vmem_limit_bytes=32 * 1024 * 1024),
        name="place_raw",
    )(lengths, offsets, part, pltpu.with_memory_space_constraint(pieces[0], pltpu.HBM), *pieces[1:])


def place_kernel(len_ref, off_ref, in_ref, partial_ref, out_ref, sem):
    per_block = BLOCK // TILE

    def each(act):
        def one(n, carry):
            m = n // DONE
            i = n % DONE
            u = m * MINE + RAW + i
            for blocks in (1, MAXB):
                tiles = blocks * per_block
                copy = pltpu.make_async_copy(
                    in_ref.at[i % HALVES, pl.ds(0, tiles), m, i // HALVES],
                    out_ref.at[pl.ds(off_ref[u] * per_block, tiles)],
                    sem.at[n],
                )
                pl.when((len_ref[u] > BLOCK) == (blocks == MAXB))(lambda copy=copy: act(copy))
            return carry

        lax.fori_loop(0, N_MP * DONE, one, 0, unroll=True)

    each(lambda copy: copy.start())
    each(lambda copy: copy.wait())


def place(arrived, partial, lengths, offsets):
    return pl.pallas_call(
        place_kernel,
        grid_spec=pltpu.PrefetchScalarGridSpec(
            num_scalar_prefetch=2,
            grid=(1,),
            in_specs=[in_vmem(), in_hbm()],
            out_specs=in_hbm(),
            scratch_shapes=[pltpu.SemaphoreType.DMA((N_MP * DONE,))],
        ),
        out_shape=jax.ShapeDtypeStruct(OUT_SHAPE, BF16),
        input_output_aliases={3: 0},
        compiler_params=pltpu.CompilerParams(vmem_limit_bytes=56 * 1024 * 1024),
        name="place",
    )(lengths, offsets, keep(arrived), partial).reshape(BLK_DEV * BLOCK, HEAD)


def along_mp(array, s):
    return lax.ppermute(array, "mp", [(i, (i + s) % N_MP) for i in range(N_MP)])


def per_device(tokens, w_uvqk, w_out, hist_len, owner, recv_offset, block_start):
    me = lax.axis_index("dp")
    part = lax.axis_index("mp")
    first = part * MINE
    core = me % 2
    seat = N_DP - 1 - me
    half = seat // GROUPS
    part_1, core_1 = part[None], core[None]

    raw, mine_rows = pack(
        tokens, block_start, part_1, core_1, w_uvqk, owner, hist_len, recv_offset
    )
    swap = [(i, i ^ 1) for i in range(N_DP)]
    ring = [
        (d * N_MP + m, d * N_MP + (m + (1 if d % 2 == 0 else N_MP - 1)) % N_MP)
        for d in range(N_DP)
        for m in range(N_MP)
    ]
    side = lax.ppermute(w_uvqk, ("dp", "mp"), ring)
    across = along_mp(mine_rows, 2)
    other_side = lax.ppermute(side, "dp", swap)
    other_across = lax.ppermute(across, "dp", swap)
    weights = (side, other_side, across, other_across)
    raw_in = lax.all_to_all(
        raw.reshape(N_DP, RAW_MSG * TILE, HEAD), "dp", 0, 0, axis_index_groups=[SEATS], tiled=True
    ).reshape(N_DP, RAW_MSG, TILE, HEAD)
    kept = own_head(tokens, block_start, part_1, w_uvqk)
    message, last = layer(
        tokens, block_start, hist_len, part_1, core_1, kept, weights, w_out
    )
    message = merge(
        raw_in, (first + half)[None], message.reshape(N_DP, MSG, TILE, HEAD)
    )
    spread = lax.all_to_all(
        message.reshape(N_DP, MSG * TILE, HEAD), "dp", 0, 0, axis_index_groups=[SEATS], tiled=True
    ).reshape(N_DP, MSG, TILE, HEAD)
    _, raw_last = raw_layer(
        raw.reshape(N_DP, RAW_MSG, TILE, HEAD), 0, hist_len, part_1, core_1,
        w_uvqk, weights, w_out,
    )

    table = raw_in[:, N_MP, 0, :].astype(jnp.int32)
    owners = table[:, :USERS]
    held = lax.dynamic_slice_in_dim(owners, first + RAW + half, HALVES * (ROUND - 1) + 1, 1)
    ids = jnp.arange(N_DP, dtype=jnp.int32)
    source = jnp.sum(
        jnp.where(held[:, ::HALVES].T[:, None, :] == ids[None, :, None], ids[None, None, :], 0), axis=2
    ).reshape(-1)
    mine = owners == seat
    recv_len = jnp.sum(jnp.where(mine, table[:, USERS : 2 * USERS], 0), axis=0)
    recv_off = jnp.sum(jnp.where(mine, table[:, 2 * USERS : 3 * USERS], 0), axis=0)

    sorted_rows = regroup(spread, source)
    arrived = lax.all_to_all(
        sorted_rows.reshape(N_DP * N_MP, ROUND * TILE, HEAD), ("dp", "mp"), 0, 0,
        axis_index_groups=[[d * N_MP + m for d in SEATS for m in range(N_MP)]], tiled=True
    )
    pieces, _ = raw_layer(
        spread, ROUND * N_MP, recv_len[None], part_1, core_1,
        w_uvqk, weights, w_out,
    )
    pieces = [pieces[0]] + [along_mp(pieces[s], s) for s in range(1, N_MP)]
    partial = place_raw(pieces, recv_len, recv_off, part_1)
    packed = place(
        arrived.reshape(HALVES, GROUPS, N_MP, ROUND, TILE, HEAD), partial, recv_len, recv_off
    )

    columns = jnp.concatenate([raw_last, last], axis=0).reshape(MINE, N_MP, HEAD)
    state = jnp.zeros((N_MP, MINE, HEAD), BF16)
    for s in range(N_MP):
        to_part = (part + s) % N_MP
        piece = lax.dynamic_slice_in_dim(columns, to_part, 1, 1)[:, 0]
        if s:
            piece = along_mp(piece, s)
        state = lax.dynamic_update_slice_in_dim(state, piece[None], (part - s) % N_MP, 0)
    return packed, state.reshape(USERS, HEAD)


def solution(mesh):
    in_specs = (
        P("dp", None),
        P(None, "mp"),
        P(),
        P("dp", None),
        P("dp", None),
        P("dp", None),
        P("dp", None),
    )
    out_specs = (P("dp", "mp"), P("dp", "mp"))
    return jax.shard_map(
        per_device, mesh=mesh, in_specs=in_specs, out_specs=out_specs, check_vma=False
    )
```
